256 devices in a mesh: seq: 32 (over y, z), grp: 8 (over x, core).
Axes of the slice: x: 4, y: 4, z: 8, core: 2. Of those that a mesh axis runs over, the one named last changes fastest.
Arguments:
- tokens: bfloat16 [16384, 2560], P('seq'), may hold values from -6 to 6
- norm_gain: float32 [2560], replicated, may hold values from 0.25 to 1.75
- inner_weight: bfloat16 [2560, 2, 5120], P(None, None, ('grp', 'seq')), may hold values from -0.125 to 0.125
- state_weight: bfloat16 [2560, 2, 128], replicated, may hold values from -0.125 to 0.125
- step_weight: bfloat16 [2560, 80], P(None, 'grp'), may hold values from -0.125 to 0.125
- step_bias: float32 [80], P('grp'), may hold values from -1 to 1
- decay_rate: float32 [80], P('grp'), may hold values from 1.2207031e-06 to 0.05
- skip_scale: float32 [80], P('grp'), may hold values from 0.5 to 1.5
- conv_inner: bfloat16 [4, 5120], P(None, 'grp'), may hold values from -3 to 3
- conv_state: bfloat16 [4, 2, 128], replicated, may hold values from -3 to 3
- out_gain: float32 [5120], P('grp'), may hold values from 0.25 to 1.75
- out_weight: bfloat16 [5120, 2560], P(None, 'grp'), may hold values from -0.078125 to 0.078125
Outputs:
- mixed: bfloat16 [16384, 2560], P('seq', 'grp')
The draws below stay inside these ranges and needn't reach their ends.
All inputs are finite; a program needn't handle non-finite values.
Results may differ from the reference program's by a relative error of at most 0.0075.
Values may be sent and summed in bfloat16 or wider, within the bound.
A program may use at most 64 MiB of HBM per device.

```python
import math
from functools import partial
import jax
import jax.numpy as jnp
from jax import lax

D = 2560
D_INNER = 5120
HEADS = 80
HEAD_DIM = 64
D_STATE = 128
SPAN = 256
KERNEL = 4
SEQ_LEN = 16384


def block_levels(key, dims, cuts, smallest, high):
    def one(position, parts):
        draws = jax.random.uniform(jax.random.fold_in(jax.random.fold_in(key, 6), position), (parts,), jnp.float32, smallest / len(cuts), high / len(cuts))
        return jnp.repeat(jnp.exp(draws), dims[position] // parts).reshape((-1,) + (1,) * (len(dims) - position - 1))

    gain = one(*cuts[0])
    for cut in cuts[1:]:
        gain = gain * one(*cut)
    return gain


def bell_draw(rng, extent, scale, limit, split=(), held_as=jnp.bfloat16):
    level = block_levels(rng, extent, split, -0.22, 0.18) if split else 1.0
    drawn = jax.random.normal(rng, extent, jnp.float32) * scale * level
    return jnp.minimum(jnp.maximum(drawn, -limit), limit).astype(held_as)


def setup_inputs(seed: int = 0) -> dict:
    seeds = jax.random.split(jax.random.key(seed), 13)
    return {
        "tokens": bell_draw(seeds[0], (SEQ_LEN, D), 1.0, 6.0, ((0, 32),)),
        "norm_gain": jnp.clip(1.0 + 0.15 * jax.random.normal(seeds[1], (D,), jnp.float32), 0.25, 1.75),
        "inner_weight": bell_draw(seeds[2], (D, 2, D_INNER), D ** -0.5, 0.125, ((2, 256),)),
        "state_weight": bell_draw(seeds[3], (D, 2, D_STATE), D ** -0.5, 0.125),
        "step_weight": bell_draw(seeds[4], (D, HEADS), D ** -0.5, 0.125, ((1, 8),)),
        "step_bias": jnp.clip(jax.random.uniform(seeds[5], (HEADS,), jnp.float32, -1.0, 1.0) * block_levels(seeds[5], (HEADS,), ((0, 8),), -0.4, 0.0), -1.0, 1.0),
        "decay_rate": jnp.clip(jnp.exp(math.log(0.05) - 10.620351 * jax.random.uniform(seeds[6], (HEADS,), jnp.float32) ** block_levels(seeds[6], (HEADS,), ((0, 8),), -0.2, 0.2)), 1.220703097715159e-06, 0.05),
        "skip_scale": jnp.clip(0.5 + 1.0 * jax.random.uniform(seeds[7], (HEADS,), jnp.float32) ** block_levels(seeds[7], (HEADS,), ((0, 8),), -0.2, 0.2), 0.5, 1.5),
        "conv_inner": bell_draw(seeds[8], (KERNEL, D_INNER), KERNEL ** -0.5, 3.0, ((1, 8),)),
        "conv_state": bell_draw(seeds[9], (KERNEL, 2, D_STATE), KERNEL ** -0.5, 3.0),
        "out_gain": jnp.clip(1.0 + 0.15 * jax.random.normal(seeds[10], (D_INNER,), jnp.float32), 0.25, 1.75),
        "out_weight": bell_draw(seeds[11], (D_INNER, D), D_INNER ** -0.5, 0.078125, ((1, 8),)),
    }


EPS = 1e-05
HIGH = lax.Precision.HIGHEST

def causal_conv(current, weight):
    width = weight.shape[0]
    before = jnp.zeros((width - 1,) + current.shape[1:], current.dtype)
    padded = jnp.concatenate([before, current], axis=0).astype(jnp.float32)
    length = current.shape[0]
    total = jnp.zeros(current.shape, jnp.float32)
    for offset in range(width):
        total = total + weight[offset].astype(jnp.float32) * padded[offset:offset + length]
    return jax.nn.silu(total).astype(jnp.bfloat16)

def span_step(rate, skip, state, inputs):
    xvals, bmat, cmat, delta = inputs
    logdec = -delta * rate[None, :]
    cumul = jnp.cumsum(logdec, axis=0)
    length = cumul.shape[0]
    scores = jnp.einsum('tn,sn->ts', cmat.astype(jnp.float32), bmat.astype(jnp.float32), precision=HIGH)
    lower = jnp.arange(length)[:, None] >= jnp.arange(length)[None, :]
    diffs = cumul.T[:, :, None] - cumul.T[:, None, :]
    decay = jnp.exp(jnp.where(lower[None], diffs, -jnp.inf))
    mixer = (scores[None] * decay * delta.T[:, None, :]).astype(jnp.bfloat16)
    xwide = xvals.astype(jnp.float32)
    intra = jnp.einsum('hts,shp->thp', mixer.astype(jnp.float32), xwide, precision=HIGH)
    inter = jnp.exp(cumul)[:, :, None] * jnp.einsum('tn,hpn->thp', cmat.astype(jnp.float32), state, precision=HIGH)
    output = intra + inter + skip[None, :, None] * xwide
    tail = jnp.exp(cumul[-1][None, :] - cumul) * delta
    weighted = (tail[:, :, None] * bmat.astype(jnp.float32)[:, None, :]).astype(jnp.bfloat16)
    update = jnp.einsum('shp,shn->hpn', xwide, weighted.astype(jnp.float32), precision=HIGH)
    new_state = jnp.exp(cumul[-1])[:, None, None] * state + update
    return (new_state, output)

def reference(tokens, norm_gain, inner_weight, state_weight, step_weight, step_bias, decay_rate, skip_scale, conv_inner, conv_state, out_gain, out_weight):
    length = tokens.shape[0]
    wide = tokens.astype(jnp.float32)
    normed = (wide * lax.rsqrt(lax.optimization_barrier(jnp.mean(wide * wide, axis=1, keepdims=True)) + EPS) * norm_gain).astype(jnp.bfloat16)
    normed_wide = normed.astype(jnp.float32)
    inner = jnp.dot(normed_wide, inner_weight.reshape(D, 2 * D_INNER).astype(jnp.float32), precision=HIGH)
    inner = inner.astype(jnp.bfloat16).reshape(length, 2, D_INNER)
    state_pre = jnp.dot(normed_wide, state_weight.reshape(D, 2 * D_STATE).astype(jnp.float32), precision=HIGH)
    state_pre = state_pre.astype(jnp.bfloat16).reshape(length, 2, D_STATE)
    delta = jax.nn.softplus(jnp.dot(normed_wide, step_weight.astype(jnp.float32), precision=HIGH) + step_bias)
    values = causal_conv(inner[:, 0, :], conv_inner)
    conv_out = causal_conv(state_pre, conv_state)
    blocks = length // SPAN
    xs_blocks = values.reshape(blocks, SPAN, HEADS, HEAD_DIM)
    b_blocks = conv_out[:, 0, :].reshape(blocks, SPAN, D_STATE)
    c_blocks = conv_out[:, 1, :].reshape(blocks, SPAN, D_STATE)
    d_blocks = delta.reshape(blocks, SPAN, HEADS)
    initial = jnp.zeros((HEADS, HEAD_DIM, D_STATE), jnp.float32)
    _, outputs = lax.scan(partial(span_step, decay_rate, skip_scale), initial, (xs_blocks, b_blocks, c_blocks, d_blocks))
    mixed_heads = outputs.reshape(length, D_INNER)
    gated = mixed_heads * jax.nn.silu(inner[:, 1, :].astype(jnp.float32))
    meansq = lax.optimization_barrier(jnp.mean(gated * gated, axis=1))
    scaled = (gated * out_gain).astype(jnp.bfloat16)
    projected = jnp.dot(scaled.astype(jnp.float32), out_weight.astype(jnp.float32), precision=HIGH)
    return (projected * lax.rsqrt(meansq + EPS)[:, None]).astype(jnp.bfloat16)
```

```python
import functools

import jax
import jax.numpy as jnp
from jax import lax
from jax.experimental import pallas as pl
from jax.experimental.pallas import tpu as pltpu
from jax.sharding import PartitionSpec as P

MESH = pl.DeviceIdType.MESH
BF = jnp.bfloat16
F32 = jnp.float32
EPS = 1e-05

TOK = 512
D = 2560
CH = 640
HEADS = 10
SPAN = 256
KA, KB = 512, 768
FEAT = 320
NY, NZ, NX = 4, 8, 4


def dot(a, b):
    return jnp.dot(a, b, preferred_element_type=F32)


def half_messages(h):
    m = {}
    for d in (1, -1):
        m["Ay", h, d] = (("y", d), 0.88, [])
        m["Ay2", h, d] = (("y", d), 0.44, [("Ay", h, d)])
        for k in range(1, 5):
            rels = (0, -1, 1, 2) if k < 4 else ((0, -1) if d == 1 else (1, 2))
            for rel in rels:
                if k > 1:
                    dep = [("Az", h, d, k - 1, rel)]
                else:
                    dep = {
                        0: [],
                        -1: [("Ay", h, 1)],
                        1: [("Ay", h, -1)],
                        2: [("Ay2", h, 1), ("Ay2", h, -1)],
                    }[rel]
                m["Az", h, d, k, rel] = (("z", d), 0.88, dep)
            dep = [("Bz", h, d, k - 1)] if k > 1 else []
            m["Bz", h, d, k] = (("z", d), 1.32 if k < 4 else 0.66, dep)
        for zr in range(-3, 5):
            if zr == 0:
                dep = []
            elif zr == 4:
                dep = [("Bz", h, 1, 4), ("Bz", h, -1, 4)]
            else:
                dep = [("Bz", h, 1, -zr)] if zr < 0 else [("Bz", h, -1, zr)]
            m["By", h, d, zr] = (("y", d), 1.32, dep)
            if (zr <= 0) == (d == 1):
                m["By2", h, d, zr] = (("y", d), 1.32, [("By", h, d, zr)])
    return m


def build_schedule():
    msgs = {}
    for d in (1, -1):
        msgs["X2", d] = (("x", d), 10.5, [])
        msgs["X1", d] = (("x", d), 21.0, [])
        msgs["X2f", d] = (("x", d), 10.5, [("X2", d)])
    for h in (0, 1):
        msgs.update(half_messages(h))
    order = {k: i for i, k in enumerate(msgs)}

    def rank(k):
        h = k[1] if k[0][0] in "AB" else 0
        fan = 0 if k[0] in ("Bz", "Ay", "X2", "X2f") else 1
        return (h, fan, order[k])

    latency = 2.2
    arrived, started = {}, {}
    free = {}
    pending = set(msgs)
    while pending:
        best = None
        for k in pending:
            link, dur, deps = msgs[k]
            if any(q not in arrived for q in deps):
                continue
            ready = max([arrived[q] for q in deps], default=0.0)
            t = max(ready, free.get(link, 0.0))
            key = (t, rank(k))
            if best is None or key < best[0]:
                best = (key, k, t)
        _, k, t = best
        link, dur, _ = msgs[k]
        started[k] = t
        free[link] = t + dur
        arrived[k] = t + dur + latency
        pending.remove(k)
    events = []
    for k in msgs:
        ready = max([arrived[q] for q in msgs[k][2]], default=0.0)
        events.append((max(ready, started[k] - 3.0), started[k], order[k], k))
    events.sort()
    half_done = [max(arrived[k] for k in msgs if k[0][0] in "AB" and k[1] == h) for h in (0, 1)]
    return msgs, [(e[0], e[3]) for e in events], half_done


MSGS, EVENTS, HALF_DONE = build_schedule()
IDS = {k: i for i, k in enumerate(MSGS)}
N_MSG = len(MSGS)


def kernel(
    tok, gain, own_a, own_b, sw, st, bias, rate, skip, cwin, cwst, og, ow,
    out,
    wa, wb, nrm, nt, spf, cb, ct, dec, cum, ecum, tailw, d01, scores, mix, colt,
    p0s, p1s, inn, gat, vt, vw, u, yv, cs, cr, co, ci, tt, rowd, prefix,
    sbf, s_t, scb, wr, relay, sq, rs_out, rs_in1, rs2_out, rs2_in, own_p,
    halo, send, recv, xsend, xrecv, lsem,
):
    seq = lax.axis_index("seq")
    grp = lax.axis_index("grp")
    y, z = seq // NZ, lax.rem(seq, NZ)
    x, c = grp // 2, lax.rem(grp, 2)

    def yy(d):
        return lax.rem(y + d + NY, NY)

    def zz(d):
        return lax.rem(z + d + NZ, NZ)

    def xx(d):
        return lax.rem(x + d + NX, NX)

    def dev(dy=0, dz=0, dx=0, dc=0):
        return (yy(dy) * NZ + zz(dz), xx(dx) * 2 + lax.rem(c + dc, 2))

    nxt = (lax.rem(seq + 1, NY * NZ), grp)
    prv = (lax.rem(seq + NY * NZ - 1, NY * NZ), grp)

    barrier = pltpu.get_barrier_semaphore()
    peers = [nxt, prv]
    peers += [dev(dz=k) for k in range(1, NZ)]
    peers += [dev(dy=k) for k in range(1, NY)]
    peers += [dev(dx=k // 2, dc=k % 2) for k in range(1, 8)]
    for p in peers:
        pl.semaphore_signal(barrier, inc=1, device_id=p, device_id_type=MESH)

    own_out = pltpu.make_async_copy(
        ow.at[pl.ds(pl.multiple_of(x * 1280, 1280), 1280)], wr.at[x], lsem.at[0]
    )
    own_out.start()
    own_in = []
    for h in (0, 1):
        own_in.append(pltpu.make_async_copy(own_a.at[h], wa.at[h, y, z], lsem.at[1 + h]))
        own_in.append(pltpu.make_async_copy(own_b.at[h], wb.at[h, y, z], lsem.at[3 + h]))
    for q in own_in:
        q.start()
    nrm[0:128, :] = jnp.zeros((128, D), BF)
    pl.semaphore_wait(barrier, len(peers))

    def remote(src, dst, s, r, to):
        return pltpu.make_async_remote_copy(
            src_ref=src, dst_ref=dst, send_sem=s, recv_sem=r, device_id=to, device_id_type=MESH
        )

    def message(k):
        i = IDS[k]
        kind = k[0]
        if kind[0] == "X":
            d = k[1]
            if kind == "X1":
                src = ow.at[pl.ds(pl.multiple_of(xx(d) * 1280, 1280), 1280)]
                dst = wr.at[x]
            elif kind == "X2":
                off = 0 if d == 1 else 640
                src = ow.at[pl.ds(pl.multiple_of(xx(2) * 1280, 1280) + off, 640)]
                dst = relay.at[0 if d == 1 else 1]
            else:
                off = 0 if d == 1 else 640
                src = relay.at[0 if d == 1 else 1]
                dst = wr.at[xx(-d), pl.ds(off, 640)]
            return remote(src, dst, send.at[i], recv.at[i], dev(dx=d))
        h, d = k[1], k[2]
        if kind == "Ay":
            src, dst, to = own_a.at[h], wa.at[h, y, z], dev(dy=d)
        elif kind == "Ay2":
            cols = pl.ds(0 if d == 1 else KA // 2, KA // 2)
            src = dst = wa.at[h, yy(-d), z, :, cols]
            to = dev(dy=d)
        elif kind == "Az":
            step, rel = k[3], k[4]
            dst = wa.at[h, yy(rel), zz(-d * (step - 1))]
            src = own_a.at[h] if (step == 1 and rel == 0) else dst
            to = dev(dz=d)
        elif kind == "Bz":
            step = k[3]
            dst = wb.at[h, y, zz(-d * (step - 1))]
            src = own_b.at[h] if step == 1 else dst
            if step == 4:
                cols = pl.ds(0 if d == 1 else KB // 2, KB // 2)
                src = dst = wb.at[h, y, zz(-d * 3), :, cols]
            to = dev(dz=d)
        elif kind == "By":
            zr = k[3]
            dst = wb.at[h, y, zz(zr)]
            src = own_b.at[h] if zr == 0 else dst
            to = dev(dy=d)
        else:
            src = dst = wb.at[h, yy(-d), zz(k[3])]
            to = dev(dy=d)
        return remote(src, dst, send.at[i], recv.at[i], to)

    waited = set()
    queue = list(EVENTS)

    def take(k):
        if k not in waited:
            waited.add(k)
            message(k).wait_recv()

    def progress(until):
        while queue and queue[0][0] <= until:
            _, k = queue.pop(0)
            for q in MSGS[k][2]:
                take(q)
            message(k).start()

    def complete(h):
        for k in MSGS:
            if k[0][0] in "AB" and k[1] == h:
                take(k)

    extra_sends = []

    def extra(src, dst, to, slot):
        q = remote(src, dst, xsend.at[slot], xrecv.at[slot], to)
        q.start()
        extra_sends.append(q)
        return q

    halo_copy = extra(tok.at[pl.ds(TOK - 16, 16)], halo, nxt, 0)

    def norm_rows(v):
        wide = v.astype(F32)
        ms = jnp.mean(wide * wide, axis=1, keepdims=True)
        return wide * lax.rsqrt(ms + EPS) * gain[...]

    def piece_norm(part):
        def step(i, carry):
            r = pl.multiple_of(part * 128 + i * 16, 16)
            nrm[pl.ds(128 + r, 16), :] = norm_rows(tok[pl.ds(r, 16), :]).astype(BF)
            return carry

        lax.fori_loop(0, 8, step, 0)

    def piece_halo():
        halo_copy.wait_recv()
        n = jnp.where(seq > 0, norm_rows(halo[...]), 0.0)
        nrm[112:128, :] = n.astype(BF)

    def piece_transpose(tb):
        def step(i, carry):
            k = pl.multiple_of(i * 128, 128)
            nt[pl.ds(k, 128), tb * 128 : (tb + 1) * 128] = nrm[
                tb * 128 : (tb + 1) * 128, pl.ds(k, 128)
            ].T
            return carry

        lax.fori_loop(0, D // 128, step, 0)

    def piece_state(part):
        r = part * 176
        got = dot(nrm[112 + r : 112 + r + 176, :], sw[...])
        spf[r : r + 176, :] = got.astype(BF).astype(F32)

    def piece_state_conv():
        for q in range(4):
            acc = jnp.zeros((128, 256), F32)
            for j in range(4):
                acc = acc + cwst[j : j + 1, :] * spf[q * 128 + 13 + j : q * 128 + 13 + j + 128, :]
            v = acc * lax.logistic(acc)
            cb[q * 128 : (q + 1) * 128, :] = v[:, :128].astype(BF)
            ct[:, q * 128 : (q + 1) * 128] = v[:, 128:].T.astype(BF)

    def piece_delta():
        pre = dot(st[...], nt[:, 128:640]) + bias[:, 0:1]
        delta = jnp.maximum(pre, 0.0) + jnp.log1p(jnp.exp(-jnp.abs(pre)))
        run = -delta * rate[:, 0:1]
        lane = lax.broadcasted_iota(jnp.int32, (16, TOK), 1) % SPAN
        k = 1
        while k < SPAN:
            run = run + jnp.where(lane >= k, pltpu.roll(run, k, 1), 0.0)
            k *= 2
        cum[...] = run
        ecum[...] = jnp.exp(run)
        tot0, tot1 = run[:, 255:256], run[:, 511:512]
        tailw[:, :SPAN] = jnp.exp(tot0 - run[:, :SPAN]) * delta[:, :SPAN]
        tailw[:, SPAN:] = jnp.exp(tot1 - run[:, SPAN:]) * delta[:, SPAN:]
        d01[0] = jnp.broadcast_to(jnp.exp(tot0), (16, 128))
        d01[1] = jnp.broadcast_to(jnp.exp(tot1), (16, 128))
        whole = jnp.broadcast_to(jnp.exp(tot0) * jnp.exp(tot1), (16, 128))
        for h in range(HEADS):
            dec[8, h] = whole[h : h + 1, :]
            dec[z, h] = whole[h : h + 1, :]
        term = jnp.log(delta) - run
        filled = jnp.concatenate([term, jnp.zeros((112, TOK), F32)], axis=0)
        for q in range(4):
            colt[q * 128 : (q + 1) * 128, :] = filled[:, q * 128 : (q + 1) * 128].T
        for b in range(2):
            s = slice(b * SPAN, (b + 1) * SPAN)
            scores[b] = dot(cb[s, :], ct[:, s])

    dec_copies = []

    def piece_dec_send():
        for k in range(1, NZ):
            dec_copies.append(extra(dec.at[8], dec.at[z], dev(dz=k), k))

    def piece_dec_recv():
        for q in dec_copies:
            q.wait_recv()
        prod = dec[0]
        for k in range(1, NZ):
            prod = prod * dec[k]
        rowd[4] = prod
        rowd[y] = prod
        for k in range(1, NY):
            dec_copies.append(extra(rowd.at[4], rowd.at[y], dev(dy=k), 7 + k))

    def piece_mix(h):
        keep = lax.broadcasted_iota(jnp.int32, (128, 128), 1) >= lax.broadcasted_iota(
            jnp.int32, (128, 128), 0
        )
        for b in range(2):
            for s0 in range(2):
                r = b * SPAN + s0 * 128
                col = jnp.broadcast_to(colt[r : r + 128, h : h + 1], (128, 128))
                for t0 in range(2):
                    sl = (slice(s0 * 128, s0 * 128 + 128), slice(t0 * 128, t0 * 128 + 128))
                    if t0 < s0:
                        mix[(h, b) + sl] = jnp.zeros((128, 128), BF)
                        continue
                    q = b * SPAN + t0 * 128
                    arg = col + cum[h : h + 1, q : q + 128]
                    if s0 == t0:
                        arg = jnp.where(keep, arg, -jnp.inf)
                    mix[(h, b) + sl] = (scores[(b,) + sl] * jnp.exp(arg)).astype(BF)

    def product(h, r, first, width):
        la = wa[h, r].reshape(NZ * 40, KA)
        lb = wb[h, r].reshape(NZ * 40, KB)
        cols = slice(first, first + width)
        p0s[:, :width] = dot(la, nt[0:512, cols]) + dot(lb, nt[512:1280, cols])
        p1s[:, :width] = dot(la, nt[1280:1792, cols]) + dot(lb, nt[1792:2560, cols])

    def piece_inner(r):
        product(0, r, 0, 640)
        for i in range(NZ):
            v = p0s[40 * i : 40 * i + 20, :] + p1s[40 * i + 20 : 40 * i + 40, :]
            inn[r, 20 * i : 20 * i + 20, :] = v.astype(BF).astype(F32)

    def piece_gate(r):
        product(1, r, 128, 512)
        for i in range(NZ):
            v = p0s[40 * i : 40 * i + 20, :512] + p1s[40 * i + 20 : 40 * i + 40, :512]
            gat[r, 20 * i : 20 * i + 20, :] = v.astype(BF).astype(F32)

    def piece_conv(r):
        def step(i, carry):
            q = pl.multiple_of(i * 32, 32)
            row = pl.multiple_of(r * 160 + q, 32)
            v = inn[r, pl.ds(q, 32), :]
            w = cwin[pl.ds(row, 32), :]
            acc = w[:, 3:4] * v[:, 128:]
            for j in range(3):
                acc = acc + w[:, j : j + 1] * pltpu.roll(v, 3 - j, 1)[:, 128:]
            vt[pl.ds(row, 32), :] = (acc * lax.logistic(acc)).astype(BF)
            return carry

        lax.fori_loop(0, 5, step, 0)

    def head_rows(h):
        return pl.ds(pl.multiple_of(h * 64, 64), 64)

    def piece_update():
        def weigh(h, carry):
            vw[head_rows(h), :] = (vt[head_rows(h), :].astype(F32) * tailw[pl.ds(h, 1), :]).astype(BF)
            return carry

        lax.fori_loop(0, HEADS, weigh, 0)
        for b in range(2):
            s = slice(b * SPAN, (b + 1) * SPAN)
            u[b] = dot(vw[:, s], cb[s, :])

        def total(h, carry):
            v = u[0, head_rows(h), :] * d01[1, pl.ds(h, 1), :] + u[1, head_rows(h), :]
            for j in range(NZ):
                cs[j, h] = v[8 * j : 8 * j + 8, :].astype(BF)
            return carry

        lax.fori_loop(0, HEADS, total, 0)
        cr[z] = cs[z]

    carry1, carry2, carry3 = [], [], []

    def piece_carry1():
        for k in range(1, NZ):
            carry1.append(extra(cs.at[zz(k)], cr.at[z], dev(dz=k), 10 + k))

    def piece_carry2():
        for q in carry1:
            q.wait_recv()
        run = jnp.zeros((HEADS, 8, 128), F32)
        for k in range(NZ):
            prefix[k] = run
            run = run * dec[k] + cr[k].astype(F32)
        tt[4] = run
        tt[y] = run
        for k in range(1, NY):
            carry2.append(extra(tt.at[4], tt.at[y], dev(dy=k), 17 + k))

    def piece_carry3():
        for q in carry2 + dec_copies[7:]:
            q.wait_recv()
        r = jnp.zeros((HEADS, 8, 128), F32)
        for k in range(NY - 1):
            r = jnp.where(y > k, r * rowd[k] + tt[k], r)
        for k in range(NZ):
            co[k] = (prefix[k] + r).astype(BF)
            r = r * dec[k]
        ci[z] = co[z]
        for k in range(1, NZ):
            carry3.append(extra(co.at[zz(k)], ci.at[z], dev(dz=k), 20 + k))

    def piece_carry4():
        for q in carry3:
            q.wait_recv()

        def step(h, carry):
            v = jnp.concatenate([ci[j, h].astype(F32) for j in range(NZ)], axis=0)
            sbf[0, head_rows(h), :] = v.astype(BF)
            sbf[1, head_rows(h), :] = (v * d01[0, pl.ds(h, 1), :] + u[0, head_rows(h), :]).astype(BF)
            return carry

        lax.fori_loop(0, HEADS, step, 0)

    def piece_intra(b):
        s = slice(b * SPAN, (b + 1) * SPAN)

        def step(h, carry):
            v = vt[head_rows(h), s]
            yv[head_rows(h), s] = dot(v, mix[h, b]) + skip[h] * v.astype(F32)
            return carry

        lax.fori_loop(0, HEADS, step, 0)

    def piece_inter(b):
        s = slice(b * SPAN, (b + 1) * SPAN)

        def step(h, carry):
            got = dot(sbf[b, head_rows(h), :], ct[:, s])
            yv[head_rows(h), s] = yv[head_rows(h), s] + ecum[pl.ds(h, 1), s] * got
            return carry

        lax.fori_loop(0, HEADS, step, 0)

    pair_copies, sq_copies = [], []

    def piece_gated(b):
        s = slice(b * SPAN, (b + 1) * SPAN)
        total = jnp.zeros((8, SPAN), F32)
        for r in range(NY):

            def step(i, total):
                q = pl.multiple_of(i * 32, 32)
                row = pl.multiple_of(r * 160 + q, 32)
                g = gat[r, pl.ds(q, 32), s]
                v = yv[pl.ds(row, 32), s] * (g * lax.logistic(g))
                for e in range(4):
                    w = v[8 * e : 8 * e + 8, :]
                    total = total + w * w
                s_t[pl.ds(row, 32), s] = (v * og[pl.ds(row, 32), 0:1]).astype(BF)
                return total

            total = lax.fori_loop(0, 5, step, total)
        sq[8, :, s] = total
        for q in range(CH // 128):
            for e in range(2):
                r0 = b * SPAN + e * 128
                scb[c, r0 : r0 + 128, q * 128 : q * 128 + 128] = s_t[
                    q * 128 : q * 128 + 128, r0 : r0 + 128
                ].T
        pair_copies.append(
            extra(scb.at[c, pl.ds(b * SPAN, SPAN)], scb.at[c, pl.ds(b * SPAN, SPAN)], dev(dc=1), 28 + b)
        )

    def piece_squares():
        sq[grp] = sq[8]
        for k in range(1, 8):
            sq_copies.append(extra(sq.at[8], sq.at[grp], dev(dx=k // 2, dc=k % 2), 29 + k))

    def project(dx, half):
        s = slice(half * SPAN, (half + 1) * SPAN)
        p = xx(dx)
        return dot(scb[0, s, :], wr[p, 0:CH, :]) + dot(scb[1, s, :], wr[p, CH : 2 * CH, :])

    for q in own_in:
        q.wait()
    clock = 0.5
    progress(clock)
    front = [(functools.partial(piece_norm, i), 0.5) for i in range(4)]
    front += [(piece_halo, 0.1)]
    front += [(functools.partial(piece_transpose, i), 0.5) for i in range(5)]
    front += [(functools.partial(piece_state, i), 0.3) for i in range(3)]
    front += [(piece_state_conv, 0.3), (piece_delta, 0.6), (piece_dec_send, 0.1)]
    front += [(functools.partial(piece_mix, i), 0.25) for i in range(HEADS)]
    front += [(piece_dec_recv, 0.1)]
    for piece, cost in front:
        piece()
        clock += cost
        progress(clock)
    progress(HALF_DONE[0])
    clock = HALF_DONE[0]
    complete(0)
    middle = []
    for i in range(NY):
        middle += [(functools.partial(piece_inner, i), 1.0), (functools.partial(piece_conv, i), 0.4)]
    middle += [(piece_update, 0.6), (piece_carry1, 0.1)]
    middle += [(functools.partial(piece_intra, i), 0.8) for i in range(2)]
    for piece, cost in middle:
        piece()
        clock += cost
        progress(clock)
    clock += 3.0
    progress(clock)
    piece_carry2()
    clock += 4.0
    progress(clock)
    piece_carry3()
    clock += 5.0
    progress(clock)
    piece_carry4()
    for i in range(2):
        piece_inter(i)
        clock += 0.4
        progress(clock)
    progress(1e9)
    complete(1)
    for i in range(NY):
        piece_gate(i)
    for i in range(2):
        piece_gated(i)
    piece_squares()
    own_out.wait()
    for k in (("X1", 1), ("X1", -1), ("X2f", 1), ("X2f", -1)):
        take(k)
    for q in pair_copies:
        q.wait_recv()
    far = []
    for half, d in ((0, 1), (1, -1)):
        rs_out[half] = project(2, half).astype(BF)
        far.append(extra(rs_out.at[half], rs_in1.at[half], dev(dx=d), 40 + half))
    near = []
    for i, d in enumerate((1, -1)):
        direct = 1 if d == 1 else 0
        rs2_out[i, direct] = project(d, direct).astype(BF)
        near.append(extra(rs2_out.at[i, direct], rs2_in.at[i, direct], dev(dx=d), 42 + 2 * i))
    for i, d in enumerate((1, -1)):
        relayed = 0 if d == 1 else 1
        v = project(d, relayed)
        far[relayed].wait_recv()
        rs2_out[i, relayed] = (v + rs_in1[relayed].astype(F32)).astype(BF)
        near.append(extra(rs2_out.at[i, relayed], rs2_in.at[i, relayed], dev(dx=d), 43 + 2 * i))
    for half in range(2):
        own_p[half] = project(0, half)
    for q in sq_copies:
        q.wait_recv()
    total = sq[0]
    for k in range(1, 8):
        total = total + sq[k]
    total = jnp.sum(total, axis=0, keepdims=True)
    scale = lax.rsqrt(total / (8 * CH) + EPS)
    scale = jnp.broadcast_to(scale, (128, TOK))
    for q in near:
        q.wait_recv()
    for half in range(2):
        v = own_p[half] + rs2_in[0, half].astype(F32) + rs2_in[1, half].astype(F32)
        for e in range(2):
            r0 = half * SPAN + e * 128
            column = scale[:, r0 : r0 + 128].T[:, 0:1]
            out[r0 : r0 + 128, :] = (v[e * 128 : e * 128 + 128, :] * column).astype(BF)
    for k in MSGS:
        message(k).wait_send()
    for q in extra_sends:
        q.wait_send()


def run(*args):
    vm = pl.BlockSpec(memory_space=pltpu.VMEM)
    specs = [vm] * 13
    specs[8] = pl.BlockSpec(memory_space=pltpu.SMEM)
    specs[12] = pl.BlockSpec(memory_space=pl.ANY)
    V = pltpu.VMEM
    scratch = [
        V((2, NY, NZ, 40, KA), BF),
        V((2, NY, NZ, 40, KB), BF),
        V((640, D), BF),
        V((D, 640), BF),
        V((528, 256), F32),
        V((TOK, 128), BF),
        V((128, TOK), BF),
        V((9, HEADS, 1, 128), F32),
        V((16, TOK), F32),
        V((16, TOK), F32),
        V((16, TOK), F32),
        V((2, 16, 128), F32),
        V((2, SPAN, SPAN), F32),
        V((HEADS, 2, SPAN, SPAN), BF),
        V((TOK, 128), F32),
        V((320, 640), F32),
        V((320, 640), F32),
        V((NY, 160, 640), F32),
        V((NY, 160, TOK), F32),
        V((CH, TOK), BF),
        V((CH, TOK), BF),
        V((2, CH, 128), F32),
        V((CH, TOK), F32),
        V((NZ, HEADS, 8, 128), BF),
        V((NZ, HEADS, 8, 128), BF),
        V((NZ, HEADS, 8, 128), BF),
        V((NZ, HEADS, 8, 128), BF),
        V((5, HEADS, 8, 128), F32),
        V((5, HEADS, 1, 128), F32),
        V((NZ, HEADS, 8, 128), F32),
        V((2, CH, 128), BF),
        V((CH, TOK), BF),
        V((2, TOK, CH), BF),
        V((NX, 1280, FEAT), BF),
        V((2, 640, FEAT), BF),
        V((9, 8, TOK), F32),
        V((2, SPAN, FEAT), BF),
        V((2, SPAN, FEAT), BF),
        V((2, 2, SPAN, FEAT), BF),
        V((2, 2, SPAN, FEAT), BF),
        V((2, SPAN, FEAT), F32),
        V((16, D), BF),
        pltpu.SemaphoreType.DMA((N_MSG,)),
        pltpu.SemaphoreType.DMA((N_MSG,)),
        pltpu.SemaphoreType.DMA((48,)),
        pltpu.SemaphoreType.DMA((48,)),
        pltpu.SemaphoreType.DMA((5,)),
    ]
    return pl.pallas_call(
        kernel,
        out_shape=jax.ShapeDtypeStruct((TOK, FEAT), BF),
        in_specs=specs,
        out_specs=vm,
        scratch_shapes=scratch,
        compiler_params=pltpu.CompilerParams(
            collective_id=0, has_side_effects=True, vmem_limit_bytes=64 * 2**20 - 65536
        ),
        name="layer",
    )(*args)


def body(
    tokens, norm_gain, inner_weight, state_weight, step_weight, step_bias, decay_rate,
    skip_scale, conv_inner, conv_state, out_gain, out_weight,
):
    folded = inner_weight.transpose(1, 2, 0).reshape(2, 20, 2, D // 2)
    folded = folded.transpose(0, 2, 1, 3).reshape(2, 40, D // 2)
    steps = jnp.pad(step_weight.T, ((0, 6), (0, 0)))

    def columns(v):
        return jnp.broadcast_to(jnp.pad(v, (0, 6))[:, None], (16, 128))

    return run(
        tokens,
        norm_gain[None, :],
        folded[:, :, :KA],
        folded[:, :, KA:],
        state_weight.reshape(D, 256),
        steps,
        columns(step_bias),
        columns(decay_rate),
        skip_scale,
        conv_inner.T.astype(F32),
        conv_state.reshape(4, 256).astype(F32),
        out_gain[:, None],
        out_weight,
    )


def solution(mesh):
    return jax.shard_map(
        body,
        mesh=mesh,
        in_specs=(
            P("seq", None), P(), P(None, None, ("grp", "seq")), P(), P(None, "grp"), P("grp"),
            P("grp"), P("grp"), P(None, "grp"), P(), P("grp"), P(None, "grp"),
        ),
        out_specs=P("seq", "grp"),
        check_vma=False,
    )
```

```python
import functools

import jax
import jax.numpy as jnp
from jax import lax
from jax.experimental import pallas as pl
from jax.experimental.pallas import tpu as pltpu
from jax.sharding import PartitionSpec as P

MESH = pl.DeviceIdType.MESH
BF = jnp.bfloat16
F32 = jnp.float32
EPS = 1e-05

TOK = 512
D = 2560
CH = 640
HEADS = 10
SPAN = 256
KA, KB = 512, 768
FEAT = 320
NY, NZ, NX = 4, 8, 4


def dot(a, b):
    return jnp.dot(a, b, preferred_element_type=F32)


def half_messages(h):
    m = {}
    for d in (1, -1):
        m["Ay", h, d] = (("y", d), 0.88, [])
        m["Ay2", h, d] = (("y", d), 0.44, [("Ay", h, d)])
        for k in range(1, 5):
            rels = (0, -1, 1, 2) if k < 4 else ((0, -1) if d == 1 else (1, 2))
            for rel in rels:
                if k > 1:
                    dep = [("Az", h, d, k - 1, rel)]
                else:
                    dep = {
                        0: [],
                        -1: [("Ay", h, 1)],
                        1: [("Ay", h, -1)],
                        2: [("Ay2", h, 1), ("Ay2", h, -1)],
                    }[rel]
                m["Az", h, d, k, rel] = (("z", d), 0.88, dep)
            dep = [("Bz", h, d, k - 1)] if k > 1 else []
            m["Bz", h, d, k] = (("z", d), 1.32 if k < 4 else 0.66, dep)
        for zr in range(-3, 5):
            if zr == 0:
                dep = []
            elif zr == 4:
                dep = [("Bz", h, 1, 4), ("Bz", h, -1, 4)]
            else:
                dep = [("Bz", h, 1, -zr)] if zr < 0 else [("Bz", h, -1, zr)]
            m["By", h, d, zr] = (("y", d), 1.32, dep)
            if (zr <= 0) == (d == 1):
                m["By2", h, d, zr] = (("y", d), 1.32, [("By", h, d, zr)])
    return m


def build_schedule():
    msgs = {}
    for d in (1, -1):
        msgs["X2", d] = (("x", d), 10.5, [])
        msgs["X1", d] = (("x", d), 21.0, [])
        msgs["X2f", d] = (("x", d), 10.5, [("X2", d)])
    for h in (0, 1):
        msgs.update(half_messages(h))
    order = {k: i for i, k in enumerate(msgs)}

    def rank(k):
        h = k[1] if k[0][0] in "AB" else 0
        fan = 0 if k[0] in ("Bz", "Ay", "X2", "X2f") else 1
        return (h, fan, order[k])

    latency = 2.2
    arrived, started = {}, {}
    free = {}
    pending = set(msgs)
    while pending:
        best = None
        for k in pending:
            link, dur, deps = msgs[k]
            if any(q not in arrived for q in deps):
                continue
            ready = max([arrived[q] for q in deps], default=0.0)
            t = max(ready, free.get(link, 0.0))
            key = (t, rank(k))
            if best is None or key < best[0]:
                best = (key, k, t)
        _, k, t = best
        link, dur, _ = msgs[k]
        started[k] = t
        free[link] = t + dur
        arrived[k] = t + dur + latency
        pending.remove(k)
    events = []
    for k in msgs:
        ready = max([arrived[q] for q in msgs[k][2]], default=0.0)
        events.append((max(ready, started[k] - 3.0), started[k], order[k], k))
    events.sort()
    half_done = [max(arrived[k] for k in msgs if k[0][0] in "AB" and k[1] == h) for h in (0, 1)]
    return msgs, [(e[0], e[3]) for e in events], half_done


MSGS, EVENTS, HALF_DONE = build_schedule()
IDS = {k: i for i, k in enumerate(MSGS)}
N_MSG = len(MSGS)


def kernel(
    tok_in, gain, own_in, sw_in, st, bias, rate, skip, cw_in, cwst, og_in, ow,
    out,
    tok, own_a, own_b, own_f, sw, swd, cwin, og, wa, wb, nrm, nt, spf, cb, ct, dec, cum, ecum, tailw, d01, scores, mix, term, colt,
    p0s, p1s, inn, gat, vt, vw, u, yv, cs, cr, co, ci, tt, rowd, prefix,
    sbf, scb, wr, relay, sq, rs_out, rs_in1, rs2_out, rs2_in, own_p,
    halo, send, recv, xsend, xrecv, lsem,
):
    seq = lax.axis_index("seq")
    grp = lax.axis_index("grp")
    y, z = seq // NZ, lax.rem(seq, NZ)
    x, c = grp // 2, lax.rem(grp, 2)

    def yy(d):
        return lax.rem(y + d + NY, NY)

    def zz(d):
        return lax.rem(z + d + NZ, NZ)

    def xx(d):
        return lax.rem(x + d + NX, NX)

    def dev(dy=0, dz=0, dx=0, dc=0):
        return (yy(dy) * NZ + zz(dz), xx(dx) * 2 + lax.rem(c + dc, 2))

    nxt = (lax.rem(seq + 1, NY * NZ), grp)
    prv = (lax.rem(seq + NY * NZ - 1, NY * NZ), grp)

    barrier = pltpu.get_barrier_semaphore()
    peers = [nxt, prv]
    peers += [dev(dz=k) for k in range(1, NZ)]
    peers += [dev(dy=k) for k in range(1, NY)]
    peers += [dev(dx=k // 2, dc=k % 2) for k in range(1, 8)]
    for p in peers:
        pl.semaphore_signal(barrier, inc=1, device_id=p, device_id_type=MESH)

    def feature_columns(d, first, count):
        return ow.at[:, pl.ds(pl.multiple_of(xx(d) * 1280 + first, 128), count)]

    tok_copies = []
    for q in range(4):
        part = pl.ds(q * 128, 128)
        tok_copies.append(pltpu.make_async_copy(tok_in.at[part], tok.at[part], lsem.at[q]))
        tok_copies[q].start()
    sw_copy = pltpu.make_async_copy(sw_in, sw, lsem.at[4])
    sw_copy.start()
    own_out = pltpu.make_async_copy(feature_columns(0, 0, 1280), wr.at[x], lsem.at[5])
    own_out.start()
    for r in range(20):
        v = own_in[r].astype(F32)
        for h in (0, 1):
            for part in (0, 1):
                own_f[h, 20 * part + r : 20 * part + r + 1, :] = v[
                    h : h + 1, part * (D // 2) : (part + 1) * (D // 2)
                ]
    for h in (0, 1):
        v = own_f[h].astype(BF)
        own_a[h] = v[:, :KA]
        own_b[h] = v[:, KA:]
        wa[h, y, z] = v[:, :KA]
        wb[h, y, z] = v[:, KA:]
    nrm[0:128, :] = jnp.zeros((128, D), BF)
    with jax.named_scope("barrier"):
        pl.semaphore_wait(barrier, len(peers))

    def remote(src, dst, s, r, to):
        return pltpu.make_async_remote_copy(
            src_ref=src, dst_ref=dst, send_sem=s, recv_sem=r, device_id=to, device_id_type=MESH
        )

    def message(k):
        i = IDS[k]
        kind = k[0]
        if kind[0] == "X":
            d = k[1]
            if kind == "X1":
                src, dst = feature_columns(d, 0, 1280), wr.at[x]
            elif kind == "X2":
                off = 0 if d == 1 else 640
                src = feature_columns(2, off, 640)
                dst = relay.at[0 if d == 1 else 1]
            else:
                off = 0 if d == 1 else 640
                src = relay.at[0 if d == 1 else 1]
                dst = wr.at[xx(-d), :, pl.ds(off, 640)]
            return remote(src, dst, send.at[i], recv.at[i], dev(dx=d))
        h, d = k[1], k[2]
        if kind == "Ay":
            src, dst, to = own_a.at[h], wa.at[h, y, z], dev(dy=d)
        elif kind == "Ay2":
            cols = pl.ds(0 if d == 1 else KA // 2, KA // 2)
            src = dst = wa.at[h, yy(-d), z, :, cols]
            to = dev(dy=d)
        elif kind == "Az":
            step, rel = k[3], k[4]
            dst = wa.at[h, yy(rel), zz(-d * (step - 1))]
            src = own_a.at[h] if (step == 1 and rel == 0) else dst
            to = dev(dz=d)
        elif kind == "Bz":
            step = k[3]
            dst = wb.at[h, y, zz(-d * (step - 1))]
            src = own_b.at[h] if step == 1 else dst
            if step == 4:
                cols = pl.ds(0 if d == 1 else KB // 2, KB // 2)
                src = dst = wb.at[h, y, zz(-d * 3), :, cols]
            to = dev(dz=d)
        elif kind == "By":
            zr = k[3]
            dst = wb.at[h, y, zz(zr)]
            src = own_b.at[h] if zr == 0 else dst
            to = dev(dy=d)
        else:
            src = dst = wb.at[h, yy(-d), zz(k[3])]
            to = dev(dy=d)
        return remote(src, dst, send.at[i], recv.at[i], to)

    waited = set()
    queue = list(EVENTS)

    def take(k):
        if k not in waited:
            waited.add(k)
            message(k).wait_recv()

    def progress(until):
        while queue and queue[0][0] <= until:
            _, k = queue.pop(0)
            for q in MSGS[k][2]:
                take(q)
            message(k).start()

    def complete(h):
        for k in MSGS:
            if k[0][0] in "AB" and k[1] == h:
                take(k)

    extra_sends = []

    def extra(src, dst, to, slot):
        q = remote(src, dst, xsend.at[slot], xrecv.at[slot], to)
        q.start()
        extra_sends.append(q)
        return q

    halo_copy = extra(tok_in.at[pl.ds(TOK - 16, 16)], halo, nxt, 0)

    def norm_rows(v):
        wide = v.astype(F32)
        ms = jnp.mean(wide * wide, axis=1, keepdims=True)
        return wide * lax.rsqrt(ms + EPS) * gain[...].reshape(1, D)

    def piece_norm(part):
        tok_copies[part].wait()

        def step(i, carry):
            r = pl.multiple_of(part * 128 + i * 16, 16)
            nrm[pl.ds(128 + r, 16), :] = norm_rows(tok[pl.ds(r, 16), :]).astype(BF)
            return carry

        lax.fori_loop(0, 8, step, 0)

    def piece_halo():
        halo_copy.wait_recv()
        n = jnp.where(seq > 0, norm_rows(halo[...]), 0.0)
        nrm[112:128, :] = n.astype(BF)

    def piece_transpose(tb):
        def step(i, carry):
            k = pl.multiple_of(i * 128, 128)
            nt[pl.ds(k, 128), tb * 128 : (tb + 1) * 128] = nrm[
                tb * 128 : (tb + 1) * 128, pl.ds(k, 128)
            ].T
            return carry

        lax.fori_loop(0, D // 128, step, 0)

    def piece_state_weight():
        sw_copy.wait()

        def step(i, carry):
            r = pl.multiple_of(i * 128, 128)
            v = sw[pl.ds(r, 128), :, :].astype(F32)
            swd[pl.ds(r, 128), 0:128] = v[:, 0, :].astype(BF)
            swd[pl.ds(r, 128), 128:256] = v[:, 1, :].astype(BF)
            return carry

        lax.fori_loop(0, D // 128, step, 0)

    def piece_state(part):
        r = part * 176
        got = dot(nrm[112 + r : 112 + r + 176, :], swd[...])
        spf[r : r + 176, :] = got.astype(BF).astype(F32)

    def piece_state_conv():
        for q in range(4):
            for k in (0, 1):
                acc = jnp.zeros((128, 128), F32)
                for j in range(4):
                    first = q * 128 + 13 + j
                    w = cwst[j].astype(F32)[k : k + 1, :]
                    acc = acc + w * spf[first : first + 128, k * 128 : (k + 1) * 128]
                v = acc * lax.logistic(acc)
                if k == 0:
                    cb[q * 128 : (q + 1) * 128, :] = v.astype(BF)
                else:
                    ct[:, q * 128 : (q + 1) * 128] = v.T.astype(BF)

    def piece_delta():
        row = lax.broadcasted_iota(jnp.int32, (HEADS, TOK), 0)
        bias_col = rate_col = jnp.zeros((HEADS, TOK), F32)
        for h in range(HEADS):
            bias_col = jnp.where(row == h, bias[h], bias_col)
            rate_col = jnp.where(row == h, rate[h], rate_col)
        pre = dot(st[...], nt[:, 128:640]) + bias_col
        delta = jnp.maximum(pre, 0.0) + jnp.log1p(jnp.exp(-jnp.abs(pre)))
        run = -delta * rate_col
        lane = lax.broadcasted_iota(jnp.int32, (HEADS, TOK), 1) % SPAN
        k = 1
        while k < SPAN:
            run = run + jnp.where(lane >= k, pltpu.roll(run, k, 1), 0.0)
            k *= 2
        cum[...] = run
        ecum[...] = jnp.exp(run)
        tot0, tot1 = run[:, 255:256], run[:, 511:512]
        tailw[:, :SPAN] = jnp.exp(tot0 - run[:, :SPAN]) * delta[:, :SPAN]
        tailw[:, SPAN:] = jnp.exp(tot1 - run[:, SPAN:]) * delta[:, SPAN:]
        d01[0] = jnp.broadcast_to(jnp.exp(tot0), (HEADS, 128))
        d01[1] = jnp.broadcast_to(jnp.exp(tot1), (HEADS, 128))
        whole = jnp.broadcast_to(jnp.exp(tot0) * jnp.exp(tot1), (HEADS, 128))
        for h in range(HEADS):
            dec[8, h] = whole[h : h + 1, :]
            dec[z, h] = whole[h : h + 1, :]
        term[...] = jnp.zeros((128, TOK), F32)
        term[0:HEADS, :] = jnp.log(delta) - run
        for q in range(4):
            colt[q * 128 : (q + 1) * 128, :] = term[:, q * 128 : (q + 1) * 128].T
        for b in range(2):
            s = slice(b * SPAN, (b + 1) * SPAN)
            scores[b] = dot(cb[s, :], ct[:, s])

    dec_copies = []

    def piece_dec_send():
        for k in range(1, NZ):
            dec_copies.append(extra(dec.at[8], dec.at[z], dev(dz=k), k))

    def piece_dec_recv():
        for q in dec_copies:
            q.wait_recv()
        prod = dec[0]
        for k in range(1, NZ):
            prod = prod * dec[k]
        rowd[4] = prod
        rowd[y] = prod
        for k in range(1, NY):
            dec_copies.append(extra(rowd.at[4], rowd.at[y], dev(dy=k), 7 + k))

    def piece_mix(h):
        keep = lax.broadcasted_iota(jnp.int32, (128, 128), 1) >= lax.broadcasted_iota(
            jnp.int32, (128, 128), 0
        )
        for b in range(2):
            for s0 in range(2):
                r = b * SPAN + s0 * 128
                col = jnp.broadcast_to(colt[r : r + 128, h : h + 1], (128, 128))
                for t0 in range(2):
                    sl = (slice(s0 * 128, s0 * 128 + 128), slice(t0 * 128, t0 * 128 + 128))
                    if t0 < s0:
                        mix[(h, b) + sl] = jnp.zeros((128, 128), BF)
                        continue
                    q = b * SPAN + t0 * 128
                    arg = col + cum[h : h + 1, q : q + 128]
                    if s0 == t0:
                        arg = jnp.where(keep, arg, -jnp.inf)
                    mix[(h, b) + sl] = (scores[(b,) + sl] * jnp.exp(arg)).astype(BF)

    def product(h, r, first, width):
        la = wa[h, r].reshape(NZ * 40, KA)
        lb = wb[h, r].reshape(NZ * 40, KB)
        cols = slice(first, first + width)
        p0s[:, :width] = dot(la, nt[0:512, cols]) + dot(lb, nt[512:1280, cols])
        p1s[:, :width] = dot(la, nt[1280:1792, cols]) + dot(lb, nt[1792:2560, cols])

    def piece_inner(r):
        product(0, r, 0, 640)
        for i in range(NZ):
            v = p0s[40 * i : 40 * i + 20, :] + p1s[40 * i + 20 : 40 * i + 40, :]
            inn[r, 20 * i : 20 * i + 20, :] = v.astype(BF).astype(F32)

    def piece_gate(r):
        product(1, r, 128, 512)
        for i in range(NZ):
            v = p0s[40 * i : 40 * i + 20, :512] + p1s[40 * i + 20 : 40 * i + 40, :512]
            gat[r, 20 * i : 20 * i + 20, :] = v.astype(BF).astype(F32)

    def piece_conv(r):
        def step(i, carry):
            q = pl.multiple_of(i * 32, 32)
            row = pl.multiple_of(r * 160 + q, 32)
            v = inn[r, pl.ds(q, 32), :]
            w = cwin[pl.ds(row, 32), :]
            acc = w[:, 3:4] * v[:, 128:]
            for j in range(3):
                acc = acc + w[:, j : j + 1] * pltpu.roll(v, 3 - j, 1)[:, 128:]
            vt[pl.ds(row, 32), :] = (acc * lax.logistic(acc)).astype(BF)
            return carry

        lax.fori_loop(0, 5, step, 0)

    def head_rows(h):
        return pl.ds(pl.multiple_of(h * 64, 64), 64)

    def piece_update():
        def weigh(h, carry):
            vw[head_rows(h), :] = (vt[head_rows(h), :].astype(F32) * tailw[pl.ds(h, 1), :]).astype(BF)
            return carry

        lax.fori_loop(0, HEADS, weigh, 0)
        for b in range(2):
            s = slice(b * SPAN, (b + 1) * SPAN)
            u[b] = dot(vw[:, s], cb[s, :])

        def total(h, carry):
            v = u[0, head_rows(h), :] * d01[1, pl.ds(h, 1), :] + u[1, head_rows(h), :]
            for j in range(NZ):
                cs[j, h] = v[8 * j : 8 * j + 8, :].astype(BF)
            return carry

        lax.fori_loop(0, HEADS, total, 0)
        cr[z] = cs[z]

    carry1, carry2, carry3 = [], [], []

    def piece_carry1():
        for k in range(1, NZ):
            carry1.append(extra(cs.at[zz(k)], cr.at[z], dev(dz=k), 10 + k))

    def piece_carry2():
        for q in carry1:
            q.wait_recv()
        run = jnp.zeros((HEADS, 8, 128), F32)
        for k in range(NZ):
            prefix[k] = run
            run = run * dec[k] + cr[k].astype(F32)
        tt[4] = run
        tt[y] = run
        for k in range(1, NY):
            carry2.append(extra(tt.at[4], tt.at[y], dev(dy=k), 17 + k))

    def piece_carry3():
        for q in carry2 + dec_copies[7:]:
            q.wait_recv()
        r = jnp.zeros((HEADS, 8, 128), F32)
        for k in range(NY - 1):
            r = jnp.where(y > k, r * rowd[k] + tt[k], r)
        for k in range(NZ):
            co[k] = (prefix[k] + r).astype(BF)
            r = r * dec[k]
        ci[z] = co[z]
        for k in range(1, NZ):
            carry3.append(extra(co.at[zz(k)], ci.at[z], dev(dz=k), 20 + k))

    def piece_carry4():
        for q in carry3:
            q.wait_recv()

        def step(h, carry):
            v = jnp.concatenate([ci[j, h].astype(F32) for j in range(NZ)], axis=0)
            sbf[0, head_rows(h), :] = v.astype(BF)
            sbf[1, head_rows(h), :] = (v * d01[0, pl.ds(h, 1), :] + u[0, head_rows(h), :]).astype(BF)
            return carry

        lax.fori_loop(0, HEADS, step, 0)

    def piece_intra(b):
        s = slice(b * SPAN, (b + 1) * SPAN)

        def step(h, carry):
            v = vt[head_rows(h), s]
            yv[head_rows(h), s] = dot(v, mix[h, b]) + skip[h] * v.astype(F32)
            return carry

        lax.fori_loop(0, HEADS, step, 0)

    def piece_inter(b):
        s = slice(b * SPAN, (b + 1) * SPAN)

        def step(h, carry):
            got = dot(sbf[b, head_rows(h), :], ct[:, s])
            yv[head_rows(h), s] = yv[head_rows(h), s] + ecum[pl.ds(h, 1), s] * got
            return carry

        lax.fori_loop(0, HEADS, step, 0)

    pair_copies, sq_copies = [], []

    def piece_gated(b):
        s = slice(b * SPAN, (b + 1) * SPAN)
        total = jnp.zeros((8, SPAN), F32)
        for r in range(NY):

            def step(i, total):
                q = pl.multiple_of(i * 32, 32)
                row = pl.multiple_of(r * 160 + q, 32)
                g = gat[r, pl.ds(q, 32), s]
                v = yv[pl.ds(row, 32), s] * (g * lax.logistic(g))
                for e in range(4):
                    w = v[8 * e : 8 * e + 8, :]
                    total = total + w * w
                scb[c, pl.ds(row, 32), s] = (v * og[pl.ds(row, 32), 0:1]).astype(BF)
                return total

            total = lax.fori_loop(0, 5, step, total)
        sq[8, :, s] = total
        own = scb.at[c, :, pl.ds(b * SPAN, SPAN)]
        pair_copies.append(extra(own, own, dev(dc=1), 28 + b))

    def piece_squares():
        sq[grp] = sq[8]
        for k in range(1, 8):
            sq_copies.append(extra(sq.at[8], sq.at[grp], dev(dx=k // 2, dc=k % 2), 29 + k))

    def project(dx, half):
        s = slice(half * SPAN, (half + 1) * SPAN)
        p = xx(dx)
        return dot(wr[p, :, 0:CH], scb[0, :, s]) + dot(wr[p, :, CH : 2 * CH], scb[1, :, s])

    def piece_gains():
        term[...] = jnp.zeros((128, TOK), F32)
        for q in range(CH // 128):
            cols = slice(q * 128, q * 128 + 128)
            term[0:4, 0:128] = cw_in[:, cols].astype(F32)
            cwin[cols, :] = term[:, 0:128].T
            og[cols, :] = jnp.broadcast_to(og_in[cols].reshape(1, 128), (128, 128)).T

    def piece_name(piece):
        inside = getattr(piece, "func", piece)
        return inside.__name__ + "".join(f"#i={a}" for a in getattr(piece, "args", ()))

    def call(piece, *args):
        with jax.named_scope(piece.__name__ + "".join(f"#i={a}" for a in args)):
            return piece(*args)

    clock = 0.5
    progress(clock)
    front = [(functools.partial(piece_norm, i), 0.5) for i in range(4)]
    front += [(piece_halo, 0.1), (piece_gains, 0.4)]
    front += [(functools.partial(piece_transpose, i), 0.5) for i in range(5)]
    front += [(piece_state_weight, 1.0)]
    front += [(functools.partial(piece_state, i), 0.3) for i in range(3)]
    front += [(piece_state_conv, 0.3), (piece_delta, 0.6), (piece_dec_send, 0.1)]
    front += [(functools.partial(piece_mix, i), 0.25) for i in range(HEADS)]
    front += [(piece_dec_recv, 0.1)]
    for piece, cost in front:
        with jax.named_scope(piece_name(piece)):
            piece()
        clock += cost
        progress(clock)
    progress(HALF_DONE[0])
    clock = HALF_DONE[0]
    call(complete, 0)
    middle = []
    for i in range(NY):
        middle += [(functools.partial(piece_inner, i), 1.0), (functools.partial(piece_conv, i), 0.4)]
    middle += [(piece_update, 0.6), (piece_carry1, 0.1)]
    middle += [(functools.partial(piece_intra, i), 0.8) for i in range(2)]
    for piece, cost in middle:
        with jax.named_scope(piece_name(piece)):
            piece()
        clock += cost
        progress(clock)
    clock += 3.0
    progress(clock)
    call(piece_carry2)
    clock += 4.0
    progress(clock)
    call(piece_carry3)
    clock += 5.0
    progress(clock)
    call(piece_carry4)
    for i in range(2):
        call(piece_inter, i)
        clock += 0.4
        progress(clock)
    progress(1e9)
    call(complete, 1)
    for i in range(NY):
        call(piece_gate, i)
    for i in range(2):
        call(piece_gated, i)
    call(piece_squares)
    with jax.named_scope("wait_weights"):
        own_out.wait()
        for k in (("X1", 1), ("X1", -1), ("X2f", 1), ("X2f", -1)):
            take(k)
    with jax.named_scope("wait_pair"):
        for q in pair_copies:
            q.wait_recv()
    far = []
    for half, d in ((0, 1), (1, -1)):
        rs_out[half] = call(project, 2, half).astype(BF)
        far.append(extra(rs_out.at[half], rs_in1.at[half], dev(dx=d), 40 + half))
    near = []
    for i, d in enumerate((1, -1)):
        direct = 1 if d == 1 else 0
        rs2_out[i, direct] = call(project, d, direct).astype(BF)
        near.append(extra(rs2_out.at[i, direct], rs2_in.at[i, direct], dev(dx=d), 42 + 2 * i))
    for i, d in enumerate((1, -1)):
        relayed = 0 if d == 1 else 1
        v = call(project, d, relayed)
        with jax.named_scope("wait_far"):
            far[relayed].wait_recv()
        rs2_out[i, relayed] = (v + rs_in1[relayed].astype(F32)).astype(BF)
        near.append(extra(rs2_out.at[i, relayed], rs2_in.at[i, relayed], dev(dx=d), 43 + 2 * i))
    for half in range(2):
        own_p[half] = call(project, 0, half)
    for q in sq_copies:
        q.wait_recv()
    total = sq[0]
    for k in range(1, 8):
        total = total + sq[k]
    total = jnp.sum(total, axis=0, keepdims=True)
    scale = lax.rsqrt(total / (8 * CH) + EPS)
    with jax.named_scope("wait_near"):
        for q in near:
            q.wait_recv()
    for half in range(2):
        v = own_p[half] + rs2_in[0, half].astype(F32) + rs2_in[1, half].astype(F32)
        s = slice(half * SPAN, (half + 1) * SPAN)
        out[:, s] = (v * scale[:, s]).astype(BF)
    with jax.named_scope("wait_sends"):
        for k in MSGS:
            message(k).wait_send()
    for q in extra_sends:
        q.wait_send()


def run(*args):
    vm = pl.BlockSpec(memory_space=pltpu.VMEM)
    specs = [vm] * 12
    for i in (5, 6, 7):
        specs[i] = pl.BlockSpec(memory_space=pltpu.SMEM)
    for i in (0, 3, 11):
        specs[i] = pl.BlockSpec(memory_space=pl.ANY)
    V = pltpu.VMEM
    scratch = [
        V((TOK, D), BF),
        V((2, 40, KA), BF),
        V((2, 40, KB), BF),
        V((2, 40, D // 2), F32),
        V((D, 2, 128), BF),
        V((D, 256), BF),
        V((CH, 128), F32),
        V((CH, 128), F32),
        V((2, NY, NZ, 40, KA), BF),
        V((2, NY, NZ, 40, KB), BF),
        V((640, D), BF),
        V((D, 640), BF),
        V((528, 256), F32),
        V((TOK, 128), BF),
        V((128, TOK), BF),
        V((9, HEADS, 1, 128), F32),
        V((HEADS, TOK), F32),
        V((HEADS, TOK), F32),
        V((HEADS, TOK), F32),
        V((2, HEADS, 128), F32),
        V((2, SPAN, SPAN), F32),
        V((HEADS, 2, SPAN, SPAN), BF),
        V((128, TOK), F32),
        V((TOK, 128), F32),
        V((320, 640), F32),
        V((320, 640), F32),
        V((NY, 160, 640), F32),
        V((NY, 160, TOK), F32),
        V((CH, TOK), BF),
        V((CH, TOK), BF),
        V((2, CH, 128), F32),
        V((CH, TOK), F32),
        V((NZ, HEADS, 8, 128), BF),
        V((NZ, HEADS, 8, 128), BF),
        V((NZ, HEADS, 8, 128), BF),
        V((NZ, HEADS, 8, 128), BF),
        V((5, HEADS, 8, 128), F32),
        V((5, HEADS, 1, 128), F32),
        V((NZ, HEADS, 8, 128), F32),
        V((2, CH, 128), BF),
        V((2, CH, TOK), BF),
        V((NX, FEAT, 1280), BF),
        V((2, FEAT, 640), BF),
        V((9, 8, TOK), F32),
        V((2, FEAT, SPAN), BF),
        V((2, FEAT, SPAN), BF),
        V((2, 2, FEAT, SPAN), BF),
        V((2, 2, FEAT, SPAN), BF),
        V((2, FEAT, SPAN), F32),
        V((16, D), BF),
        pltpu.SemaphoreType.DMA((N_MSG,)),
        pltpu.SemaphoreType.DMA((N_MSG,)),
        pltpu.SemaphoreType.DMA((48,)),
        pltpu.SemaphoreType.DMA((48,)),
        pltpu.SemaphoreType.DMA((6,)),
    ]
    return pl.pallas_call(
        kernel,
        out_shape=jax.ShapeDtypeStruct((FEAT, TOK), BF),
        in_specs=specs,
        out_specs=vm,
        scratch_shapes=scratch,
        compiler_params=pltpu.CompilerParams(
            collective_id=0, has_side_effects=True, vmem_limit_bytes=64 * 2**20 - 65536
        ),
        name="layer",
    )(*args)


def body(
    tokens, norm_gain, inner_weight, state_weight, step_weight, step_bias, decay_rate,
    skip_scale, conv_inner, conv_state, out_gain, out_weight,
):
    return run(
        tokens, norm_gain, inner_weight.transpose(2, 1, 0), state_weight, step_weight.T,
        step_bias, decay_rate, skip_scale, conv_inner, conv_state, out_gain, out_weight.T,
    ).T


def solution(mesh):
    return jax.shard_map(
        body,
        mesh=mesh,
        in_specs=(
            P("seq", None), P(), P(None, None, ("grp", "seq")), P(), P(None, "grp"), P("grp"),
            P("grp"), P("grp"), P(None, "grp"), P(), P("grp"), P(None, "grp"),
        ),
        out_specs=P("seq", "grp"),
        check_vma=False,
    )
```

```python
import functools

import jax
import jax.numpy as jnp
from jax import lax
from jax.experimental import pallas as pl
from jax.experimental.pallas import tpu as pltpu
from jax.sharding import PartitionSpec as P

MESH = pl.DeviceIdType.MESH
BF = jnp.bfloat16
F32 = jnp.float32
EPS = 1e-05

TOK = 512
D = 2560
CH = 640
HEADS = 10
SPAN = 256
KA, KB = 512, 768
FEAT = 320
NY, NZ, NX = 4, 8, 4


def dot(a, b):
    return jnp.dot(a, b, preferred_element_type=F32)


def half_messages(h):
    m = {}
    for d in (1, -1):
        m["Ay", h, d] = (("y", d), 0.88, [])
        m["Ay2", h, d] = (("y", d), 0.44, [("Ay", h, d)])
        for k in range(1, 5):
            rels = (0, -1, 1, 2) if k < 4 else ((0, -1) if d == 1 else (1, 2))
            for rel in rels:
                if k > 1:
                    dep = [("Az", h, d, k - 1, rel)]
                else:
                    dep = {
                        0: [],
                        -1: [("Ay", h, 1)],
                        1: [("Ay", h, -1)],
                        2: [("Ay2", h, 1), ("Ay2", h, -1)],
                    }[rel]
                m["Az", h, d, k, rel] = (("z", d), 0.88, dep)
            dep = [("Bz", h, d, k - 1)] if k > 1 else []
            m["Bz", h, d, k] = (("z", d), 1.32 if k < 4 else 0.66, dep)
        for zr in range(-3, 5):
            if zr == 0:
                dep = []
            elif zr == 4:
                dep = [("Bz", h, 1, 4), ("Bz", h, -1, 4)]
            else:
                dep = [("Bz", h, 1, -zr)] if zr < 0 else [("Bz", h, -1, zr)]
            m["By", h, d, zr] = (("y", d), 1.32, dep)
            if (zr <= 0) == (d == 1):
                m["By2", h, d, zr] = (("y", d), 1.32, [("By", h, d, zr)])
    return m


def row_of(k):
    kind = k[0]
    if kind == "Bz":
        return 0
    if kind in ("Ay", "By"):
        return -k[2]
    return k[4] if kind == "Az" else 2


SLOWER = 1.12
LATENCY = 2.4
AHEAD = (1.5, 0.8)
GATE_FROM = 4.0
RELS = (0, -1, 1, 2)


def build_messages():
    msgs = {}
    for d in (1, -1):
        msgs["X2", d] = (("x", d), 8.8, [])
        msgs["X1", d] = (("x", d), 17.6, [])
        msgs["X2f", d] = (("x", d), 8.8, [("X2", d)])
    for h in (0, 1):
        msgs.update(half_messages(h))
    return msgs


def build_pieces():
    p = {}

    def add(name, cost, after=(), rows=(), sends=(), delay=0.0):
        p[name] = (cost, list(after), list(rows), list(sends), delay)

    z_swap = [(("z", 1), 2.5), (("z", -1), 2.5)]
    y_swap = [(("y", 1), 0.9), (("y", -1), 0.9)]
    add(("carry4",), 0.5, [("carry3",)])
    add(("carry3",), 0.5, [("carry2",), ("dec_recv",)], (), z_swap, 2.5)
    add(("carry2",), 0.4, [("carry1",), ("dec_recv",)], (), y_swap, 2.6)
    add(("carry1",), 0.1, [("update",)], (), z_swap, 2.5)
    convs = [("conv", rel) for rel in RELS]
    add(("update",), 0.5, convs + [("delta",), ("state_conv",)])
    ready = [("transpose", i) for i in range(5)]
    for rel in RELS:
        add(("conv", rel), 0.6, [("inner", rel, 0), ("inner", rel, 1), ("gains",)])
        add(("inner", rel, 0), 0.9, ready, [(0, rel)])
        add(("inner", rel, 1), 0.65, ready, [(0, rel)])
    for i in range(4):
        add(("norm", i), 0.56)
    add(("halo",), 0.3, [("norm", 3)], (), (), 0.0)
    for i in range(5):
        add(("transpose", i), 0.42, [("halo",)])
    add(("gains",), 0.2, [("norm", 3)])
    for i in range(4):
        add(("state_weight", i), 0.48, ready)
    for i in range(3):
        add(("state", i), 0.6, [("state_weight", e) for e in range(4)])
    add(("state_conv",), 0.4, [("state", i) for i in range(3)])
    add(("delta",), 1.2, ready + [("gains",)])
    add(("scores",), 0.3, [("state_conv",)])
    add(("dec_send",), 0.1, [("delta",)], (), (), 5.0)
    for i in range(HEADS):
        add(("mix", i), 0.16, [("delta",), ("scores",)])
    add(("dec_recv",), 0.2, [("dec_send",)], (), (), 3.5)
    mixes = [("mix", i) for i in range(HEADS)]
    for rel in RELS:
        add(("gated", rel), 0.12, [("inter", rel), ("gate", rel, 0), ("gate", rel, 1)])
        add(("inter", rel), 0.2, [("carry4",), ("intra", 0), ("intra", 1)])
    for i in range(2):
        add(("intra", i), 0.9, mixes + convs)
    for rel in RELS:
        add(("gate", rel, 0), 0.53, ready, [(1, rel)])
        add(("gate", rel, 1), 0.53, ready, [(1, rel)])
    return p


def build_program():
    msgs, pieces = build_messages(), build_pieces()
    order = {k: i for i, k in enumerate(msgs)}

    def rank(k):
        if k[0][0] == "X":
            return (0, 9 if k[0] == "X1" else 0, order[k])
        if k[0] in ("Bz", "Ay"):
            p = 0
        elif k[0] == "Ay2":
            p = 0.5
        elif k[0] == "Az":
            p = 1 + k[3] + (0, 0.2, 0.4)[abs(k[4])]
        else:
            p = 1 + abs(k[3]) + (2 if k[0] == "By2" else 0)
        return (k[1], p, order[k])

    arrived, done, free, program = {}, {}, {}, []
    todo = sorted(msgs, key=rank)
    work = list(pieces)
    now = 0.0
    rows = {}
    for k in msgs:
        if k[0][0] in "AB":
            rows.setdefault((k[1], row_of(k)), []).append(k)
    while todo or work:
        moved = True
        while moved:
            moved = False
            for k in todo:
                link, dur, deps = msgs[k]
                later = k[0][0] != "X" and k[1] == 1
                if free.get(link, 0.0) > now + AHEAD[later] or (later and now < GATE_FROM):
                    continue
                if any(arrived.get(q, 1e9) > now for q in deps):
                    continue
                start = max(now, free.get(link, 0.0))
                free[link] = start + dur * SLOWER
                arrived[k] = free[link] + LATENCY
                program.append(("issue", k))
                todo.remove(k)
                now += 0.02
                moved = True
                break
        for name in work:
            cost, after, need, sends, delay = pieces[name]
            if any(done.get(q, 1e9) > now for q in after):
                continue
            if any(arrived.get(k, 1e9) > now for e in need for k in rows[e]):
                continue
            program.append(("piece", name))
            work.remove(name)
            now += cost
            end = now
            for link, dur in sends:
                free[link] = max(now, free.get(link, 0.0)) + dur * SLOWER
                end = max(end, free[link])
            done[name] = end + delay
            break
        else:
            now += 0.05
    return msgs, program, done, arrived


MSGS, PROGRAM, DONE, ARRIVED = build_program()
IDS = {k: i for i, k in enumerate(MSGS)}
N_MSG = len(MSGS)


def kernel(
    tok_in, gain, own_in, sw_in, st, bias, rate, skip, cw_in, cwst, og_in, ow,
    out,
    tok, own_a, own_b, own_f, sw, swd, cwin, og, wa, wb, nrm, nt, spf, cb, ct, dec, cum, ecum, tailw, d01, scores, mix, term, colt,
    p0s, p1s, inn, gat, vt, vw, u, yv, cs, cr, co, ci, tt, rowd, prefix,
    sbf, scb, wr, relay, sq, rs_out, rs_in1, rs2_out, rs2_in, keep, own_p,
    halo, send, recv, xsend, xrecv, lsem,
):
    seq = lax.axis_index("seq")
    grp = lax.axis_index("grp")
    y, z = seq // NZ, lax.rem(seq, NZ)
    x, c = grp // 2, lax.rem(grp, 2)

    def yy(d):
        return lax.rem(y + d + NY, NY)

    def zz(d):
        return lax.rem(z + d + NZ, NZ)

    def xx(d):
        return lax.rem(x + d + NX, NX)

    def dev(dy=0, dz=0, dx=0, dc=0):
        return (yy(dy) * NZ + zz(dz), xx(dx) * 2 + lax.rem(c + dc, 2))

    nxt = (lax.rem(seq + 1, NY * NZ), grp)
    prv = (lax.rem(seq + NY * NZ - 1, NY * NZ), grp)

    barrier = pltpu.get_barrier_semaphore()
    peers = [nxt, prv]
    peers += [dev(dz=k) for k in range(1, NZ)]
    peers += [dev(dy=k) for k in range(1, NY)]
    peers += [dev(dx=k // 2, dc=k % 2) for k in range(1, 8)]
    for p in peers:
        pl.semaphore_signal(barrier, inc=1, device_id=p, device_id_type=MESH)

    def feature_columns(d, first, count):
        return ow.at[:, pl.ds(pl.multiple_of(xx(d) * 1280 + first, 128), count)]

    tok_copies = []
    for q in range(4):
        part = pl.ds(q * 128, 128)
        tok_copies.append(pltpu.make_async_copy(tok_in.at[part], tok.at[part], lsem.at[q]))
        tok_copies[q].start()
    sw_copy = pltpu.make_async_copy(sw_in, sw, lsem.at[4])
    sw_copy.start()
    own_out = pltpu.make_async_copy(feature_columns(0, 0, 1280), wr.at[x], lsem.at[5])
    own_out.start()
    for r in range(20):
        v = own_in[r].astype(F32)
        for h in (0, 1):
            for part in (0, 1):
                own_f[h, 20 * part + r : 20 * part + r + 1, :] = v[
                    h : h + 1, part * (D // 2) : (part + 1) * (D // 2)
                ]
    for h in (0, 1):
        v = own_f[h].astype(BF)
        own_a[h] = v[:, :KA]
        own_b[h] = v[:, KA:]
        wa[h, y, z] = v[:, :KA]
        wb[h, y, z] = v[:, KA:]
    nrm[0:128, :] = jnp.zeros((128, D), BF)
    with jax.named_scope("barrier"):
        pl.semaphore_wait(barrier, len(peers))

    def remote(src, dst, s, r, to):
        return pltpu.make_async_remote_copy(
            src_ref=src, dst_ref=dst, send_sem=s, recv_sem=r, device_id=to, device_id_type=MESH
        )

    def message(k):
        i = IDS[k]
        kind = k[0]
        if kind[0] == "X":
            d = k[1]
            if kind == "X1":
                src, dst = feature_columns(d, 0, 1280), wr.at[x]
            elif kind == "X2":
                off = 0 if d == 1 else 640
                src = feature_columns(2, off, 640)
                dst = relay.at[0 if d == 1 else 1]
            else:
                off = 0 if d == 1 else 640
                src = relay.at[0 if d == 1 else 1]
                dst = wr.at[xx(-d), :, pl.ds(off, 640)]
            return remote(src, dst, send.at[i], recv.at[i], dev(dx=d))
        h, d = k[1], k[2]
        if kind == "Ay":
            src, dst, to = own_a.at[h], wa.at[h, y, z], dev(dy=d)
        elif kind == "Ay2":
            cols = pl.ds(0 if d == 1 else KA // 2, KA // 2)
            src = dst = wa.at[h, yy(-d), z, :, cols]
            to = dev(dy=d)
        elif kind == "Az":
            step, rel = k[3], k[4]
            dst = wa.at[h, yy(rel), zz(-d * (step - 1))]
            src = own_a.at[h] if (step == 1 and rel == 0) else dst
            to = dev(dz=d)
        elif kind == "Bz":
            step = k[3]
            dst = wb.at[h, y, zz(-d * (step - 1))]
            src = own_b.at[h] if step == 1 else dst
            if step == 4:
                cols = pl.ds(0 if d == 1 else KB // 2, KB // 2)
                src = dst = wb.at[h, y, zz(-d * 3), :, cols]
            to = dev(dz=d)
        elif kind == "By":
            zr = k[3]
            dst = wb.at[h, y, zz(zr)]
            src = own_b.at[h] if zr == 0 else dst
            to = dev(dy=d)
        else:
            src = dst = wb.at[h, yy(-d), zz(k[3])]
            to = dev(dy=d)
        return remote(src, dst, send.at[i], recv.at[i], to)

    waited = set()
    def take(k):
        if k not in waited:
            waited.add(k)
            message(k).wait_recv()

    def issue(k):
        for q in MSGS[k][2]:
            take(q)
        message(k).start()

    def complete(h, rel):
        for k in MSGS:
            if k[0][0] in "AB" and k[1] == h and row_of(k) == rel:
                take(k)

    extra_sends = []

    def extra(src, dst, to, slot):
        q = remote(src, dst, xsend.at[slot], xrecv.at[slot], to)
        q.start()
        extra_sends.append(q)
        return q

    halo_copy = extra(tok_in.at[pl.ds(TOK - 16, 16)], halo, nxt, 0)

    def norm_rows(v):
        wide = v.astype(F32)
        ms = jnp.mean(wide * wide, axis=1, keepdims=True)
        return wide * lax.rsqrt(ms + EPS) * gain[...].reshape(1, D)

    def piece_norm(part):
        tok_copies[part].wait()

        def step(i, carry):
            r = pl.multiple_of(part * 128 + i * 16, 16)
            nrm[pl.ds(128 + r, 16), :] = norm_rows(tok[pl.ds(r, 16), :]).astype(BF)
            return carry

        lax.fori_loop(0, 8, step, 0, unroll=2)

    def piece_halo():
        halo_copy.wait_recv()
        n = jnp.where(seq > 0, norm_rows(halo[...]), 0.0)
        nrm[112:128, :] = n.astype(BF)

    def piece_transpose(tb):
        def step(i, carry):
            k = pl.multiple_of(i * 128, 128)
            nt[pl.ds(k, 128), tb * 128 : (tb + 1) * 128] = nrm[
                tb * 128 : (tb + 1) * 128, pl.ds(k, 128)
            ].T
            return carry

        lax.fori_loop(0, D // 128, step, 0, unroll=5)

    def piece_state_weight(part):
        if part == 0:
            sw_copy.wait()

        def step(i, carry):
            r = pl.multiple_of(i * 128 + part * 640, 128)
            v = sw[pl.ds(r, 128), :, :].astype(F32)
            swd[pl.ds(r, 128), 0:128] = v[:, 0, :].astype(BF)
            swd[pl.ds(r, 128), 128:256] = v[:, 1, :].astype(BF)
            return carry

        lax.fori_loop(0, 5, step, 0)

    def piece_state(part):
        r = part * 176
        got = dot(nrm[112 + r : 112 + r + 176, :], swd[...])
        spf[r : r + 176, :] = got.astype(BF).astype(F32)

    def piece_state_conv():
        for q in range(4):
            for k in (0, 1):
                acc = jnp.zeros((128, 128), F32)
                for j in range(4):
                    first = q * 128 + 13 + j
                    w = cwst[j].astype(F32)[k : k + 1, :]
                    acc = acc + w * spf[first : first + 128, k * 128 : (k + 1) * 128]
                v = acc * lax.logistic(acc)
                if k == 0:
                    cb[q * 128 : (q + 1) * 128, :] = v.astype(BF)
                else:
                    ct[:, q * 128 : (q + 1) * 128] = v.T.astype(BF)

    def piece_delta():
        row = lax.broadcasted_iota(jnp.int32, (HEADS, TOK), 0)
        bias_col = rate_col = jnp.zeros((HEADS, TOK), F32)
        for h in range(HEADS):
            bias_col = jnp.where(row == h, bias[h], bias_col)
            rate_col = jnp.where(row == h, rate[h], rate_col)
        pre = dot(st[...], nt[:, 128:640]) + bias_col
        delta = jnp.maximum(pre, 0.0) + jnp.log1p(jnp.exp(-jnp.abs(pre)))
        run = -delta * rate_col
        lane = lax.broadcasted_iota(jnp.int32, (HEADS, TOK), 1) % SPAN
        k = 1
        while k < SPAN:
            run = run + jnp.where(lane >= k, pltpu.roll(run, k, 1), 0.0)
            k *= 2
        cum[...] = run
        ecum[...] = jnp.exp(run)
        tot0, tot1 = run[:, 255:256], run[:, 511:512]
        tailw[:, :SPAN] = jnp.exp(tot0 - run[:, :SPAN]) * delta[:, :SPAN]
        tailw[:, SPAN:] = jnp.exp(tot1 - run[:, SPAN:]) * delta[:, SPAN:]
        d01[0] = jnp.broadcast_to(jnp.exp(tot0), (HEADS, 128))
        d01[1] = jnp.broadcast_to(jnp.exp(tot1), (HEADS, 128))
        whole = jnp.broadcast_to(jnp.exp(tot0) * jnp.exp(tot1), (HEADS, 128))
        for h in range(HEADS):
            dec[8, h] = whole[h : h + 1, :]
            dec[z, h] = whole[h : h + 1, :]
        term[...] = jnp.zeros((128, TOK), F32)
        term[0:HEADS, :] = jnp.log(delta) - run
        for q in range(4):
            colt[q * 128 : (q + 1) * 128, :] = term[:, q * 128 : (q + 1) * 128].T

    def piece_scores():
        for b in range(2):
            s = slice(b * SPAN, (b + 1) * SPAN)
            scores[b] = dot(cb[s, :], ct[:, s])

    dec_copies = []

    def piece_dec_send():
        for k in range(1, NZ):
            dec_copies.append(extra(dec.at[8], dec.at[z], dev(dz=k), k))

    def piece_dec_recv():
        for q in dec_copies:
            q.wait_recv()
        prod = dec[0]
        for k in range(1, NZ):
            prod = prod * dec[k]
        rowd[4] = prod
        rowd[y] = prod
        for k in range(1, NY):
            dec_copies.append(extra(rowd.at[4], rowd.at[y], dev(dy=k), 7 + k))

    def piece_mix(h):
        keep = lax.broadcasted_iota(jnp.int32, (128, 128), 1) >= lax.broadcasted_iota(
            jnp.int32, (128, 128), 0
        )
        for b in range(2):
            for s0 in range(2):
                r = b * SPAN + s0 * 128
                col = jnp.broadcast_to(colt[r : r + 128, h : h + 1], (128, 128))
                for t0 in range(2):
                    sl = (slice(s0 * 128, s0 * 128 + 128), slice(t0 * 128, t0 * 128 + 128))
                    if t0 < s0:
                        mix[(h, b) + sl] = jnp.zeros((128, 128), BF)
                        continue
                    q = b * SPAN + t0 * 128
                    arg = col + cum[h : h + 1, q : q + 128]
                    if s0 == t0:
                        arg = jnp.where(keep, arg, -jnp.inf)
                    mix[(h, b) + sl] = (scores[(b,) + sl] * jnp.exp(arg)).astype(BF)

    def product(h, r, first, cols):
        la = wa[h, r].reshape(NZ * 40, KA)
        lb = wb[h, r].reshape(NZ * 40, KB)
        n = slice(first + cols.start, first + cols.stop)
        p0s[:, cols] = dot(la, nt[0:512, n]) + dot(lb, nt[512:1280, n])
        p1s[:, cols] = dot(la, nt[1280:1792, n]) + dot(lb, nt[1792:2560, n])

    def piece_inner(r, part):
        cols = (slice(0, 384), slice(384, 640))[part]
        product(0, r, 0, cols)
        for i in range(NZ):
            v = p0s[40 * i : 40 * i + 20, cols] + p1s[40 * i + 20 : 40 * i + 40, cols]
            inn[r, 20 * i : 20 * i + 20, cols] = v.astype(BF).astype(F32)

    def piece_gate(r, part):
        cols = slice(part * SPAN, (part + 1) * SPAN)
        product(1, r, 128, cols)
        for i in range(NZ):
            v = p0s[40 * i : 40 * i + 20, cols] + p1s[40 * i + 20 : 40 * i + 40, cols]
            gat[r, 20 * i : 20 * i + 20, cols] = v.astype(BF).astype(F32)

    def piece_conv(r):
        def step(i, carry):
            q = pl.multiple_of(i * 32, 32)
            row = pl.multiple_of(r * 160 + q, 32)
            v = inn[r, pl.ds(q, 32), :]
            w = cwin[pl.ds(row, 32), :]
            acc = w[:, 3:4] * v[:, 128:]
            for j in range(3):
                acc = acc + w[:, j : j + 1] * pltpu.roll(v, 3 - j, 1)[:, 128:]
            vt[pl.ds(row, 32), :] = (acc * lax.logistic(acc)).astype(BF)
            return carry

        lax.fori_loop(0, 5, step, 0, unroll=5)

    def head_rows(h):
        return pl.ds(pl.multiple_of(h * 64, 64), 64)

    def piece_update():
        def weigh(h, carry):
            vw[head_rows(h), :] = (vt[head_rows(h), :].astype(F32) * tailw[pl.ds(h, 1), :]).astype(BF)
            return carry

        lax.fori_loop(0, HEADS, weigh, 0, unroll=2)
        for b in range(2):
            s = slice(b * SPAN, (b + 1) * SPAN)
            u[b] = dot(vw[:, s], cb[s, :])

        def total(h, carry):
            v = u[0, head_rows(h), :] * d01[1, pl.ds(h, 1), :] + u[1, head_rows(h), :]
            for j in range(NZ):
                cs[j, h] = v[8 * j : 8 * j + 8, :].astype(BF)
            return carry

        lax.fori_loop(0, HEADS, total, 0, unroll=2)
        cr[z] = cs[z]

    carry1, carry2, carry3 = [], [], []

    def piece_carry1():
        for k in range(1, NZ):
            carry1.append(extra(cs.at[zz(k)], cr.at[z], dev(dz=k), 10 + k))

    def piece_carry2():
        for q in carry1:
            q.wait_recv()
        run = jnp.zeros((HEADS, 8, 128), F32)
        for k in range(NZ):
            prefix[k] = run
            run = run * dec[k] + cr[k].astype(F32)
        tt[4] = run.astype(BF)
        tt[y] = run.astype(BF)
        for k in range(1, NY):
            carry2.append(extra(tt.at[4], tt.at[y], dev(dy=k), 17 + k))

    def piece_carry3():
        for q in carry2 + dec_copies[7:]:
            q.wait_recv()
        r = jnp.zeros((HEADS, 8, 128), F32)
        for k in range(NY - 1):
            r = jnp.where(y > k, r * rowd[k] + tt[k].astype(F32), r)
        for k in range(NZ):
            co[k] = (prefix[k] + r).astype(BF)
            r = r * dec[k]
        ci[z] = co[z]
        for k in range(1, NZ):
            carry3.append(extra(co.at[zz(k)], ci.at[z], dev(dz=k), 20 + k))

    def piece_carry4():
        for q in carry3:
            q.wait_recv()

        def step(h, carry):
            v = jnp.concatenate([ci[j, h].astype(F32) for j in range(NZ)], axis=0)
            sbf[0, head_rows(h), :] = v.astype(BF)
            sbf[1, head_rows(h), :] = (v * d01[0, pl.ds(h, 1), :] + u[0, head_rows(h), :]).astype(BF)
            return carry

        lax.fori_loop(0, HEADS, step, 0)

    def piece_intra(b):
        s = slice(b * SPAN, (b + 1) * SPAN)

        def step(h, carry):
            v = vt[head_rows(h), s]
            yv[head_rows(h), s] = dot(v, mix[h, b]) + skip[h] * v.astype(F32)
            return carry

        lax.fori_loop(0, HEADS, step, 0, unroll=2)

    def piece_inter(r):
        rows = pl.ds(pl.multiple_of(r * 160, 160), 160)
        for b in range(2):
            s = slice(b * SPAN, (b + 1) * SPAN)
            p0s[0:160, s] = dot(sbf[b, rows, :], ct[:, s])

        def step(i, carry):
            q = pl.multiple_of(i * 32, 32)
            row = pl.ds(pl.multiple_of(r * 160 + q, 32), 32)
            e = ecum[pl.ds((5 * r + i) // 2, 1), :]
            yv[row, :] = yv[row, :] + e * p0s[pl.ds(q, 32), 0:TOK]
            return carry

        lax.fori_loop(0, 5, step, 0, unroll=5)

    pair_copies, sq_copies = [], []
    sq[8] = jnp.zeros((8, TOK), F32)

    def piece_gated(r, slot):
        def step(i, total):
            q = pl.multiple_of(i * 32, 32)
            row = pl.ds(pl.multiple_of(r * 160 + q, 32), 32)
            g = gat[r, pl.ds(q, 32), :]
            v = yv[row, :] * (g * lax.logistic(g))
            for e in range(4):
                w = v[8 * e : 8 * e + 8, :]
                total = total + w * w
            scb[c, row, :] = (v * og[row, 0:1]).astype(BF)
            return total

        sq[8] = lax.fori_loop(0, 5, step, sq[8], unroll=5)
        own = scb.at[c, pl.ds(pl.multiple_of(r * 160, 160), 160)]
        pair_copies.append(extra(own, own, dev(dc=1), 28 + slot))

    def piece_squares():
        sq[grp] = sq[8]
        for k in range(1, 8):
            sq_copies.append(extra(sq.at[8], sq.at[grp], dev(dx=k // 2, dc=k % 2), 31 + k))

    def project(dx, half):
        s = slice(half * SPAN, (half + 1) * SPAN)
        p = xx(dx)
        return dot(wr[p, :, 0:CH], scb[0, :, s]) + dot(wr[p, :, CH : 2 * CH], scb[1, :, s])

    def piece_gains():
        term[...] = jnp.zeros((128, TOK), F32)
        for q in range(CH // 128):
            cols = slice(q * 128, q * 128 + 128)
            term[0:4, 0:128] = cw_in[:, cols].astype(F32)
            cwin[cols, :] = term[:, 0:128].T
            og[cols, :] = jnp.broadcast_to(og_in[cols].reshape(1, 128), (128, 128)).T

    def call(piece, *args):
        with jax.named_scope(piece.__name__ + "".join(f"#i={a}" for a in args if isinstance(a, int))):
            return piece(*args)

    def inner_row(rel, part):
        complete(0, rel)
        piece_inner(yy(rel), part)

    def gate_row(rel, part):
        complete(1, rel)
        piece_gate(yy(rel), part)

    does = {
        "norm": piece_norm,
        "halo": piece_halo,
        "gains": piece_gains,
        "transpose": piece_transpose,
        "state_weight": piece_state_weight,
        "state": piece_state,
        "state_conv": piece_state_conv,
        "delta": piece_delta,
        "scores": piece_scores,
        "dec_send": piece_dec_send,
        "dec_recv": piece_dec_recv,
        "mix": piece_mix,
        "inner": inner_row,
        "conv": lambda rel: piece_conv(yy(rel)),
        "update": piece_update,
        "carry1": piece_carry1,
        "carry2": piece_carry2,
        "carry3": piece_carry3,
        "carry4": piece_carry4,
        "intra": piece_intra,
        "inter": lambda rel: piece_inter(yy(rel)),
        "gate": gate_row,
        "gated": lambda rel: piece_gated(yy(rel), rel + 1),
    }
    for what, k in PROGRAM:
        if what == "issue":
            issue(k)
        else:
            with jax.named_scope("#".join(str(e) for e in k)):
                does[k[0]](*k[1:])
    call(piece_squares)
    with jax.named_scope("wait_weights"):
        own_out.wait()
        for k in (("X1", 1), ("X1", -1), ("X2f", 1), ("X2f", -1)):
            take(k)
    with jax.named_scope("wait_pair"):
        for q in pair_copies:
            q.wait_recv()

    top, low = slice(0, 160), slice(160, 320)
    far, near = {}, []

    def send_far(half):
        got = call(project, 2, half)
        rs_out[half] = got.astype(BF)
        for i, d in enumerate((1, -1)):
            rows = pl.ds(160 * i, 160)
            far[half, d] = extra(
                rs_out.at[half, rows], rs_in1.at[half, rows], dev(dx=d), 40 + 2 * half + i
            )

    def send_direct(half):
        for i, d in enumerate((1, -1)):
            keep[i] = call(project, d, half)
            rows = low if d == 1 else top
            rs2_out[i, half, rows] = keep[i, rows].astype(BF)
            rows = pl.ds(160 * (1 - i), 160)
            part = (i, half, rows)
            near.append(extra(rs2_out.at[part], rs2_in.at[part], dev(dx=d), 44 + 4 * half + i))

    def send_relayed(half):
        for i, d in enumerate((1, -1)):
            with jax.named_scope("wait_far"):
                far[half, d].wait_recv()
            rows = top if d == 1 else low
            rs2_out[i, half, rows] = (keep[i, rows] + rs_in1[half, rows].astype(F32)).astype(BF)
            rows = pl.ds(160 * i, 160)
            part = (i, half, rows)
            near.append(extra(rs2_out.at[part], rs2_in.at[part], dev(dx=d), 46 + 4 * half + i))

    send_far(0)
    send_direct(0)
    send_far(1)
    send_relayed(0)
    send_direct(1)
    own_p[0] = call(project, 0, 0)
    send_relayed(1)
    own_p[1] = call(project, 0, 1)
    with jax.named_scope("wait_sq"):
        for q in sq_copies:
            q.wait_recv()
    total = sq[0]
    for k in range(1, 8):
        total = total + sq[k]
    total = jnp.sum(total, axis=0, keepdims=True)
    scale = lax.rsqrt(total / (8 * CH) + EPS)
    for half in range(2):
        with jax.named_scope("wait_near"):
            for q in near[4 * half : 4 * half + 4]:
                q.wait_recv()
        v = own_p[half] + rs2_in[0, half].astype(F32) + rs2_in[1, half].astype(F32)
        s = slice(half * SPAN, (half + 1) * SPAN)
        out[:, s] = (v * scale[:, s]).astype(BF)
    with jax.named_scope("wait_sends"):
        for k in MSGS:
            message(k).wait_send()
    for q in extra_sends:
        q.wait_send()


def run(*args):
    vm = pl.BlockSpec(memory_space=pltpu.VMEM)
    specs = [vm] * 12
    for i in (5, 6, 7):
        specs[i] = pl.BlockSpec(memory_space=pltpu.SMEM)
    for i in (0, 3, 11):
        specs[i] = pl.BlockSpec(memory_space=pl.ANY)
    V = pltpu.VMEM
    scratch = [
        V((TOK, D), BF),
        V((2, 40, KA), BF),
        V((2, 40, KB), BF),
        V((2, 40, D // 2), F32),
        V((D, 2, 128), BF),
        V((D, 256), BF),
        V((CH, 128), F32),
        V((CH, 128), F32),
        V((2, NY, NZ, 40, KA), BF),
        V((2, NY, NZ, 40, KB), BF),
        V((640, D), BF),
        V((D, 640), BF),
        V((528, 256), F32),
        V((TOK, 128), BF),
        V((128, TOK), BF),
        V((9, HEADS, 1, 128), F32),
        V((HEADS, TOK), F32),
        V((HEADS, TOK), F32),
        V((HEADS, TOK), F32),
        V((2, HEADS, 128), F32),
        V((2, SPAN, SPAN), F32),
        V((HEADS, 2, SPAN, SPAN), BF),
        V((128, TOK), F32),
        V((TOK, 128), F32),
        V((320, 640), F32),
        V((320, 640), F32),
        V((NY, 160, 640), F32),
        V((NY, 160, TOK), F32),
        V((CH, TOK), BF),
        V((CH, TOK), BF),
        V((2, CH, 128), F32),
        V((CH, TOK), F32),
        V((NZ, HEADS, 8, 128), BF),
        V((NZ, HEADS, 8, 128), BF),
        V((NZ, HEADS, 8, 128), BF),
        V((NZ, HEADS, 8, 128), BF),
        V((5, HEADS, 8, 128), BF),
        V((5, HEADS, 1, 128), F32),
        V((NZ, HEADS, 8, 128), F32),
        V((2, CH, 128), BF),
        V((2, CH, TOK), BF),
        V((NX, FEAT, 1280), BF),
        V((2, FEAT, 640), BF),
        V((9, 8, TOK), F32),
        V((2, FEAT, SPAN), BF),
        V((2, FEAT, SPAN), BF),
        V((2, 2, FEAT, SPAN), BF),
        V((2, 2, FEAT, SPAN), BF),
        V((2, FEAT, SPAN), F32),
        V((2, FEAT, SPAN), F32),
        V((16, D), BF),
        pltpu.SemaphoreType.DMA((N_MSG,)),
        pltpu.SemaphoreType.DMA((N_MSG,)),
        pltpu.SemaphoreType.DMA((52,)),
        pltpu.SemaphoreType.DMA((52,)),
        pltpu.SemaphoreType.DMA((6,)),
    ]
    return pl.pallas_call(
        kernel,
        out_shape=jax.ShapeDtypeStruct((FEAT, TOK), BF),
        in_specs=specs,
        out_specs=vm,
        scratch_shapes=scratch,
        compiler_params=pltpu.CompilerParams(
            collective_id=0, has_side_effects=True, vmem_limit_bytes=64 * 2**20 - 65536
        ),
        name="layer",
    )(*args)


def body(
    tokens, norm_gain, inner_weight, state_weight, step_weight, step_bias, decay_rate,
    skip_scale, conv_inner, conv_state, out_gain, out_weight,
):
    return run(
        tokens, norm_gain, inner_weight.transpose(2, 1, 0), state_weight, step_weight.T,
        step_bias, decay_rate, skip_scale, conv_inner, conv_state, out_gain, out_weight.T,
    ).T


def solution(mesh):
    return jax.shard_map(
        body,
        mesh=mesh,
        in_specs=(
            P("seq", None), P(), P(None, None, ("grp", "seq")), P(), P(None, "grp"), P("grp"),
            P("grp"), P("grp"), P(None, "grp"), P(), P("grp"), P(None, "grp"),
        ),
        out_specs=P("seq", "grp"),
        check_vma=False,
    )
```

```python
import functools

import jax
import jax.numpy as jnp
from jax import lax
from jax.experimental import pallas as pl
from jax.experimental.pallas import tpu as pltpu
from jax.sharding import PartitionSpec as P

MESH = pl.DeviceIdType.MESH
BF = jnp.bfloat16
F32 = jnp.float32
EPS = 1e-05

TOK = 512
D = 2560
CH = 640
HEADS = 10
SPAN = 256
KA, KB = 512, 768
FEAT = 320
NY, NZ, NX = 4, 8, 4


def dot(a, b):
    return jnp.dot(a, b, preferred_element_type=F32)


def half_messages(h):
    m = {}
    for d in (1, -1):
        m["Ay", h, d] = (("y", d), 0.88, [])
        m["Ay2", h, d] = (("y", d), 0.44, [("Ay", h, d)])
        for k in range(1, 5):
            rels = (0, -1, 1, 2) if k < 4 else ((0, -1) if d == 1 else (1, 2))
            for rel in rels:
                if k > 1:
                    dep = [("Az", h, d, k - 1, rel)]
                else:
                    dep = {
                        0: [],
                        -1: [("Ay", h, 1)],
                        1: [("Ay", h, -1)],
                        2: [("Ay2", h, 1), ("Ay2", h, -1)],
                    }[rel]
                m["Az", h, d, k, rel] = (("z", d), 0.88, dep)
            dep = [("Bz", h, d, k - 1)] if k > 1 else []
            m["Bz", h, d, k] = (("z", d), 1.32 if k < 4 else 0.66, dep)
        for zr in range(-3, 5):
            if zr == 0:
                dep = []
            elif zr == 4:
                dep = [("Bz", h, 1, 4), ("Bz", h, -1, 4)]
            else:
                dep = [("Bz", h, 1, -zr)] if zr < 0 else [("Bz", h, -1, zr)]
            m["By", h, d, zr] = (("y", d), 1.32, dep)
            if (zr <= 0) == (d == 1):
                m["By2", h, d, zr] = (("y", d), 1.32, [("By", h, d, zr)])
    return m


def row_of(k):
    kind = k[0]
    if kind == "Bz":
        return 0
    if kind in ("Ay", "By"):
        return -k[2]
    return k[4] if kind == "Az" else 2


SLOWER = 1.12
LATENCY = 2.4
AHEAD = (1.5, 0.8)
GATE_FROM = 4.0
RELS = (0, -1, 1, 2)
FAR_FIRST = (4, 3, 5, 2, 6, 1, 7)


def build_messages():
    msgs = {}
    for d in (1, -1):
        msgs["X2", d] = (("x", d), 8.8, [])
        msgs["X1", d] = (("x", d), 17.6, [])
        msgs["X2f", d] = (("x", d), 8.8, [("X2", d)])
    for h in (0, 1):
        msgs.update(half_messages(h))
    return msgs


def build_pieces():
    p = {}

    def add(name, cost, after=(), rows=(), sends=(), delay=0.0):
        p[name] = (cost, list(after), list(rows), list(sends), delay)

    z_swap = [(("z", 1), 2.5), (("z", -1), 2.5)]
    y_swap = [(("y", 1), 0.9), (("y", -1), 0.9)]
    add(("carry4",), 0.5, [("carry3",)])
    add(("carry3",), 0.5, [("carry2",), ("dec_recv",)], (), z_swap, 2.5)
    add(("carry2",), 0.4, [("carry1",), ("dec_recv",)], (), y_swap, 2.6)
    add(("carry1",), 0.1, [("update",)], (), z_swap, 2.5)
    convs = [("conv", rel) for rel in RELS]
    add(("update",), 0.5, convs + [("delta",), ("state_conv",)])
    ready = [("transpose", i) for i in range(5)]
    for rel in RELS:
        add(("conv", rel), 1.0, [("mul", 0, rel, "A"), ("mul", 0, rel, "B"), ("gains",)])
        add(("mul", 0, rel, "A"), 0.6, ready, [(0, rel, "A")])
        add(("mul", 0, rel, "B"), 0.85, ready, [(0, rel, "B")])
    for i in range(4):
        add(("norm", i), 0.56)
    add(("halo",), 0.3, [("norm", 3)], (), (), 0.0)
    for i in range(5):
        add(("transpose", i), 0.42, [("halo",)])
    add(("gains",), 0.2, [("norm", 3)])
    for i in range(4):
        add(("state_weight", i), 0.48, ready)
    for i in range(3):
        add(("state", i), 0.6, [("state_weight", e) for e in range(4)])
    add(("state_conv",), 0.4, [("state", i) for i in range(3)])
    add(("delta",), 1.2, ready + [("gains",)])
    add(("scores",), 0.3, [("state_conv",)])
    add(("dec_send",), 0.1, [("delta",)], (), (), 5.0)
    for i in range(HEADS):
        add(("mix", i), 0.16, [("delta",), ("scores",)])
    add(("dec_recv",), 0.2, [("dec_send",)], (), (), 3.5)
    mixes = [("mix", i) for i in range(HEADS)]
    for rel in RELS:
        add(("gated", rel), 0.12, [("inter", rel), ("gate", rel)])
        add(("gate", rel), 0.35, [("mul", 1, rel, "A"), ("mul", 1, rel, "B")])
        add(("inter", rel), 0.2, [("carry4",), ("intra", 0), ("intra", 1)])
    for i in range(2):
        add(("intra", i), 0.9, mixes + convs)
    for rel in RELS:
        add(("mul", 1, rel, "A"), 0.5, [("conv", rel)], [(1, rel, "A")])
        add(("mul", 1, rel, "B"), 0.7, [("conv", rel)], [(1, rel, "B")])
    return p


def build_program():
    msgs, pieces = build_messages(), build_pieces()
    order = {k: i for i, k in enumerate(msgs)}

    def rank(k):
        if k[0][0] == "X":
            return (0, 9 if k[0] == "X1" else 0, order[k])
        if k[0] in ("Bz", "Ay"):
            p = 0
        elif k[0] == "Ay2":
            p = 0.5
        elif k[0] == "Az":
            p = 1 + k[3] + (0, 0.2, 0.4)[abs(k[4])]
        else:
            p = 1 + abs(k[3]) + (2 if k[0] == "By2" else 0)
        return (k[1], p, order[k])

    arrived, done, free, program = {}, {}, {}, []
    todo = sorted(msgs, key=rank)
    work = list(pieces)
    now = 0.0
    rows = {}
    for k in msgs:
        if k[0][0] in "AB":
            rows.setdefault((k[1], row_of(k), k[0][0]), []).append(k)
    while todo or work:
        moved = True
        while moved:
            moved = False
            for k in todo:
                link, dur, deps = msgs[k]
                later = k[0][0] != "X" and k[1] == 1
                if free.get(link, 0.0) > now + AHEAD[later] or (later and now < GATE_FROM):
                    continue
                if any(arrived.get(q, 1e9) > now for q in deps):
                    continue
                start = max(now, free.get(link, 0.0))
                free[link] = start + dur * SLOWER
                arrived[k] = free[link] + LATENCY
                program.append(("issue", k))
                todo.remove(k)
                now += 0.02
                moved = True
                break
        for name in work:
            cost, after, need, sends, delay = pieces[name]
            if any(done.get(q, 1e9) > now for q in after):
                continue
            if any(arrived.get(k, 1e9) > now for e in need for k in rows[e]):
                continue
            program.append(("piece", name))
            work.remove(name)
            now += cost
            end = now
            for link, dur in sends:
                free[link] = max(now, free.get(link, 0.0)) + dur * SLOWER
                end = max(end, free[link])
            done[name] = end + delay
            break
        else:
            now += 0.05
    return msgs, program, done, arrived


MSGS, PROGRAM, DONE, ARRIVED = build_program()
IDS = {k: i for i, k in enumerate(MSGS)}
N_MSG = len(MSGS)


def kernel(
    tok_in, gain_in, own_w, sw_in, st_in, bias_in, rate_in, skip_in, cw_w, cwst_in, og_w, ow,
    out,
    gain, own_in, st, bias, rate, skip, cw_in, cwst, og_in,
    tok, own_a, own_b, own_f, sw, swd, cwin, og, wa, wb, nrm, nt, spf, cb, ct, dec, cum, ecum, tailw, d01, scores, mix, term, colt,
    acc, joined, inn, gat, vt, vw, u, yv, cs, cr, co, ci, tt, rowd, prefix,
    sbf, scb, wr, relay, sq, rs_out, rs_in1, rs2_out, rs2_in, keep, own_p,
    halo, send, recv, xsend, xrecv, lsem,
):
    seq = lax.axis_index("seq")
    grp = lax.axis_index("grp")
    y, z = seq // NZ, lax.rem(seq, NZ)
    x, c = grp // 2, lax.rem(grp, 2)

    def yy(d):
        return lax.rem(y + d + NY, NY)

    def zz(d):
        return lax.rem(z + d + NZ, NZ)

    def xx(d):
        return lax.rem(x + d + NX, NX)

    def dev(dy=0, dz=0, dx=0, dc=0):
        return (yy(dy) * NZ + zz(dz), xx(dx) * 2 + lax.rem(c + dc, 2))

    nxt = (lax.rem(seq + 1, NY * NZ), grp)
    prv = (lax.rem(seq + NY * NZ - 1, NY * NZ), grp)

    barrier = pltpu.get_barrier_semaphore()
    peers = [nxt, prv]
    peers += [dev(dz=k) for k in range(1, NZ)]
    peers += [dev(dy=k) for k in range(1, NY)]
    peers += [dev(dx=k // 2, dc=k % 2) for k in range(1, 8)]
    for p in peers:
        pl.semaphore_signal(barrier, inc=1, device_id=p, device_id_type=MESH)

    def feature_columns(d, first, count):
        return ow.at[:, pl.ds(pl.multiple_of(xx(d) * 1280 + first, 128), count)]

    own_copy = pltpu.make_async_copy(own_w, own_in, lsem.at[6])
    own_copy.start()
    small = ((gain_in, gain), (st_in, st), (bias_in, bias), (rate_in, rate), (skip_in, skip),
             (cw_w, cw_in), (cwst_in, cwst), (og_w, og_in))
    small_copies = [pltpu.make_async_copy(a, b, lsem.at[7 + i]) for i, (a, b) in enumerate(small)]
    for q in small_copies:
        q.start()
    tok_copies = []
    for q in range(4):
        part = pl.ds(q * 128, 128)
        tok_copies.append(pltpu.make_async_copy(tok_in.at[part], tok.at[part], lsem.at[q]))
        tok_copies[q].start()
    sw_copy = pltpu.make_async_copy(sw_in, sw, lsem.at[4])
    sw_copy.start()
    own_out = pltpu.make_async_copy(feature_columns(0, 0, 1280), wr.at[x], lsem.at[5])
    own_out.start()
    own_copy.wait()
    for r in range(20):
        v = own_in[r].astype(F32)
        for h in (0, 1):
            for part in (0, 1):
                own_f[h, 20 * part + r : 20 * part + r + 1, :] = v[
                    h : h + 1, part * (D // 2) : (part + 1) * (D // 2)
                ]
    for h in (0, 1):
        v = own_f[h].astype(BF)
        own_a[h] = v[:, :KA]
        own_b[h] = v[:, KA:]
        wa[h, y, z] = v[:, :KA]
        wb[h, y, z] = v[:, KA:]
    nrm[0:128, :] = jnp.zeros((128, D), BF)
    for q in small_copies:
        q.wait()
    with jax.named_scope("barrier"):
        pl.semaphore_wait(barrier, len(peers))

    def remote(src, dst, s, r, to):
        return pltpu.make_async_remote_copy(
            src_ref=src, dst_ref=dst, send_sem=s, recv_sem=r, device_id=to, device_id_type=MESH
        )

    def message(k):
        i = IDS[k]
        kind = k[0]
        if kind[0] == "X":
            d = k[1]
            if kind == "X1":
                src, dst = feature_columns(d, 0, 1280), wr.at[x]
            elif kind == "X2":
                off = 0 if d == 1 else 640
                src = feature_columns(2, off, 640)
                dst = relay.at[0 if d == 1 else 1]
            else:
                off = 0 if d == 1 else 640
                src = relay.at[0 if d == 1 else 1]
                dst = wr.at[xx(-d), :, pl.ds(off, 640)]
            return remote(src, dst, send.at[i], recv.at[i], dev(dx=d))
        h, d = k[1], k[2]
        if kind == "Ay":
            src, dst, to = own_a.at[h], wa.at[h, y, z], dev(dy=d)
        elif kind == "Ay2":
            cols = pl.ds(0 if d == 1 else KA // 2, KA // 2)
            src = dst = wa.at[h, yy(-d), z, :, cols]
            to = dev(dy=d)
        elif kind == "Az":
            step, rel = k[3], k[4]
            dst = wa.at[h, yy(rel), zz(-d * (step - 1))]
            src = own_a.at[h] if (step == 1 and rel == 0) else dst
            to = dev(dz=d)
        elif kind == "Bz":
            step = k[3]
            dst = wb.at[h, y, zz(-d * (step - 1))]
            src = own_b.at[h] if step == 1 else dst
            if step == 4:
                cols = pl.ds(0 if d == 1 else KB // 2, KB // 2)
                src = dst = wb.at[h, y, zz(-d * 3), :, cols]
            to = dev(dz=d)
        elif kind == "By":
            zr = k[3]
            dst = wb.at[h, y, zz(zr)]
            src = own_b.at[h] if zr == 0 else dst
            to = dev(dy=d)
        else:
            src = dst = wb.at[h, yy(-d), zz(k[3])]
            to = dev(dy=d)
        return remote(src, dst, send.at[i], recv.at[i], to)

    waited = set()
    def take(k):
        if k not in waited:
            waited.add(k)
            message(k).wait_recv()

    def issue(k):
        for q in MSGS[k][2]:
            take(q)
        message(k).start()

    def complete(h, rel, route):
        for k in MSGS:
            if k[0][0] == route and k[1] == h and row_of(k) == rel:
                take(k)

    extra_sends = []

    def extra(src, dst, to, slot):
        q = remote(src, dst, xsend.at[slot], xrecv.at[slot], to)
        q.start()
        extra_sends.append(q)
        return q

    halo_copy = extra(tok_in.at[pl.ds(TOK - 16, 16)], halo, nxt, 0)

    def norm_rows(v):
        wide = v.astype(F32)
        ms = jnp.mean(wide * wide, axis=1, keepdims=True)
        return wide * lax.rsqrt(ms + EPS) * gain[...].reshape(1, D)

    def piece_norm(part):
        tok_copies[part].wait()

        def step(i, carry):
            r = pl.multiple_of(part * 128 + i * 16, 16)
            nrm[pl.ds(128 + r, 16), :] = norm_rows(tok[pl.ds(r, 16), :]).astype(BF)
            return carry

        lax.fori_loop(0, 8, step, 0, unroll=2)

    def piece_halo():
        halo_copy.wait_recv()
        n = jnp.where(seq > 0, norm_rows(halo[...]), 0.0)
        nrm[112:128, :] = n.astype(BF)

    def piece_transpose(tb):
        def step(i, carry):
            k = pl.multiple_of(i * 128, 128)
            nt[pl.ds(k, 128), tb * 128 : (tb + 1) * 128] = nrm[
                tb * 128 : (tb + 1) * 128, pl.ds(k, 128)
            ].T
            return carry

        lax.fori_loop(0, D // 128, step, 0, unroll=5)

    def piece_state_weight(part):
        if part == 0:
            sw_copy.wait()

        def step(i, carry):
            r = pl.multiple_of(i * 128 + part * 640, 128)
            v = sw[pl.ds(r, 128), :, :].astype(F32)
            swd[pl.ds(r, 128), 0:128] = v[:, 0, :].astype(BF)
            swd[pl.ds(r, 128), 128:256] = v[:, 1, :].astype(BF)
            return carry

        lax.fori_loop(0, 5, step, 0)

    def piece_state(part):
        r = part * 176
        got = dot(nrm[112 + r : 112 + r + 176, :], swd[...])
        spf[r : r + 176, :] = got.astype(BF).astype(F32)

    def piece_state_conv():
        for q in range(4):
            for k in (0, 1):
                acc = jnp.zeros((128, 128), F32)
                for j in range(4):
                    first = q * 128 + 13 + j
                    w = cwst[j].astype(F32)[k : k + 1, :]
                    acc = acc + w * spf[first : first + 128, k * 128 : (k + 1) * 128]
                v = acc * lax.logistic(acc)
                if k == 0:
                    cb[q * 128 : (q + 1) * 128, :] = v.astype(BF)
                else:
                    ct[:, q * 128 : (q + 1) * 128] = v.T.astype(BF)

    def piece_delta():
        row = lax.broadcasted_iota(jnp.int32, (HEADS, TOK), 0)
        bias_col = rate_col = jnp.zeros((HEADS, TOK), F32)
        for h in range(HEADS):
            bias_col = jnp.where(row == h, bias[h], bias_col)
            rate_col = jnp.where(row == h, rate[h], rate_col)
        pre = dot(st[...], nt[:, 128:640]) + bias_col
        delta = jnp.maximum(pre, 0.0) + jnp.log1p(jnp.exp(-jnp.abs(pre)))
        run = -delta * rate_col
        lane = lax.broadcasted_iota(jnp.int32, (HEADS, TOK), 1) % SPAN
        k = 1
        while k < SPAN:
            run = run + jnp.where(lane >= k, pltpu.roll(run, k, 1), 0.0)
            k *= 2
        cum[...] = run
        ecum[...] = jnp.exp(run)
        tot0, tot1 = run[:, 255:256], run[:, 511:512]
        tailw[:, :SPAN] = jnp.exp(tot0 - run[:, :SPAN]) * delta[:, :SPAN]
        tailw[:, SPAN:] = jnp.exp(tot1 - run[:, SPAN:]) * delta[:, SPAN:]
        d01[0] = jnp.broadcast_to(jnp.exp(tot0), (HEADS, 128))
        d01[1] = jnp.broadcast_to(jnp.exp(tot1), (HEADS, 128))
        whole = jnp.broadcast_to(jnp.exp(tot0) * jnp.exp(tot1), (HEADS, 128))
        for h in range(HEADS):
            dec[8, h] = whole[h : h + 1, :]
            dec[z, h] = whole[h : h + 1, :]
        term[...] = jnp.zeros((128, TOK), F32)
        term[0:HEADS, :] = jnp.log(delta) - run
        for q in range(4):
            colt[q * 128 : (q + 1) * 128, :] = term[:, q * 128 : (q + 1) * 128].T

    def piece_scores():
        for b in range(2):
            s = slice(b * SPAN, (b + 1) * SPAN)
            scores[b] = dot(cb[s, :], ct[:, s])

    dec_copies = []

    def piece_dec_send():
        for k in range(1, NZ):
            dec_copies.append(extra(dec.at[8], dec.at[z], dev(dz=k), k))

    def piece_dec_recv():
        for q in dec_copies:
            q.wait_recv()
        prod = dec[0]
        for k in range(1, NZ):
            prod = prod * dec[k]
        rowd[4] = prod
        rowd[y] = prod
        for k in range(1, NY):
            dec_copies.append(extra(rowd.at[4], rowd.at[y], dev(dy=k), 7 + k))

    def piece_mix(h):
        keep = lax.broadcasted_iota(jnp.int32, (128, 128), 1) >= lax.broadcasted_iota(
            jnp.int32, (128, 128), 0
        )
        for b in range(2):
            for s0 in range(2):
                r = b * SPAN + s0 * 128
                col = jnp.broadcast_to(colt[r : r + 128, h : h + 1], (128, 128))
                for t0 in range(2):
                    sl = (slice(s0 * 128, s0 * 128 + 128), slice(t0 * 128, t0 * 128 + 128))
                    if t0 < s0:
                        mix[(h, b) + sl] = jnp.zeros((128, 128), BF)
                        continue
                    q = b * SPAN + t0 * 128
                    arg = col + cum[h : h + 1, q : q + 128]
                    if s0 == t0:
                        arg = jnp.where(keep, arg, -jnp.inf)
                    mix[(h, b) + sl] = (scores[(b,) + sl] * jnp.exp(arg)).astype(BF)

    begun = set()

    def piece_mul(h, rel, route):
        i = RELS.index(rel)
        held, k0, kn = (wa, 0, KA) if route == "A" else (wb, KA, KB)
        lhs = held[h, yy(rel)].reshape(NZ * 40, kn)
        for cols in (slice(0, 256), slice(256, 512), slice(512, 640))[: 3 - h]:
            n = slice(128 * h + cols.start, 128 * h + cols.stop)
            for e in (0, 1):
                v = dot(lhs, nt[1280 * e + k0 : 1280 * e + k0 + kn, n])
                if (h, rel) in begun:
                    acc[i, e, :, cols] += v
                else:
                    acc[i, e, :, cols] = v
        begun.add((h, rel))

    def unfold(rel, into, width):
        i, r = RELS.index(rel), yy(rel)
        for e in range(NZ):
            v = acc[i, 0, 40 * e : 40 * e + 20, :width] + acc[i, 1, 40 * e + 20 : 40 * e + 40, :width]
            into[r, 20 * e : 20 * e + 20, :] = v.astype(BF).astype(F32)

    def piece_conv(r):
        def step(i, carry):
            q = pl.multiple_of(i * 32, 32)
            row = pl.multiple_of(r * 160 + q, 32)
            v = inn[r, pl.ds(q, 32), :]
            w = cwin[pl.ds(row, 32), :]
            acc = w[:, 3:4] * v[:, 128:]
            for j in range(3):
                acc = acc + w[:, j : j + 1] * pltpu.roll(v, 3 - j, 1)[:, 128:]
            vt[pl.ds(row, 32), :] = (acc * lax.logistic(acc)).astype(BF)
            return carry

        lax.fori_loop(0, 5, step, 0, unroll=5)

    def head_rows(h):
        return pl.ds(pl.multiple_of(h * 64, 64), 64)

    def piece_update():
        def weigh(h, carry):
            vw[head_rows(h), :] = (vt[head_rows(h), :].astype(F32) * tailw[pl.ds(h, 1), :]).astype(BF)
            return carry

        lax.fori_loop(0, HEADS, weigh, 0, unroll=2)
        for b in range(2):
            s = slice(b * SPAN, (b + 1) * SPAN)
            u[b] = dot(vw[:, s], cb[s, :])

        def total(h, carry):
            v = u[0, head_rows(h), :] * d01[1, pl.ds(h, 1), :] + u[1, head_rows(h), :]
            for j in range(NZ):
                cs[j, h] = v[8 * j : 8 * j + 8, :].astype(BF)
            return carry

        lax.fori_loop(0, HEADS, total, 0, unroll=2)
        cr[z] = cs[z]

    carry1, carry2, carry3 = [], [], []

    def piece_carry1():
        for k in FAR_FIRST:
            carry1.append(extra(cs.at[zz(k)], cr.at[z], dev(dz=k), 10 + k))

    def piece_carry2():
        for q in carry1:
            q.wait_recv()
        run = jnp.zeros((HEADS, 8, 128), F32)
        for k in range(NZ):
            prefix[k] = run
            run = run * dec[k] + cr[k].astype(F32)
        tt[4] = run.astype(BF)
        tt[y] = run.astype(BF)
        for k in (2, 1, 3):
            carry2.append(extra(tt.at[4], tt.at[y], dev(dy=k), 17 + k))

    def piece_carry3():
        for q in carry2 + dec_copies[7:]:
            q.wait_recv()
        r = jnp.zeros((HEADS, 8, 128), F32)
        for k in range(NY - 1):
            r = jnp.where(y > k, r * rowd[k] + tt[k].astype(F32), r)
        for k in range(NZ):
            co[k] = (prefix[k] + r).astype(BF)
            r = r * dec[k]
        ci[z] = co[z]
        for k in FAR_FIRST:
            carry3.append(extra(co.at[zz(k)], ci.at[z], dev(dz=k), 20 + k))

    def piece_carry4():
        for q in carry3:
            q.wait_recv()

        def step(h, carry):
            v = jnp.concatenate([ci[j, h].astype(F32) for j in range(NZ)], axis=0)
            sbf[0, head_rows(h), :] = v.astype(BF)
            sbf[1, head_rows(h), :] = (v * d01[0, pl.ds(h, 1), :] + u[0, head_rows(h), :]).astype(BF)
            return carry

        lax.fori_loop(0, HEADS, step, 0)

    def piece_intra(b):
        s = slice(b * SPAN, (b + 1) * SPAN)

        def step(h, carry):
            v = vt[head_rows(h), s]
            yv[head_rows(h), s] = dot(v, mix[h, b]) + skip[h] * v.astype(F32)
            return carry

        lax.fori_loop(0, HEADS, step, 0, unroll=2)

    def piece_inter(r):
        rows = pl.ds(pl.multiple_of(r * 160, 160), 160)
        for b in range(2):
            s = slice(b * SPAN, (b + 1) * SPAN)
            joined[:, s] = dot(sbf[b, rows, :], ct[:, s])

        def step(i, carry):
            q = pl.multiple_of(i * 32, 32)
            row = pl.ds(pl.multiple_of(r * 160 + q, 32), 32)
            e = ecum[pl.ds((5 * r + i) // 2, 1), :]
            yv[row, :] = yv[row, :] + e * joined[pl.ds(q, 32), :]
            return carry

        lax.fori_loop(0, 5, step, 0, unroll=5)

    pair_copies, sq_copies = [], []
    sq[8] = jnp.zeros((8, TOK), F32)

    def piece_gated(r, slot):
        def step(i, total):
            q = pl.multiple_of(i * 32, 32)
            row = pl.ds(pl.multiple_of(r * 160 + q, 32), 32)
            g = gat[r, pl.ds(q, 32), :]
            v = yv[row, :] * (g * lax.logistic(g))
            for e in range(4):
                w = v[8 * e : 8 * e + 8, :]
                total = total + w * w
            scb[c, row, :] = (v * og[row, 0:1]).astype(BF)
            return total

        sq[8] = lax.fori_loop(0, 5, step, sq[8], unroll=5)
        own = scb.at[c, pl.ds(pl.multiple_of(r * 160, 160), 160)]
        pair_copies.append(extra(own, own, dev(dc=1), 28 + slot))

    def piece_squares():
        sq[grp] = sq[8]
        for k in range(1, 8):
            sq_copies.append(extra(sq.at[8], sq.at[grp], dev(dx=k // 2, dc=k % 2), 31 + k))

    def project(dx, half):
        s = slice(half * SPAN, (half + 1) * SPAN)
        p = xx(dx)
        return dot(wr[p, :, 0:CH], scb[0, :, s]) + dot(wr[p, :, CH : 2 * CH], scb[1, :, s])

    def piece_gains():
        term[...] = jnp.zeros((128, TOK), F32)
        for q in range(CH // 128):
            cols = slice(q * 128, q * 128 + 128)
            term[0:4, 0:128] = cw_in[:, cols].astype(F32)
            cwin[cols, :] = term[:, 0:128].T
            og[cols, :] = jnp.broadcast_to(og_in[cols].reshape(1, 128), (128, 128)).T

    def call(piece, *args):
        with jax.named_scope(piece.__name__ + "".join(f"#i={a}" for a in args if isinstance(a, int))):
            return piece(*args)

    def mul(h, rel, route):
        complete(h, rel, route)
        piece_mul(h, rel, route)

    def conv(rel):
        unfold(rel, inn, 640)
        piece_conv(yy(rel))

    does = {
        "norm": piece_norm,
        "halo": piece_halo,
        "gains": piece_gains,
        "transpose": piece_transpose,
        "state_weight": piece_state_weight,
        "state": piece_state,
        "state_conv": piece_state_conv,
        "delta": piece_delta,
        "scores": piece_scores,
        "dec_send": piece_dec_send,
        "dec_recv": piece_dec_recv,
        "mix": piece_mix,
        "mul": mul,
        "conv": conv,
        "update": piece_update,
        "carry1": piece_carry1,
        "carry2": piece_carry2,
        "carry3": piece_carry3,
        "carry4": piece_carry4,
        "intra": piece_intra,
        "inter": lambda rel: piece_inter(yy(rel)),
        "gate": lambda rel: unfold(rel, gat, TOK),
        "gated": lambda rel: piece_gated(yy(rel), rel + 1),
    }
    for what, k in PROGRAM:
        if what == "issue":
            issue(k)
        else:
            with jax.named_scope("#".join(str(e) for e in k)):
                does[k[0]](*k[1:])
    call(piece_squares)
    with jax.named_scope("wait_weights"):
        own_out.wait()
        for k in (("X1", 1), ("X1", -1), ("X2f", 1), ("X2f", -1)):
            take(k)
    with jax.named_scope("wait_pair"):
        for q in pair_copies:
            q.wait_recv()

    top, low = slice(0, 160), slice(160, 320)
    far, near = {}, []

    def send_far(half):
        got = call(project, 2, half)
        rs_out[half] = got.astype(BF)
        for i, d in enumerate((1, -1)):
            rows = pl.ds(160 * i, 160)
            far[half, d] = extra(
                rs_out.at[half, rows], rs_in1.at[half, rows], dev(dx=d), 40 + 2 * half + i
            )

    def send_direct(half):
        for i, d in enumerate((1, -1)):
            keep[i] = call(project, d, half)
            rows = low if d == 1 else top
            rs2_out[i, half, rows] = keep[i, rows].astype(BF)
            rows = pl.ds(160 * (1 - i), 160)
            part = (i, half, rows)
            near.append(extra(rs2_out.at[part], rs2_in.at[part], dev(dx=d), 44 + 4 * half + i))

    def send_relayed(half):
        for i, d in enumerate((1, -1)):
            with jax.named_scope("wait_far"):
                far[half, d].wait_recv()
            rows = top if d == 1 else low
            rs2_out[i, half, rows] = (keep[i, rows] + rs_in1[half, rows].astype(F32)).astype(BF)
            rows = pl.ds(160 * i, 160)
            part = (i, half, rows)
            near.append(extra(rs2_out.at[part], rs2_in.at[part], dev(dx=d), 46 + 4 * half + i))

    send_far(0)
    send_direct(0)
    send_far(1)
    send_relayed(0)
    send_direct(1)
    own_p[0] = call(project, 0, 0)
    send_relayed(1)
    own_p[1] = call(project, 0, 1)
    with jax.named_scope("wait_sq"):
        for q in sq_copies:
            q.wait_recv()
    total = sq[0]
    for k in range(1, 8):
        total = total + sq[k]
    total = jnp.sum(total, axis=0, keepdims=True)
    scale = lax.rsqrt(total / (8 * CH) + EPS)
    for half in range(2):
        with jax.named_scope("wait_near"):
            for q in near[4 * half : 4 * half + 4]:
                q.wait_recv()
        v = own_p[half] + rs2_in[0, half].astype(F32) + rs2_in[1, half].astype(F32)
        s = slice(half * SPAN, (half + 1) * SPAN)
        out[:, s] = (v * scale[:, s]).astype(BF)
    with jax.named_scope("wait_sends"):
        for k in MSGS:
            message(k).wait_send()
    for q in extra_sends:
        q.wait_send()


def run(*args):
    vm = pl.BlockSpec(memory_space=pltpu.VMEM)
    specs = [pl.BlockSpec(memory_space=pl.ANY)] * 12
    V = pltpu.VMEM
    scratch = [
        V((D,), F32),
        V((20, 2, D), BF),
        V((HEADS, D), BF),
        pltpu.SMEM((HEADS,), F32),
        pltpu.SMEM((HEADS,), F32),
        pltpu.SMEM((HEADS,), F32),
        V((4, CH), BF),
        V((4, 2, 128), BF),
        V((CH,), F32),
        V((TOK, D), BF),
        V((2, 40, KA), BF),
        V((2, 40, KB), BF),
        V((2, 40, D // 2), F32),
        V((D, 2, 128), BF),
        V((D, 256), BF),
        V((CH, 128), F32),
        V((CH, 128), F32),
        V((2, NY, NZ, 40, KA), BF),
        V((2, NY, NZ, 40, KB), BF),
        V((640, D), BF),
        V((D, 640), BF),
        V((528, 256), F32),
        V((TOK, 128), BF),
        V((128, TOK), BF),
        V((9, HEADS, 1, 128), F32),
        V((HEADS, TOK), F32),
        V((HEADS, TOK), F32),
        V((HEADS, TOK), F32),
        V((2, HEADS, 128), F32),
        V((2, SPAN, SPAN), F32),
        V((HEADS, 2, SPAN, SPAN), BF),
        V((128, TOK), F32),
        V((TOK, 128), F32),
        V((4, 2, 320, 640), F32),
        V((160, TOK), F32),
        V((NY, 160, 640), F32),
        V((NY, 160, TOK), F32),
        V((CH, TOK), BF),
        V((CH, TOK), BF),
        V((2, CH, 128), F32),
        V((CH, TOK), F32),
        V((NZ, HEADS, 8, 128), BF),
        V((NZ, HEADS, 8, 128), BF),
        V((NZ, HEADS, 8, 128), BF),
        V((NZ, HEADS, 8, 128), BF),
        V((5, HEADS, 8, 128), BF),
        V((5, HEADS, 1, 128), F32),
        V((NZ, HEADS, 8, 128), F32),
        V((2, CH, 128), BF),
        V((2, CH, TOK), BF),
        V((NX, FEAT, 1280), BF),
        V((2, FEAT, 640), BF),
        V((9, 8, TOK), F32),
        V((2, FEAT, SPAN), BF),
        V((2, FEAT, SPAN), BF),
        V((2, 2, FEAT, SPAN), BF),
        V((2, 2, FEAT, SPAN), BF),
        V((2, FEAT, SPAN), F32),
        V((2, FEAT, SPAN), F32),
        V((16, D), BF),
        pltpu.SemaphoreType.DMA((N_MSG,)),
        pltpu.SemaphoreType.DMA((N_MSG,)),
        pltpu.SemaphoreType.DMA((52,)),
        pltpu.SemaphoreType.DMA((52,)),
        pltpu.SemaphoreType.DMA((15,)),
    ]
    return pl.pallas_call(
        kernel,
        out_shape=jax.ShapeDtypeStruct((FEAT, TOK), BF),
        in_specs=specs,
        out_specs=vm,
        scratch_shapes=scratch,
        compiler_params=pltpu.CompilerParams(
            collective_id=0, has_side_effects=True, vmem_limit_bytes=64 * 2**20 - 65536
        ),
        name="layer",
    )(*args)


def body(
    tokens, norm_gain, inner_weight, state_weight, step_weight, step_bias, decay_rate,
    skip_scale, conv_inner, conv_state, out_gain, out_weight,
):
    return run(
        tokens, norm_gain, inner_weight.transpose(2, 1, 0), state_weight, step_weight.T,
        step_bias, decay_rate, skip_scale, conv_inner, conv_state, out_gain, out_weight.T,
    ).T


def solution(mesh):
    return jax.shard_map(
        body,
        mesh=mesh,
        in_specs=(
            P("seq", None), P(), P(None, None, ("grp", "seq")), P(), P(None, "grp"), P("grp"),
            P("grp"), P("grp"), P(None, "grp"), P(), P("grp"), P(None, "grp"),
        ),
        out_specs=P("seq", "grp"),
        check_vma=False,
    )
```

```python
import functools

import jax
import jax.numpy as jnp
from jax import lax
from jax.experimental import pallas as pl
from jax.experimental.pallas import tpu as pltpu
from jax.sharding import PartitionSpec as P

MESH = pl.DeviceIdType.MESH
BF = jnp.bfloat16
F32 = jnp.float32
EPS = 1e-05

TOK = 512
D = 2560
CH = 640
HEADS = 10
SPAN = 256
KA, KB = 512, 768
FEAT = 320
NY, NZ, NX = 4, 8, 4


def dot(a, b):
    return jnp.dot(a, b, preferred_element_type=F32)


def half_messages(h):
    m = {}
    for d in (1, -1):
        m["Ay", h, d] = (("y", d), 0.88, [])
        m["Ay2", h, d] = (("y", d), 0.44, [("Ay", h, d)])
        for k in range(1, 5):
            rels = (0, -1, 1, 2) if k < 4 else ((0, -1) if d == 1 else (1, 2))
            for rel in rels:
                if k > 1:
                    dep = [("Az", h, d, k - 1, rel)]
                else:
                    dep = {
                        0: [],
                        -1: [("Ay", h, 1)],
                        1: [("Ay", h, -1)],
                        2: [("Ay2", h, 1), ("Ay2", h, -1)],
                    }[rel]
                m["Az", h, d, k, rel] = (("z", d), 0.88, dep)
            dep = [("Bz", h, d, k - 1)] if k > 1 else []
            m["Bz", h, d, k] = (("z", d), 1.32 if k < 4 else 0.66, dep)
        for zr in range(-3, 5):
            if zr == 0:
                dep = []
            elif zr == 4:
                dep = [("Bz", h, 1, 4), ("Bz", h, -1, 4)]
            else:
                dep = [("Bz", h, 1, -zr)] if zr < 0 else [("Bz", h, -1, zr)]
            m["By", h, d, zr] = (("y", d), 1.32, dep)
            if (zr <= 0) == (d == 1):
                m["By2", h, d, zr] = (("y", d), 1.32, [("By", h, d, zr)])
    return m


def row_of(k):
    kind = k[0]
    if kind == "Bz":
        return 0
    if kind in ("Ay", "By"):
        return -k[2]
    return k[4] if kind == "Az" else 2


SLOWER = 1.12
LATENCY = 2.4
AHEAD = (1.2, 0.3)
GATE_FROM = 0.0
RELS = (0, -1, 1, 2)
FAR_FIRST = (4, 3, 5, 2, 6, 1, 7)


def build_messages():
    msgs = {}
    for d in (1, -1):
        msgs["X2", d] = (("x", d), 8.8, [])
        msgs["X1", d] = (("x", d), 17.6, [])
        msgs["X2f", d] = (("x", d), 8.8, [("X2", d)])
    for h in (0, 1):
        msgs.update(half_messages(h))
    return msgs


def build_pieces():
    p = {}

    def add(name, cost, after=(), rows=(), sends=(), delay=0.0):
        p[name] = (cost, list(after), list(rows), list(sends), delay)

    z_swap = [(("z", 1), 2.5), (("z", -1), 2.5)]
    y_swap = [(("y", 1), 0.9), (("y", -1), 0.9)]
    add(("carry4",), 0.5, [("carry3",)])
    add(("carry3",), 0.5, [("carry2",), ("dec_recv",)], (), z_swap, 2.5)
    add(("carry2",), 0.4, [("carry1",), ("dec_recv",)], (), y_swap, 2.6)
    add(("carry1",), 0.1, [("update",)], (), z_swap, 2.5)
    convs = [("conv", rel) for rel in RELS]
    add(("update",), 0.5, convs + [("delta",), ("state_conv",)])
    ready = [("transpose", i) for i in range(5)]
    for rel in RELS:
        add(("conv", rel), 0.4, [("mul", 0, rel, "A"), ("mul", 0, rel, "B"), ("gains",)])
        add(("mul", 0, rel, "A"), 0.44, ready, [(0, rel, "A")])
        add(("mul", 0, rel, "B"), 0.58, ready, [(0, rel, "B")])
    for i in range(4):
        add(("norm", i), 0.56)
    add(("halo",), 0.3, [("norm", 3)], (), (), 0.0)
    for i in range(5):
        add(("transpose", i), 0.42, [("halo",)])
    add(("gains",), 0.2, [("norm", 3)])
    for i in range(4):
        add(("state_weight", i), 0.48, ready)
    for i in range(3):
        add(("state", i), 0.6, [("state_weight", e) for e in range(4)])
    add(("state_conv",), 0.4, [("state", i) for i in range(3)])
    add(("delta",), 1.2, ready + [("gains",)])
    add(("scores",), 0.3, [("state_conv",)])
    add(("dec_send",), 0.1, [("delta",)], (), (), 5.0)
    for i in range(HEADS):
        add(("mix", i), 0.16, [("delta",), ("scores",)])
    add(("dec_recv",), 0.2, [("dec_send",)], (), (), 3.5)
    mixes = [("mix", i) for i in range(HEADS)]
    for rel in RELS:
        add(("gated", rel), 0.12, [("inter", rel), ("gate", rel)])
        add(("gate", rel), 0.05, [("mul", 1, rel, "A"), ("mul", 1, rel, "B")])
        add(("inter", rel), 0.2, [("carry4",), ("intra", 0), ("intra", 1)])
    for i in range(2):
        add(("intra", i), 0.9, mixes + convs)
    for rel in RELS:
        add(("mul", 1, rel, "A"), 0.35, [("conv", rel)], [(1, rel, "A")])
        add(("mul", 1, rel, "B"), 0.32, [("conv", rel)], [(1, rel, "B")])
    return p


def build_program():
    msgs, pieces = build_messages(), build_pieces()
    order = {k: i for i, k in enumerate(msgs)}

    def rank(k):
        if k[0][0] == "X":
            return (0, 9 if k[0] == "X1" else 0, order[k])
        if k[0] in ("Bz", "Ay"):
            p = 0
        elif k[0] == "Ay2":
            p = 0.5
        elif k[0] == "Az":
            p = 1 + k[3] + (0, 0.2, 0.4)[abs(k[4])]
        else:
            p = 1 + abs(k[3]) + (2 if k[0] == "By2" else 0)
        return (k[1], p, order[k])

    arrived, done, free, program = {}, {}, {}, []
    todo = sorted(msgs, key=rank)
    work = list(pieces)
    now = 0.0
    rows = {}
    for k in msgs:
        if k[0][0] in "AB":
            rows.setdefault((k[1], row_of(k), k[0][0]), []).append(k)
    while todo or work:
        moved = True
        while moved:
            moved = False
            for k in todo:
                link, dur, deps = msgs[k]
                later = k[0][0] != "X" and k[1] == 1
                if free.get(link, 0.0) > now + AHEAD[later] or (later and now < GATE_FROM):
                    continue
                if any(arrived.get(q, 1e9) > now for q in deps):
                    continue
                start = max(now, free.get(link, 0.0))
                free[link] = start + dur * SLOWER
                arrived[k] = free[link] + LATENCY
                program.append(("issue", k))
                todo.remove(k)
                now += 0.02
                moved = True
                break
        for name in work:
            cost, after, need, sends, delay = pieces[name]
            if any(done.get(q, 1e9) > now for q in after):
                continue
            if any(arrived.get(k, 1e9) > now for e in need for k in rows[e]):
                continue
            program.append(("piece", name))
            work.remove(name)
            now += cost
            end = now
            for link, dur in sends:
                free[link] = max(now, free.get(link, 0.0)) + dur * SLOWER
                end = max(end, free[link])
            done[name] = end + delay
            break
        else:
            now += 0.05
    return msgs, program, done, arrived


MSGS, PROGRAM, DONE, ARRIVED = build_program()
IDS = {k: i for i, k in enumerate(MSGS)}
N_MSG = len(MSGS)


def kernel(
    tok_in, gain_in, own_w, sw_in, st_in, bias_in, rate_in, skip_in, cw_w, cwst_in, og_w, ow,
    out,
    gain, own_in, st, bias, rate, skip, cw_in, cwst, og_in,
    tok, own_a, own_b, own_f, sw, swd, cwin, og, wa, wb, nrm, nt, spf, cb, ct, dec, cum, ecum, tailw, d01, scores, mix, term, colt,
    acc, joined, inn, gat, vt, vw, u, yv, cs, cr, co, ci, tt, rowd, prefix,
    sbf, scb, wr, relay, sq, rs_out, rs_in1, rs2_out, rs2_in, keep, own_p,
    halo, send, recv, xsend, xrecv, lsem,
):
    seq = lax.axis_index("seq")
    grp = lax.axis_index("grp")
    y, z = seq // NZ, lax.rem(seq, NZ)
    x, c = grp // 2, lax.rem(grp, 2)

    def yy(d):
        return lax.rem(y + d + NY, NY)

    def zz(d):
        return lax.rem(z + d + NZ, NZ)

    def xx(d):
        return lax.rem(x + d + NX, NX)

    def dev(dy=0, dz=0, dx=0, dc=0):
        return (yy(dy) * NZ + zz(dz), xx(dx) * 2 + lax.rem(c + dc, 2))

    nxt = (lax.rem(seq + 1, NY * NZ), grp)
    prv = (lax.rem(seq + NY * NZ - 1, NY * NZ), grp)

    barrier = pltpu.get_barrier_semaphore()
    peers = [nxt, prv]
    peers += [dev(dz=k) for k in range(1, NZ)]
    peers += [dev(dy=k) for k in range(1, NY)]
    peers += [dev(dx=k // 2, dc=k % 2) for k in range(1, 8)]
    for p in peers:
        pl.semaphore_signal(barrier, inc=1, device_id=p, device_id_type=MESH)

    def feature_columns(d, first, count):
        return ow.at[:, pl.ds(pl.multiple_of(xx(d) * 1280 + first, 128), count)]

    own_copy = pltpu.make_async_copy(own_w, own_in, lsem.at[6])
    own_copy.start()
    small = ((gain_in, gain), (st_in, st), (bias_in, bias), (rate_in, rate), (skip_in, skip),
             (cw_w, cw_in), (cwst_in, cwst), (og_w, og_in))
    small_copies = [pltpu.make_async_copy(a, b, lsem.at[7 + i]) for i, (a, b) in enumerate(small)]
    for q in small_copies:
        q.start()
    tok_copies = []
    for q in range(4):
        part = pl.ds(q * 128, 128)
        tok_copies.append(pltpu.make_async_copy(tok_in.at[part], tok.at[part], lsem.at[q]))
        tok_copies[q].start()
    sw_copy = pltpu.make_async_copy(sw_in, sw, lsem.at[4])
    sw_copy.start()
    own_out = pltpu.make_async_copy(feature_columns(0, 0, 1280), wr.at[x], lsem.at[5])
    own_out.start()
    own_copy.wait()
    for r in range(20):
        v = own_in[r].astype(F32)
        for h in (0, 1):
            for part in (0, 1):
                own_f[h, 20 * part + r : 20 * part + r + 1, :] = v[
                    h : h + 1, part * (D // 2) : (part + 1) * (D // 2)
                ]
    for h in (0, 1):
        v = own_f[h].astype(BF)
        own_a[h] = v[:, :KA]
        own_b[h] = v[:, KA:]
        wa[h, y, z] = v[:, :KA]
        wb[h, y, z] = v[:, KA:]
    nrm[0:128, :] = jnp.zeros((128, D), BF)
    for q in small_copies:
        q.wait()
    with jax.named_scope("barrier"):
        pl.semaphore_wait(barrier, len(peers))

    def remote(src, dst, s, r, to):
        return pltpu.make_async_remote_copy(
            src_ref=src, dst_ref=dst, send_sem=s, recv_sem=r, device_id=to, device_id_type=MESH
        )

    def message(k):
        i = IDS[k]
        kind = k[0]
        if kind[0] == "X":
            d = k[1]
            if kind == "X1":
                src, dst = feature_columns(d, 0, 1280), wr.at[x]
            elif kind == "X2":
                off = 0 if d == 1 else 640
                src = feature_columns(2, off, 640)
                dst = relay.at[0 if d == 1 else 1]
            else:
                off = 0 if d == 1 else 640
                src = relay.at[0 if d == 1 else 1]
                dst = wr.at[xx(-d), :, pl.ds(off, 640)]
            return remote(src, dst, send.at[i], recv.at[i], dev(dx=d))
        h, d = k[1], k[2]
        if kind == "Ay":
            src, dst, to = own_a.at[h], wa.at[h, y, z], dev(dy=d)
        elif kind == "Ay2":
            cols = pl.ds(0 if d == 1 else KA // 2, KA // 2)
            src = dst = wa.at[h, yy(-d), z, :, cols]
            to = dev(dy=d)
        elif kind == "Az":
            step, rel = k[3], k[4]
            dst = wa.at[h, yy(rel), zz(-d * (step - 1))]
            src = own_a.at[h] if (step == 1 and rel == 0) else dst
            to = dev(dz=d)
        elif kind == "Bz":
            step = k[3]
            dst = wb.at[h, y, zz(-d * (step - 1))]
            src = own_b.at[h] if step == 1 else dst
            if step == 4:
                cols = pl.ds(0 if d == 1 else KB // 2, KB // 2)
                src = dst = wb.at[h, y, zz(-d * 3), :, cols]
            to = dev(dz=d)
        elif kind == "By":
            zr = k[3]
            dst = wb.at[h, y, zz(zr)]
            src = own_b.at[h] if zr == 0 else dst
            to = dev(dy=d)
        else:
            src = dst = wb.at[h, yy(-d), zz(k[3])]
            to = dev(dy=d)
        return remote(src, dst, send.at[i], recv.at[i], to)

    waited = set()
    def take(k):
        if k not in waited:
            waited.add(k)
            message(k).wait_recv()

    def issue(k):
        for q in MSGS[k][2]:
            take(q)
        message(k).start()

    def complete(h, rel, route):
        for k in MSGS:
            if k[0][0] == route and k[1] == h and row_of(k) == rel:
                take(k)

    extra_sends = []

    def extra(src, dst, to, slot):
        q = remote(src, dst, xsend.at[slot], xrecv.at[slot], to)
        q.start()
        extra_sends.append(q)
        return q

    halo_copy = extra(tok_in.at[pl.ds(TOK - 16, 16)], halo, nxt, 0)

    def norm_rows(v):
        wide = v.astype(F32)
        ms = jnp.mean(wide * wide, axis=1, keepdims=True)
        return wide * lax.rsqrt(ms + EPS) * gain[...].reshape(1, D)

    def piece_norm(part):
        tok_copies[part].wait()

        def step(i, carry):
            r = pl.multiple_of(part * 128 + i * 16, 16)
            nrm[pl.ds(128 + r, 16), :] = norm_rows(tok[pl.ds(r, 16), :]).astype(BF)
            return carry

        lax.fori_loop(0, 8, step, 0, unroll=2)

    def piece_halo():
        halo_copy.wait_recv()
        n = jnp.where(seq > 0, norm_rows(halo[...]), 0.0)
        nrm[112:128, :] = n.astype(BF)

    def piece_transpose(tb):
        def step(i, carry):
            k = pl.multiple_of(i * 128, 128)
            nt[pl.ds(k, 128), tb * 128 : (tb + 1) * 128] = nrm[
                tb * 128 : (tb + 1) * 128, pl.ds(k, 128)
            ].T
            return carry

        lax.fori_loop(0, D // 128, step, 0, unroll=5)

    def piece_state_weight(part):
        if part == 0:
            sw_copy.wait()

        def step(i, carry):
            r = pl.multiple_of(i * 128 + part * 640, 128)
            v = sw[pl.ds(r, 128), :, :].astype(F32)
            swd[pl.ds(r, 128), 0:128] = v[:, 0, :].astype(BF)
            swd[pl.ds(r, 128), 128:256] = v[:, 1, :].astype(BF)
            return carry

        lax.fori_loop(0, 5, step, 0)

    def piece_state(part):
        r = part * 176
        got = dot(nrm[112 + r : 112 + r + 176, :], swd[...])
        spf[r : r + 176, :] = got.astype(BF).astype(F32)

    def piece_state_conv():
        for q in range(4):
            for k in (0, 1):
                acc = jnp.zeros((128, 128), F32)
                for j in range(4):
                    first = q * 128 + 13 + j
                    w = cwst[j].astype(F32)[k : k + 1, :]
                    acc = acc + w * spf[first : first + 128, k * 128 : (k + 1) * 128]
                v = acc * lax.logistic(acc)
                if k == 0:
                    cb[q * 128 : (q + 1) * 128, :] = v.astype(BF)
                else:
                    ct[:, q * 128 : (q + 1) * 128] = v.T.astype(BF)

    def piece_delta():
        row = lax.broadcasted_iota(jnp.int32, (HEADS, TOK), 0)
        bias_col = rate_col = jnp.zeros((HEADS, TOK), F32)
        for h in range(HEADS):
            bias_col = jnp.where(row == h, bias[h], bias_col)
            rate_col = jnp.where(row == h, rate[h], rate_col)
        pre = dot(st[...], nt[:, 128:640]) + bias_col
        delta = jnp.maximum(pre, 0.0) + jnp.log1p(jnp.exp(-jnp.abs(pre)))
        run = -delta * rate_col
        lane = lax.broadcasted_iota(jnp.int32, (HEADS, TOK), 1) % SPAN
        k = 1
        while k < SPAN:
            run = run + jnp.where(lane >= k, pltpu.roll(run, k, 1), 0.0)
            k *= 2
        cum[...] = run
        ecum[...] = jnp.exp(run)
        tot0, tot1 = run[:, 255:256], run[:, 511:512]
        tailw[:, :SPAN] = jnp.exp(tot0 - run[:, :SPAN]) * delta[:, :SPAN]
        tailw[:, SPAN:] = jnp.exp(tot1 - run[:, SPAN:]) * delta[:, SPAN:]
        d01[0] = jnp.broadcast_to(jnp.exp(tot0), (HEADS, 128))
        d01[1] = jnp.broadcast_to(jnp.exp(tot1), (HEADS, 128))
        whole = jnp.broadcast_to(jnp.exp(tot0) * jnp.exp(tot1), (HEADS, 128))
        for h in range(HEADS):
            dec[8, h] = whole[h : h + 1, :]
            dec[z, h] = whole[h : h + 1, :]
        term[...] = jnp.zeros((128, TOK), F32)
        term[0:HEADS, :] = jnp.log(delta) - run
        for q in range(4):
            colt[q * 128 : (q + 1) * 128, :] = term[:, q * 128 : (q + 1) * 128].T

    def piece_scores():
        for b in range(2):
            s = slice(b * SPAN, (b + 1) * SPAN)
            scores[b] = dot(cb[s, :], ct[:, s])

    dec_copies = []

    def piece_dec_send():
        for k in range(1, NZ):
            dec_copies.append(extra(dec.at[8], dec.at[z], dev(dz=k), k))

    def piece_dec_recv():
        for q in dec_copies:
            q.wait_recv()
        prod = dec[0]
        for k in range(1, NZ):
            prod = prod * dec[k]
        rowd[4] = prod
        rowd[y] = prod
        for k in range(1, NY):
            dec_copies.append(extra(rowd.at[4], rowd.at[y], dev(dy=k), 7 + k))

    def piece_mix(h):
        keep = lax.broadcasted_iota(jnp.int32, (128, 128), 1) >= lax.broadcasted_iota(
            jnp.int32, (128, 128), 0
        )
        for b in range(2):
            for s0 in range(2):
                r = b * SPAN + s0 * 128
                col = jnp.broadcast_to(colt[r : r + 128, h : h + 1], (128, 128))
                for t0 in range(2):
                    sl = (slice(s0 * 128, s0 * 128 + 128), slice(t0 * 128, t0 * 128 + 128))
                    if t0 < s0:
                        mix[(h, b) + sl] = jnp.zeros((128, 128), BF)
                        continue
                    q = b * SPAN + t0 * 128
                    arg = col + cum[h : h + 1, q : q + 128]
                    if s0 == t0:
                        arg = jnp.where(keep, arg, -jnp.inf)
                    mix[(h, b) + sl] = (scores[(b,) + sl] * jnp.exp(arg)).astype(BF)

    begun = set()

    def piece_mul(h, rel, route):
        i = RELS.index(rel)
        held, k0, kn = (wa, 0, KA) if route == "A" else (wb, KA, KB)
        whole = [held[h, yy(rel), q] for q in range(NZ)]
        lhs = [
            jnp.concatenate([v[20 * e : 20 * e + 20, :] for v in whole], axis=0) for e in (0, 1)
        ]
        for cols in (slice(0, 256), slice(256, 512), slice(512, 640))[: 3 - h]:
            n = slice(128 * h + cols.start, 128 * h + cols.stop)
            v = dot(lhs[0], nt[k0 : k0 + kn, n]) + dot(lhs[1], nt[1280 + k0 : 1280 + k0 + kn, n])
            if (h, rel) in begun:
                acc[i, :, cols] += v
            else:
                acc[i, :, cols] = v
        begun.add((h, rel))

    def unfold(rel, into, width):
        i, r = RELS.index(rel), yy(rel)
        into[r] = acc[i, :, :width].astype(BF).astype(F32)

    def piece_conv(r):
        def step(i, carry):
            q = pl.multiple_of(i * 32, 32)
            row = pl.multiple_of(r * 160 + q, 32)
            v = inn[r, pl.ds(q, 32), :]
            w = cwin[pl.ds(row, 32), :]
            acc = w[:, 3:4] * v[:, 128:]
            for j in range(3):
                acc = acc + w[:, j : j + 1] * pltpu.roll(v, 3 - j, 1)[:, 128:]
            vt[pl.ds(row, 32), :] = (acc * lax.logistic(acc)).astype(BF)
            return carry

        lax.fori_loop(0, 5, step, 0, unroll=5)

    def head_rows(h):
        return pl.ds(pl.multiple_of(h * 64, 64), 64)

    def piece_update():
        def weigh(h, carry):
            vw[head_rows(h), :] = (vt[head_rows(h), :].astype(F32) * tailw[pl.ds(h, 1), :]).astype(BF)
            return carry

        lax.fori_loop(0, HEADS, weigh, 0, unroll=2)
        for b in range(2):
            s = slice(b * SPAN, (b + 1) * SPAN)
            u[b] = dot(vw[:, s], cb[s, :])

        def total(h, carry):
            v = u[0, head_rows(h), :] * d01[1, pl.ds(h, 1), :] + u[1, head_rows(h), :]
            for j in range(NZ):
                cs[j, h] = v[8 * j : 8 * j + 8, :].astype(BF)
            return carry

        lax.fori_loop(0, HEADS, total, 0, unroll=2)
        cr[z] = cs[z]

    carry1, carry2, carry3 = [], [], []

    def piece_carry1():
        for k in FAR_FIRST:
            carry1.append(extra(cs.at[zz(k)], cr.at[z], dev(dz=k), 10 + k))

    def piece_carry2():
        for q in carry1:
            q.wait_recv()
        run = jnp.zeros((HEADS, 8, 128), F32)
        for k in range(NZ):
            prefix[k] = run
            run = run * dec[k] + cr[k].astype(F32)
        tt[4] = run.astype(BF)
        tt[y] = run.astype(BF)
        for k in (2, 1, 3):
            carry2.append(extra(tt.at[4], tt.at[y], dev(dy=k), 17 + k))

    def piece_carry3():
        for q in carry2 + dec_copies[7:]:
            q.wait_recv()
        r = jnp.zeros((HEADS, 8, 128), F32)
        for k in range(NY - 1):
            r = jnp.where(y > k, r * rowd[k] + tt[k].astype(F32), r)
        for k in range(NZ):
            co[k] = (prefix[k] + r).astype(BF)
            r = r * dec[k]
        ci[z] = co[z]
        for k in FAR_FIRST:
            carry3.append(extra(co.at[zz(k)], ci.at[z], dev(dz=k), 20 + k))

    def piece_carry4():
        for q in carry3:
            q.wait_recv()

        def step(h, carry):
            v = jnp.concatenate([ci[j, h].astype(F32) for j in range(NZ)], axis=0)
            sbf[0, head_rows(h), :] = v.astype(BF)
            sbf[1, head_rows(h), :] = (v * d01[0, pl.ds(h, 1), :] + u[0, head_rows(h), :]).astype(BF)
            return carry

        lax.fori_loop(0, HEADS, step, 0)

    def piece_intra(b):
        s = slice(b * SPAN, (b + 1) * SPAN)

        def step(h, carry):
            v = vt[head_rows(h), s]
            yv[head_rows(h), s] = dot(v, mix[h, b]) + skip[h] * v.astype(F32)
            return carry

        lax.fori_loop(0, HEADS, step, 0, unroll=2)

    def piece_inter(r):
        rows = pl.ds(pl.multiple_of(r * 160, 160), 160)
        for b in range(2):
            s = slice(b * SPAN, (b + 1) * SPAN)
            joined[:, s] = dot(sbf[b, rows, :], ct[:, s])

        def step(i, carry):
            q = pl.multiple_of(i * 32, 32)
            row = pl.ds(pl.multiple_of(r * 160 + q, 32), 32)
            e = ecum[pl.ds((5 * r + i) // 2, 1), :]
            yv[row, :] = yv[row, :] + e * joined[pl.ds(q, 32), :]
            return carry

        lax.fori_loop(0, 5, step, 0, unroll=5)

    pair_copies, sq_copies = [], []
    sq[8] = jnp.zeros((8, TOK), F32)

    def piece_gated(r, slot):
        def step(i, total):
            q = pl.multiple_of(i * 32, 32)
            row = pl.ds(pl.multiple_of(r * 160 + q, 32), 32)
            g = gat[r, pl.ds(q, 32), :]
            v = yv[row, :] * (g * lax.logistic(g))
            for e in range(4):
                w = v[8 * e : 8 * e + 8, :]
                total = total + w * w
            scb[c, row, :] = (v * og[row, 0:1]).astype(BF)
            return total

        sq[8] = lax.fori_loop(0, 5, step, sq[8], unroll=5)
        own = scb.at[c, pl.ds(pl.multiple_of(r * 160, 160), 160)]
        pair_copies.append(extra(own, own, dev(dc=1), 28 + slot))

    def piece_squares():
        sq[grp] = sq[8]
        for k in range(1, 8):
            sq_copies.append(extra(sq.at[8], sq.at[grp], dev(dx=k // 2, dc=k % 2), 31 + k))

    def project(dx, half):
        s = slice(half * SPAN, (half + 1) * SPAN)
        p = xx(dx)
        return dot(wr[p, :, 0:CH], scb[0, :, s]) + dot(wr[p, :, CH : 2 * CH], scb[1, :, s])

    def piece_gains():
        term[...] = jnp.zeros((128, TOK), F32)
        for q in range(CH // 128):
            cols = slice(q * 128, q * 128 + 128)
            term[0:4, 0:128] = cw_in[:, cols].astype(F32)
            cwin[cols, :] = term[:, 0:128].T
            og[cols, :] = jnp.broadcast_to(og_in[cols].reshape(1, 128), (128, 128)).T

    def call(piece, *args):
        with jax.named_scope(piece.__name__ + "".join(f"#i={a}" for a in args if isinstance(a, int))):
            return piece(*args)

    def mul(h, rel, route):
        complete(h, rel, route)
        piece_mul(h, rel, route)

    def conv(rel):
        unfold(rel, inn, 640)
        piece_conv(yy(rel))

    does = {
        "norm": piece_norm,
        "halo": piece_halo,
        "gains": piece_gains,
        "transpose": piece_transpose,
        "state_weight": piece_state_weight,
        "state": piece_state,
        "state_conv": piece_state_conv,
        "delta": piece_delta,
        "scores": piece_scores,
        "dec_send": piece_dec_send,
        "dec_recv": piece_dec_recv,
        "mix": piece_mix,
        "mul": mul,
        "conv": conv,
        "update": piece_update,
        "carry1": piece_carry1,
        "carry2": piece_carry2,
        "carry3": piece_carry3,
        "carry4": piece_carry4,
        "intra": piece_intra,
        "inter": lambda rel: piece_inter(yy(rel)),
        "gate": lambda rel: unfold(rel, gat, TOK),
        "gated": lambda rel: piece_gated(yy(rel), rel + 1),
    }
    for what, k in PROGRAM:
        if what == "issue":
            issue(k)
        else:
            with jax.named_scope("#".join(str(e) for e in k)):
                does[k[0]](*k[1:])
    call(piece_squares)
    with jax.named_scope("wait_weights"):
        own_out.wait()
        for k in (("X1", 1), ("X1", -1), ("X2f", 1), ("X2f", -1)):
            take(k)
    with jax.named_scope("wait_pair"):
        for q in pair_copies:
            q.wait_recv()

    top, low = slice(0, 160), slice(160, 320)
    far, near = {}, []

    def send_far(half):
        got = call(project, 2, half)
        rs_out[half] = got.astype(BF)
        for i, d in enumerate((1, -1)):
            rows = pl.ds(160 * i, 160)
            far[half, d] = extra(
                rs_out.at[half, rows], rs_in1.at[half, rows], dev(dx=d), 40 + 2 * half + i
            )

    def send_direct(half):
        for i, d in enumerate((1, -1)):
            keep[i] = call(project, d, half)
            rows = low if d == 1 else top
            rs2_out[i, half, rows] = keep[i, rows].astype(BF)
            rows = pl.ds(160 * (1 - i), 160)
            part = (i, half, rows)
            near.append(extra(rs2_out.at[part], rs2_in.at[part], dev(dx=d), 44 + 4 * half + i))

    def send_relayed(half):
        for i, d in enumerate((1, -1)):
            with jax.named_scope("wait_far"):
                far[half, d].wait_recv()
            rows = top if d == 1 else low
            rs2_out[i, half, rows] = (keep[i, rows] + rs_in1[half, rows].astype(F32)).astype(BF)
            rows = pl.ds(160 * i, 160)
            part = (i, half, rows)
            near.append(extra(rs2_out.at[part], rs2_in.at[part], dev(dx=d), 46 + 4 * half + i))

    send_far(0)
    send_direct(0)
    send_far(1)
    send_relayed(0)
    send_direct(1)
    own_p[0] = call(project, 0, 0)
    send_relayed(1)
    own_p[1] = call(project, 0, 1)
    with jax.named_scope("wait_sq"):
        for q in sq_copies:
            q.wait_recv()
    total = sq[0]
    for k in range(1, 8):
        total = total + sq[k]
    total = jnp.sum(total, axis=0, keepdims=True)
    scale = lax.rsqrt(total / (8 * CH) + EPS)
    for half in range(2):
        with jax.named_scope("wait_near"):
            for q in near[4 * half : 4 * half + 4]:
                q.wait_recv()
        v = own_p[half] + rs2_in[0, half].astype(F32) + rs2_in[1, half].astype(F32)
        s = slice(half * SPAN, (half + 1) * SPAN)
        out[:, s] = (v * scale[:, s]).astype(BF)
    with jax.named_scope("wait_sends"):
        for k in MSGS:
            message(k).wait_send()
    for q in extra_sends:
        q.wait_send()


def run(*args):
    vm = pl.BlockSpec(memory_space=pltpu.VMEM)
    specs = [pl.BlockSpec(memory_space=pl.ANY)] * 12
    V = pltpu.VMEM
    scratch = [
        V((D,), F32),
        V((20, 2, D), BF),
        V((HEADS, D), BF),
        pltpu.SMEM((HEADS,), F32),
        pltpu.SMEM((HEADS,), F32),
        pltpu.SMEM((HEADS,), F32),
        V((4, CH), BF),
        V((4, 2, 128), BF),
        V((CH,), F32),
        V((TOK, D), BF),
        V((2, 40, KA), BF),
        V((2, 40, KB), BF),
        V((2, 40, D // 2), F32),
        V((D, 2, 128), BF),
        V((D, 256), BF),
        V((CH, 128), F32),
        V((CH, 128), F32),
        V((2, NY, NZ, 40, KA), BF),
        V((2, NY, NZ, 40, KB), BF),
        V((640, D), BF),
        V((D, 640), BF),
        V((528, 256), F32),
        V((TOK, 128), BF),
        V((128, TOK), BF),
        V((9, HEADS, 1, 128), F32),
        V((HEADS, TOK), F32),
        V((HEADS, TOK), F32),
        V((HEADS, TOK), F32),
        V((2, HEADS, 128), F32),
        V((2, SPAN, SPAN), F32),
        V((HEADS, 2, SPAN, SPAN), BF),
        V((128, TOK), F32),
        V((TOK, 128), F32),
        V((4, 160, 640), F32),
        V((160, TOK), F32),
        V((NY, 160, 640), F32),
        V((NY, 160, TOK), F32),
        V((CH, TOK), BF),
        V((CH, TOK), BF),
        V((2, CH, 128), F32),
        V((CH, TOK), F32),
        V((NZ, HEADS, 8, 128), BF),
        V((NZ, HEADS, 8, 128), BF),
        V((NZ, HEADS, 8, 128), BF),
        V((NZ, HEADS, 8, 128), BF),
        V((5, HEADS, 8, 128), BF),
        V((5, HEADS, 1, 128), F32),
        V((NZ, HEADS, 8, 128), F32),
        V((2, CH, 128), BF),
        V((2, CH, TOK), BF),
        V((NX, FEAT, 1280), BF),
        V((2, FEAT, 640), BF),
        V((9, 8, TOK), F32),
        V((2, FEAT, SPAN), BF),
        V((2, FEAT, SPAN), BF),
        V((2, 2, FEAT, SPAN), BF),
        V((2, 2, FEAT, SPAN), BF),
        V((2, FEAT, SPAN), F32),
        V((2, FEAT, SPAN), F32),
        V((16, D), BF),
        pltpu.SemaphoreType.DMA((N_MSG,)),
        pltpu.SemaphoreType.DMA((N_MSG,)),
        pltpu.SemaphoreType.DMA((52,)),
        pltpu.SemaphoreType.DMA((52,)),
        pltpu.SemaphoreType.DMA((15,)),
    ]
    return pl.pallas_call(
        kernel,
        out_shape=jax.ShapeDtypeStruct((FEAT, TOK), BF),
        in_specs=specs,
        out_specs=vm,
        scratch_shapes=scratch,
        compiler_params=pltpu.CompilerParams(
            collective_id=0, has_side_effects=True, vmem_limit_bytes=64 * 2**20 - 65536
        ),
        name="layer",
    )(*args)


def body(
    tokens, norm_gain, inner_weight, state_weight, step_weight, step_bias, decay_rate,
    skip_scale, conv_inner, conv_state, out_gain, out_weight,
):
    return run(
        tokens, norm_gain, inner_weight.transpose(2, 1, 0), state_weight, step_weight.T,
        step_bias, decay_rate, skip_scale, conv_inner, conv_state, out_gain, out_weight.T,
    ).T


def solution(mesh):
    return jax.shard_map(
        body,
        mesh=mesh,
        in_specs=(
            P("seq", None), P(), P(None, None, ("grp", "seq")), P(), P(None, "grp"), P("grp"),
            P("grp"), P("grp"), P(None, "grp"), P(), P("grp"), P(None, "grp"),
        ),
        out_specs=P("seq", "grp"),
        check_vma=False,
    )
```

```python
import functools

import jax
import jax.numpy as jnp
from jax import lax
from jax.experimental import pallas as pl
from jax.experimental.pallas import tpu as pltpu
from jax.sharding import PartitionSpec as P

MESH = pl.DeviceIdType.MESH
BF = jnp.bfloat16
F32 = jnp.float32
EPS = 1e-05

TOK = 512
D = 2560
CH = 640
HEADS = 10
SPAN = 256
KA, KB = 512, 768
FEAT = 320
NY, NZ, NX = 4, 8, 4


def dot(a, b):
    return jnp.dot(a, b, preferred_element_type=F32)


def half_messages(h):
    m = {}
    for d in (1, -1):
        m["Ay", h, d] = (("y", d), 0.88, [])
        m["Ay2", h, d] = (("y", d), 0.44, [("Ay", h, d)])
        for k in range(1, 5):
            rels = (0, -1, 1, 2) if k < 4 else ((0, -1) if d == 1 else (1, 2))
            for rel in rels:
                if k > 1:
                    dep = [("Az", h, d, k - 1, rel)]
                else:
                    dep = {
                        0: [],
                        -1: [("Ay", h, 1)],
                        1: [("Ay", h, -1)],
                        2: [("Ay2", h, 1), ("Ay2", h, -1)],
                    }[rel]
                m["Az", h, d, k, rel] = (("z", d), 0.88, dep)
            dep = [("Bz", h, d, k - 1)] if k > 1 else []
            m["Bz", h, d, k] = (("z", d), 1.32 if k < 4 else 0.66, dep)
        for zr in range(-3, 5):
            if zr == 0:
                dep = []
            elif zr == 4:
                dep = [("Bz", h, 1, 4), ("Bz", h, -1, 4)]
            else:
                dep = [("Bz", h, 1, -zr)] if zr < 0 else [("Bz", h, -1, zr)]
            m["By", h, d, zr] = (("y", d), 1.32, dep)
            if (zr <= 0) == (d == 1):
                m["By2", h, d, zr] = (("y", d), 1.32, [("By", h, d, zr)])
    return m


def row_of(k):
    kind = k[0]
    if kind == "Bz":
        return 0
    if kind in ("Ay", "By"):
        return -k[2]
    return k[4] if kind == "Az" else 2


SLOWER = 1.12
LATENCY = 2.4
AHEAD = (1.2, 0.3)
GATE_FROM = 0.0
RELS = (0, -1, 1, 2)
FAR_FIRST = (4, 3, 5, 2, 6, 1, 7)


def build_messages():
    msgs = {}
    for d in (1, -1):
        msgs["X2", d] = (("x", d), 8.8, [])
        msgs["X1", d] = (("x", d), 17.6, [])
        msgs["X2f", d] = (("x", d), 8.8, [("X2", d)])
    for h in (0, 1):
        msgs.update(half_messages(h))
    return msgs


def build_pieces():
    p = {}

    def add(name, cost, after=(), rows=(), sends=(), delay=0.0):
        p[name] = (cost, list(after), list(rows), list(sends), delay)

    z_swap = [(("z", 1), 2.5), (("z", -1), 2.5)]
    y_swap = [(("y", 1), 0.9), (("y", -1), 0.9)]
    add(("carry4",), 0.5, [("carry3",)])
    add(("carry3",), 0.5, [("carry2",), ("dec_recv",)], (), z_swap, 2.5)
    add(("carry2",), 0.4, [("carry1",), ("dec_recv",)], (), y_swap, 2.6)
    add(("carry1",), 0.1, [("update",)], (), z_swap, 2.5)
    convs = [("conv", rel) for rel in RELS]
    add(("update",), 0.5, convs + [("delta",), ("state_conv",)])
    ready = [("transpose", i) for i in range(5)]
    for rel in RELS:
        add(("conv", rel), 0.4, [("mul", 0, rel, "A"), ("mul", 0, rel, "B"), ("gains",)])
        add(("mul", 0, rel, "A"), 0.44, ready, [(0, rel, "A")])
        add(("mul", 0, rel, "B"), 0.58, ready, [(0, rel, "B")])
    for i in range(4):
        add(("norm", i), 0.56)
    add(("halo",), 0.3, [("norm", 3)], (), (), 0.0)
    for i in range(5):
        add(("transpose", i), 0.42, [("halo",)])
    add(("gains",), 0.2, [("norm", 3)])
    for i in range(4):
        add(("state_weight", i), 0.48, ready)
    for i in range(3):
        add(("state", i), 0.6, [("state_weight", e) for e in range(4)])
    add(("state_conv",), 0.4, [("state", i) for i in range(3)])
    add(("delta",), 1.2, ready + [("gains",)])
    add(("scores",), 0.3, [("state_conv",)])
    add(("dec_send",), 0.1, [("delta",)], (), (), 5.0)
    for i in range(HEADS):
        add(("mix", i), 0.16, [("delta",), ("scores",)])
    add(("dec_recv",), 0.2, [("dec_send",)], (), (), 3.5)
    mixes = [("mix", i) for i in range(HEADS)]
    for rel in RELS:
        add(("gated", rel), 0.12, [("inter", rel), ("gate", rel)])
        add(("gate", rel), 0.05, [("mul", 1, rel, "A"), ("mul", 1, rel, "B")])
        add(("inter", rel), 0.2, [("carry4",), ("intra", 0), ("intra", 1)])
    for i in range(2):
        add(("intra", i), 0.9, mixes + convs)
    for rel in RELS:
        add(("mul", 1, rel, "A"), 0.35, [("conv", rel)], [(1, rel, "A")])
        add(("mul", 1, rel, "B"), 0.32, [("conv", rel)], [(1, rel, "B")])
    return p


def build_program():
    msgs, pieces = build_messages(), build_pieces()
    order = {k: i for i, k in enumerate(msgs)}

    def rank(k):
        if k[0][0] == "X":
            return (0, 9 if k[0] == "X1" else 0, order[k])
        if k[0] in ("Bz", "Ay"):
            p = 0
        elif k[0] == "Ay2":
            p = 0.5
        elif k[0] == "Az":
            p = 1 + k[3] + (0, 0.2, 0.4)[abs(k[4])]
        else:
            p = 1 + abs(k[3]) + (2 if k[0] == "By2" else 0)
        return (k[1], p, order[k])

    arrived, done, free, program = {}, {}, {}, []
    todo = sorted(msgs, key=rank)
    work = list(pieces)
    now = 0.0
    rows = {}
    for k in msgs:
        if k[0][0] in "AB":
            rows.setdefault((k[1], row_of(k), k[0][0]), []).append(k)
    while todo or work:
        moved = True
        while moved:
            moved = False
            for k in todo:
                link, dur, deps = msgs[k]
                later = k[0][0] != "X" and k[1] == 1
                if free.get(link, 0.0) > now + AHEAD[later] or (later and now < GATE_FROM):
                    continue
                if any(arrived.get(q, 1e9) > now for q in deps):
                    continue
                start = max(now, free.get(link, 0.0))
                free[link] = start + dur * SLOWER
                arrived[k] = free[link] + LATENCY
                program.append(("issue", k))
                todo.remove(k)
                now += 0.02
                moved = True
                break
        for name in work:
            cost, after, need, sends, delay = pieces[name]
            if any(done.get(q, 1e9) > now for q in after):
                continue
            if any(arrived.get(k, 1e9) > now for e in need for k in rows[e]):
                continue
            program.append(("piece", name))
            work.remove(name)
            now += cost
            end = now
            for link, dur in sends:
                free[link] = max(now, free.get(link, 0.0)) + dur * SLOWER
                end = max(end, free[link])
            done[name] = end + delay
            break
        else:
            now += 0.05
    return msgs, program, done, arrived


MSGS, PROGRAM, DONE, ARRIVED = build_program()
IDS = {k: i for i, k in enumerate(MSGS)}
N_MSG = len(MSGS)


def kernel(
    tok_in, gain_in, own_w, sw_in, st_in, bias_in, rate_in, skip_in, cw_w, cwst_in, og_w, ow,
    out,
    gain, own_in, st, bias, rate, skip, cw_in, cwst, og_in,
    tok, own_a, own_b, own_f, sw, swd, cwin, og, wa, wb, nrm, nt, spf, cb, ct, dec, cum, ecum, tailw, d01, scores, mix, term, colt,
    acc, joined, inn, gat, vt, vw, u, yv, cs, cr, co, ci, tt, rowd, lead, prefix,
    sbf, scb, wr, relay, sq, rs_out, rs_in1, rs2_out, rs2_in, keep, own_p,
    halo, send, recv, xsend, xrecv, lsem,
):
    seq = lax.axis_index("seq")
    grp = lax.axis_index("grp")
    y, z = seq // NZ, lax.rem(seq, NZ)
    x, c = grp // 2, lax.rem(grp, 2)

    def yy(d):
        return lax.rem(y + d + NY, NY)

    def zz(d):
        return lax.rem(z + d + NZ, NZ)

    def xx(d):
        return lax.rem(x + d + NX, NX)

    def dev(dy=0, dz=0, dx=0, dc=0):
        return (yy(dy) * NZ + zz(dz), xx(dx) * 2 + lax.rem(c + dc, 2))

    nxt = (lax.rem(seq + 1, NY * NZ), grp)
    prv = (lax.rem(seq + NY * NZ - 1, NY * NZ), grp)

    barrier = pltpu.get_barrier_semaphore()
    peers = [nxt, prv]
    peers += [dev(dz=k) for k in range(1, NZ)]
    peers += [dev(dy=k) for k in range(1, NY)]
    peers += [dev(dx=k // 2, dc=k % 2) for k in range(1, 8)]
    for p in peers:
        pl.semaphore_signal(barrier, inc=1, device_id=p, device_id_type=MESH)

    def feature_columns(d, first, count):
        return ow.at[:, pl.ds(pl.multiple_of(xx(d) * 1280 + first, 128), count)]

    own_copy = pltpu.make_async_copy(own_w, own_in, lsem.at[6])
    own_copy.start()
    small = ((gain_in, gain), (st_in, st), (bias_in, bias), (rate_in, rate), (skip_in, skip),
             (cw_w, cw_in), (cwst_in, cwst), (og_w, og_in))
    small_copies = [pltpu.make_async_copy(a, b, lsem.at[7 + i]) for i, (a, b) in enumerate(small)]
    for q in small_copies:
        q.start()
    tok_copies = []
    for q in range(4):
        part = pl.ds(q * 128, 128)
        tok_copies.append(pltpu.make_async_copy(tok_in.at[part], tok.at[part], lsem.at[q]))
        tok_copies[q].start()
    sw_copy = pltpu.make_async_copy(sw_in, sw, lsem.at[4])
    sw_copy.start()
    own_out = pltpu.make_async_copy(feature_columns(0, 0, 1280), wr.at[x], lsem.at[5])
    own_out.start()
    own_copy.wait()
    for r in range(20):
        v = own_in[r].astype(F32)
        for h in (0, 1):
            for part in (0, 1):
                own_f[h, 20 * part + r : 20 * part + r + 1, :] = v[
                    h : h + 1, part * (D // 2) : (part + 1) * (D // 2)
                ]
    for h in (0, 1):
        v = own_f[h].astype(BF)
        own_a[h] = v[:, :KA]
        own_b[h] = v[:, KA:]
        wa[h, y, z] = v[:, :KA]
        wb[h, y, z] = v[:, KA:]
    nrm[0:128, :] = jnp.zeros((128, D), BF)
    for q in small_copies:
        q.wait()
    with jax.named_scope("barrier"):
        pl.semaphore_wait(barrier, len(peers))

    def remote(src, dst, s, r, to):
        return pltpu.make_async_remote_copy(
            src_ref=src, dst_ref=dst, send_sem=s, recv_sem=r, device_id=to, device_id_type=MESH
        )

    def message(k):
        i = IDS[k]
        kind = k[0]
        if kind[0] == "X":
            d = k[1]
            if kind == "X1":
                src, dst = feature_columns(d, 0, 1280), wr.at[x]
            elif kind == "X2":
                off = 0 if d == 1 else 640
                src = feature_columns(2, off, 640)
                dst = relay.at[0 if d == 1 else 1]
            else:
                off = 0 if d == 1 else 640
                src = relay.at[0 if d == 1 else 1]
                dst = wr.at[xx(-d), :, pl.ds(off, 640)]
            return remote(src, dst, send.at[i], recv.at[i], dev(dx=d))
        h, d = k[1], k[2]
        if kind == "Ay":
            src, dst, to = own_a.at[h], wa.at[h, y, z], dev(dy=d)
        elif kind == "Ay2":
            cols = pl.ds(0 if d == 1 else KA // 2, KA // 2)
            src = dst = wa.at[h, yy(-d), z, :, cols]
            to = dev(dy=d)
        elif kind == "Az":
            step, rel = k[3], k[4]
            dst = wa.at[h, yy(rel), zz(-d * (step - 1))]
            src = own_a.at[h] if (step == 1 and rel == 0) else dst
            to = dev(dz=d)
        elif kind == "Bz":
            step = k[3]
            dst = wb.at[h, y, zz(-d * (step - 1))]
            src = own_b.at[h] if step == 1 else dst
            if step == 4:
                cols = pl.ds(0 if d == 1 else KB // 2, KB // 2)
                src = dst = wb.at[h, y, zz(-d * 3), :, cols]
            to = dev(dz=d)
        elif kind == "By":
            zr = k[3]
            dst = wb.at[h, y, zz(zr)]
            src = own_b.at[h] if zr == 0 else dst
            to = dev(dy=d)
        else:
            src = dst = wb.at[h, yy(-d), zz(k[3])]
            to = dev(dy=d)
        return remote(src, dst, send.at[i], recv.at[i], to)

    waited = set()
    def take(k):
        if k not in waited:
            waited.add(k)
            message(k).wait_recv()

    def issue(k):
        for q in MSGS[k][2]:
            take(q)
        message(k).start()

    def complete(h, rel, route):
        for k in MSGS:
            if k[0][0] == route and k[1] == h and row_of(k) == rel:
                take(k)

    extra_sends = []

    def extra(src, dst, to, slot):
        q = remote(src, dst, xsend.at[slot], xrecv.at[slot], to)
        q.start()
        extra_sends.append(q)
        return q

    halo_copy = extra(tok_in.at[pl.ds(TOK - 16, 16)], halo, nxt, 0)

    def norm_rows(v):
        wide = v.astype(F32)
        ms = jnp.mean(wide * wide, axis=1, keepdims=True)
        return wide * lax.rsqrt(ms + EPS) * gain[...].reshape(1, D)

    def piece_norm(part):
        tok_copies[part].wait()

        def step(i, carry):
            r = pl.multiple_of(part * 128 + i * 16, 16)
            nrm[pl.ds(128 + r, 16), :] = norm_rows(tok[pl.ds(r, 16), :]).astype(BF)
            return carry

        lax.fori_loop(0, 8, step, 0, unroll=2)

    def piece_halo():
        halo_copy.wait_recv()
        n = jnp.where(seq > 0, norm_rows(halo[...]), 0.0)
        nrm[112:128, :] = n.astype(BF)

    def piece_transpose(tb):
        def step(i, carry):
            k = pl.multiple_of(i * 128, 128)
            nt[pl.ds(k, 128), tb * 128 : (tb + 1) * 128] = nrm[
                tb * 128 : (tb + 1) * 128, pl.ds(k, 128)
            ].T
            return carry

        lax.fori_loop(0, D // 128, step, 0, unroll=5)

    def piece_state_weight(part):
        if part == 0:
            sw_copy.wait()

        def step(i, carry):
            r = pl.multiple_of(i * 128 + part * 640, 128)
            v = sw[pl.ds(r, 128), :, :].astype(F32)
            swd[pl.ds(r, 128), 0:128] = v[:, 0, :].astype(BF)
            swd[pl.ds(r, 128), 128:256] = v[:, 1, :].astype(BF)
            return carry

        lax.fori_loop(0, 5, step, 0)

    def piece_state(part):
        r = part * 176
        got = dot(nrm[112 + r : 112 + r + 176, :], swd[...])
        spf[r : r + 176, :] = got.astype(BF).astype(F32)

    def piece_state_conv():
        for q in range(4):
            for k in (0, 1):
                acc = jnp.zeros((128, 128), F32)
                for j in range(4):
                    first = q * 128 + 13 + j
                    w = cwst[j].astype(F32)[k : k + 1, :]
                    acc = acc + w * spf[first : first + 128, k * 128 : (k + 1) * 128]
                v = acc * lax.logistic(acc)
                if k == 0:
                    cb[q * 128 : (q + 1) * 128, :] = v.astype(BF)
                else:
                    ct[:, q * 128 : (q + 1) * 128] = v.T.astype(BF)

    def piece_delta():
        row = lax.broadcasted_iota(jnp.int32, (HEADS, TOK), 0)
        bias_col = rate_col = jnp.zeros((HEADS, TOK), F32)
        for h in range(HEADS):
            bias_col = jnp.where(row == h, bias[h], bias_col)
            rate_col = jnp.where(row == h, rate[h], rate_col)
        pre = dot(st[...], nt[:, 128:640]) + bias_col
        delta = jnp.maximum(pre, 0.0) + jnp.log1p(jnp.exp(-jnp.abs(pre)))
        run = -delta * rate_col
        lane = lax.broadcasted_iota(jnp.int32, (HEADS, TOK), 1) % SPAN
        k = 1
        while k < SPAN:
            run = run + jnp.where(lane >= k, pltpu.roll(run, k, 1), 0.0)
            k *= 2
        cum[...] = run
        ecum[...] = jnp.exp(run)
        tot0, tot1 = run[:, 255:256], run[:, 511:512]
        tailw[:, :SPAN] = jnp.exp(tot0 - run[:, :SPAN]) * delta[:, :SPAN]
        tailw[:, SPAN:] = jnp.exp(tot1 - run[:, SPAN:]) * delta[:, SPAN:]
        d01[0] = jnp.broadcast_to(jnp.exp(tot0), (HEADS, 128))
        d01[1] = jnp.broadcast_to(jnp.exp(tot1), (HEADS, 128))
        whole = jnp.broadcast_to(jnp.exp(tot0) * jnp.exp(tot1), (HEADS, 128))
        for h in range(HEADS):
            dec[8, h] = whole[h : h + 1, :]
            dec[z, h] = whole[h : h + 1, :]
        term[...] = jnp.zeros((128, TOK), F32)
        term[0:HEADS, :] = jnp.log(delta) - run
        for q in range(4):
            colt[q * 128 : (q + 1) * 128, :] = term[:, q * 128 : (q + 1) * 128].T

    def piece_scores():
        for b in range(2):
            s = slice(b * SPAN, (b + 1) * SPAN)
            scores[b] = dot(cb[s, :], ct[:, s])

    dec_copies = []

    def piece_dec_send():
        for k in range(1, NZ):
            dec_copies.append(extra(dec.at[8], dec.at[z], dev(dz=k), k))

    def piece_dec_recv():
        for q in dec_copies:
            q.wait_recv()
        prod = jnp.ones((HEADS, 1, 128), F32)
        for k in range(NZ):
            lead[k] = prod
            prod = prod * dec[k]
        rowd[4] = prod
        rowd[y] = prod
        for k in range(1, NY):
            dec_copies.append(extra(rowd.at[4], rowd.at[y], dev(dy=k), 7 + k))

    def piece_mix(h):
        keep = lax.broadcasted_iota(jnp.int32, (128, 128), 1) >= lax.broadcasted_iota(
            jnp.int32, (128, 128), 0
        )
        for b in range(2):
            for s0 in range(2):
                r = b * SPAN + s0 * 128
                col = jnp.broadcast_to(colt[r : r + 128, h : h + 1], (128, 128))
                for t0 in range(2):
                    sl = (slice(s0 * 128, s0 * 128 + 128), slice(t0 * 128, t0 * 128 + 128))
                    if t0 < s0:
                        mix[(h, b) + sl] = jnp.zeros((128, 128), BF)
                        continue
                    q = b * SPAN + t0 * 128
                    arg = col + cum[h : h + 1, q : q + 128]
                    if s0 == t0:
                        arg = jnp.where(keep, arg, -jnp.inf)
                    mix[(h, b) + sl] = (scores[(b,) + sl] * jnp.exp(arg)).astype(BF)

    begun = set()

    def piece_mul(h, rel, route):
        i = RELS.index(rel)
        held, k0, kn = (wa, 0, KA) if route == "A" else (wb, KA, KB)
        whole = [held[h, yy(rel), q] for q in range(NZ)]
        lhs = [
            jnp.concatenate([v[20 * e : 20 * e + 20, :] for v in whole], axis=0) for e in (0, 1)
        ]
        for cols in (slice(0, 256), slice(256, 512), slice(512, 640))[: 3 - h]:
            n = slice(128 * h + cols.start, 128 * h + cols.stop)
            v = dot(lhs[0], nt[k0 : k0 + kn, n]) + dot(lhs[1], nt[1280 + k0 : 1280 + k0 + kn, n])
            if (h, rel) in begun:
                acc[i, :, cols] += v
            else:
                acc[i, :, cols] = v
        begun.add((h, rel))

    def unfold(rel, into, width):
        i, r = RELS.index(rel), yy(rel)
        into[r] = acc[i, :, :width].astype(BF).astype(F32)

    def piece_conv(r):
        def step(i, carry):
            q = pl.multiple_of(i * 32, 32)
            row = pl.multiple_of(r * 160 + q, 32)
            v = inn[r, pl.ds(q, 32), :]
            w = cwin[pl.ds(row, 32), :]
            acc = w[:, 3:4] * v[:, 128:]
            for j in range(3):
                acc = acc + w[:, j : j + 1] * pltpu.roll(v, 3 - j, 1)[:, 128:]
            vt[pl.ds(row, 32), :] = (acc * lax.logistic(acc)).astype(BF)
            return carry

        lax.fori_loop(0, 5, step, 0, unroll=5)

    def head_rows(h):
        return pl.ds(pl.multiple_of(h * 64, 64), 64)

    def piece_update():
        def weigh(h, carry):
            vw[head_rows(h), :] = (vt[head_rows(h), :].astype(F32) * tailw[pl.ds(h, 1), :]).astype(BF)
            return carry

        lax.fori_loop(0, HEADS, weigh, 0, unroll=2)
        for b in range(2):
            s = slice(b * SPAN, (b + 1) * SPAN)
            u[b] = dot(vw[:, s], cb[s, :])

        def total(h, carry):
            v = u[0, head_rows(h), :] * d01[1, pl.ds(h, 1), :] + u[1, head_rows(h), :]
            for j in range(NZ):
                cs[j, h] = v[8 * j : 8 * j + 8, :].astype(BF)
            return carry

        lax.fori_loop(0, HEADS, total, 0, unroll=2)
        cr[z] = cs[z]

    carry1, carry2, carry3 = [], [], []

    def piece_carry1():
        for k in FAR_FIRST:
            carry1.append(extra(cs.at[zz(k)], cr.at[z], dev(dz=k), 10 + k))

    def piece_carry2():
        for q in carry1:
            q.wait_recv()
        run = jnp.zeros((HEADS, 8, 128), F32)
        for k in range(NZ):
            prefix[k] = run
            run = run * dec[k] + cr[k].astype(F32)
        tt[4] = run.astype(BF)
        tt[y] = run.astype(BF)
        for k in (2, 1, 3):
            carry2.append(extra(tt.at[4], tt.at[y], dev(dy=k), 17 + k))

    def piece_carry3():
        for q in carry2 + dec_copies[7:]:
            q.wait_recv()
        r = jnp.zeros((HEADS, 8, 128), F32)
        for k in range(NY - 1):
            r = jnp.where(y > k, r * rowd[k] + tt[k].astype(F32), r)
        for k in FAR_FIRST:
            co[zz(k)] = (prefix[zz(k)] + r * lead[zz(k)]).astype(BF)
            carry3.append(extra(co.at[zz(k)], ci.at[z], dev(dz=k), 20 + k))

        ci[z] = (prefix[z] + r * lead[z]).astype(BF)

    def piece_carry4():
        for q in carry3:
            q.wait_recv()

        def step(h, carry):
            v = jnp.concatenate([ci[j, h].astype(F32) for j in range(NZ)], axis=0)
            sbf[0, head_rows(h), :] = v.astype(BF)
            sbf[1, head_rows(h), :] = (v * d01[0, pl.ds(h, 1), :] + u[0, head_rows(h), :]).astype(BF)
            return carry

        lax.fori_loop(0, HEADS, step, 0)

    def piece_intra(b):
        s = slice(b * SPAN, (b + 1) * SPAN)

        def step(h, carry):
            v = vt[head_rows(h), s]
            yv[head_rows(h), s] = dot(v, mix[h, b]) + skip[h] * v.astype(F32)
            return carry

        lax.fori_loop(0, HEADS, step, 0, unroll=2)

    def piece_inter(r):
        rows = pl.ds(pl.multiple_of(r * 160, 160), 160)
        for b in range(2):
            s = slice(b * SPAN, (b + 1) * SPAN)
            joined[:, s] = dot(sbf[b, rows, :], ct[:, s])

        def step(i, carry):
            q = pl.multiple_of(i * 32, 32)
            row = pl.ds(pl.multiple_of(r * 160 + q, 32), 32)
            e = ecum[pl.ds((5 * r + i) // 2, 1), :]
            yv[row, :] = yv[row, :] + e * joined[pl.ds(q, 32), :]
            return carry

        lax.fori_loop(0, 5, step, 0, unroll=5)

    pair_copies, sq_copies = [], []
    sq[8] = jnp.zeros((8, TOK), F32)

    def piece_gated(r, slot):
        def step(i, total):
            q = pl.multiple_of(i * 32, 32)
            row = pl.ds(pl.multiple_of(r * 160 + q, 32), 32)
            g = gat[r, pl.ds(q, 32), :]
            v = yv[row, :] * (g * lax.logistic(g))
            for e in range(4):
                w = v[8 * e : 8 * e + 8, :]
                total = total + w * w
            scb[c, row, :] = (v * og[row, 0:1]).astype(BF)
            return total

        sq[8] = lax.fori_loop(0, 5, step, sq[8], unroll=5)
        own = scb.at[c, pl.ds(pl.multiple_of(r * 160, 160), 160)]
        pair_copies.append(extra(own, own, dev(dc=1), 28 + slot))

    def piece_squares():
        sq[grp] = sq[8]
        for k in range(1, 8):
            sq_copies.append(extra(sq.at[8], sq.at[grp], dev(dx=k // 2, dc=k % 2), 31 + k))

    def project(dx, half):
        s = slice(half * SPAN, (half + 1) * SPAN)
        p = xx(dx)
        return dot(wr[p, :, 0:CH], scb[0, :, s]) + dot(wr[p, :, CH : 2 * CH], scb[1, :, s])

    def piece_gains():
        term[...] = jnp.zeros((128, TOK), F32)
        for q in range(CH // 128):
            cols = slice(q * 128, q * 128 + 128)
            term[0:4, 0:128] = cw_in[:, cols].astype(F32)
            cwin[cols, :] = term[:, 0:128].T
            og[cols, :] = jnp.broadcast_to(og_in[cols].reshape(1, 128), (128, 128)).T

    def call(piece, *args):
        with jax.named_scope(piece.__name__ + "".join(f"#i={a}" for a in args if isinstance(a, int))):
            return piece(*args)

    def mul(h, rel, route):
        complete(h, rel, route)
        piece_mul(h, rel, route)

    def conv(rel):
        unfold(rel, inn, 640)
        piece_conv(yy(rel))

    does = {
        "norm": piece_norm,
        "halo": piece_halo,
        "gains": piece_gains,
        "transpose": piece_transpose,
        "state_weight": piece_state_weight,
        "state": piece_state,
        "state_conv": piece_state_conv,
        "delta": piece_delta,
        "scores": piece_scores,
        "dec_send": piece_dec_send,
        "dec_recv": piece_dec_recv,
        "mix": piece_mix,
        "mul": mul,
        "conv": conv,
        "update": piece_update,
        "carry1": piece_carry1,
        "carry2": piece_carry2,
        "carry3": piece_carry3,
        "carry4": piece_carry4,
        "intra": piece_intra,
        "inter": lambda rel: piece_inter(yy(rel)),
        "gate": lambda rel: unfold(rel, gat, TOK),
        "gated": lambda rel: piece_gated(yy(rel), rel + 1),
    }
    for what, k in PROGRAM:
        if what == "issue":
            issue(k)
        else:
            with jax.named_scope("#".join(str(e) for e in k)):
                does[k[0]](*k[1:])
    call(piece_squares)
    with jax.named_scope("wait_weights"):
        own_out.wait()
        for k in (("X1", 1), ("X1", -1), ("X2f", 1), ("X2f", -1)):
            take(k)
    with jax.named_scope("wait_pair"):
        for q in pair_copies:
            q.wait_recv()

    top, low = slice(0, 160), slice(160, 320)
    far, near = {}, []

    def send_far(half):
        got = call(project, 2, half)
        rs_out[half] = got.astype(BF)
        for i, d in enumerate((1, -1)):
            rows = pl.ds(160 * i, 160)
            far[half, d] = extra(
                rs_out.at[half, rows], rs_in1.at[half, rows], dev(dx=d), 40 + 2 * half + i
            )

    def send_direct(half):
        for i, d in enumerate((1, -1)):
            keep[i] = call(project, d, half)
            rows = low if d == 1 else top
            rs2_out[i, half, rows] = keep[i, rows].astype(BF)
            rows = pl.ds(160 * (1 - i), 160)
            part = (i, half, rows)
            near.append(extra(rs2_out.at[part], rs2_in.at[part], dev(dx=d), 44 + 4 * half + i))

    def send_relayed(half):
        for i, d in enumerate((1, -1)):
            with jax.named_scope("wait_far"):
                far[half, d].wait_recv()
            rows = top if d == 1 else low
            rs2_out[i, half, rows] = (keep[i, rows] + rs_in1[half, rows].astype(F32)).astype(BF)
            rows = pl.ds(160 * i, 160)
            part = (i, half, rows)
            near.append(extra(rs2_out.at[part], rs2_in.at[part], dev(dx=d), 46 + 4 * half + i))

    send_far(0)
    send_direct(0)
    send_far(1)
    send_relayed(0)
    send_direct(1)
    own_p[0] = call(project, 0, 0)
    send_relayed(1)
    own_p[1] = call(project, 0, 1)
    with jax.named_scope("wait_sq"):
        for q in sq_copies:
            q.wait_recv()
    total = sq[0]
    for k in range(1, 8):
        total = total + sq[k]
    total = jnp.sum(total, axis=0, keepdims=True)
    scale = lax.rsqrt(total / (8 * CH) + EPS)
    for half in range(2):
        with jax.named_scope("wait_near"):
            for q in near[4 * half : 4 * half + 4]:
                q.wait_recv()
        v = own_p[half] + rs2_in[0, half].astype(F32) + rs2_in[1, half].astype(F32)
        s = slice(half * SPAN, (half + 1) * SPAN)
        out[:, s] = (v * scale[:, s]).astype(BF)
    with jax.named_scope("wait_sends"):
        for k in MSGS:
            message(k).wait_send()
    for q in extra_sends:
        q.wait_send()


def run(*args):
    vm = pl.BlockSpec(memory_space=pltpu.VMEM)
    specs = [pl.BlockSpec(memory_space=pl.ANY)] * 12
    V = pltpu.VMEM
    scratch = [
        V((D,), F32),
        V((20, 2, D), BF),
        V((HEADS, D), BF),
        pltpu.SMEM((HEADS,), F32),
        pltpu.SMEM((HEADS,), F32),
        pltpu.SMEM((HEADS,), F32),
        V((4, CH), BF),
        V((4, 2, 128), BF),
        V((CH,), F32),
        V((TOK, D), BF),
        V((2, 40, KA), BF),
        V((2, 40, KB), BF),
        V((2, 40, D // 2), F32),
        V((D, 2, 128), BF),
        V((D, 256), BF),
        V((CH, 128), F32),
        V((CH, 128), F32),
        V((2, NY, NZ, 40, KA), BF),
        V((2, NY, NZ, 40, KB), BF),
        V((640, D), BF),
        V((D, 640), BF),
        V((528, 256), F32),
        V((TOK, 128), BF),
        V((128, TOK), BF),
        V((9, HEADS, 1, 128), F32),
        V((HEADS, TOK), F32),
        V((HEADS, TOK), F32),
        V((HEADS, TOK), F32),
        V((2, HEADS, 128), F32),
        V((2, SPAN, SPAN), F32),
        V((HEADS, 2, SPAN, SPAN), BF),
        V((128, TOK), F32),
        V((TOK, 128), F32),
        V((4, 160, 640), F32),
        V((160, TOK), F32),
        V((NY, 160, 640), F32),
        V((NY, 160, TOK), F32),
        V((CH, TOK), BF),
        V((CH, TOK), BF),
        V((2, CH, 128), F32),
        V((CH, TOK), F32),
        V((NZ, HEADS, 8, 128), BF),
        V((NZ, HEADS, 8, 128), BF),
        V((NZ, HEADS, 8, 128), BF),
        V((NZ, HEADS, 8, 128), BF),
        V((5, HEADS, 8, 128), BF),
        V((5, HEADS, 1, 128), F32),
        V((NZ, HEADS, 1, 128), F32),
        V((NZ, HEADS, 8, 128), F32),
        V((2, CH, 128), BF),
        V((2, CH, TOK), BF),
        V((NX, FEAT, 1280), BF),
        V((2, FEAT, 640), BF),
        V((9, 8, TOK), F32),
        V((2, FEAT, SPAN), BF),
        V((2, FEAT, SPAN), BF),
        V((2, 2, FEAT, SPAN), BF),
        V((2, 2, FEAT, SPAN), BF),
        V((2, FEAT, SPAN), F32),
        V((2, FEAT, SPAN), F32),
        V((16, D), BF),
        pltpu.SemaphoreType.DMA((N_MSG,)),
        pltpu.SemaphoreType.DMA((N_MSG,)),
        pltpu.SemaphoreType.DMA((52,)),
        pltpu.SemaphoreType.DMA((52,)),
        pltpu.SemaphoreType.DMA((15,)),
    ]
    return pl.pallas_call(
        kernel,
        out_shape=jax.ShapeDtypeStruct((FEAT, TOK), BF),
        in_specs=specs,
        out_specs=vm,
        scratch_shapes=scratch,
        compiler_params=pltpu.CompilerParams(
            collective_id=0, has_side_effects=True, vmem_limit_bytes=64 * 2**20 - 65536
        ),
        name="layer",
    )(*args)


def body(
    tokens, norm_gain, inner_weight, state_weight, step_weight, step_bias, decay_rate,
    skip_scale, conv_inner, conv_state, out_gain, out_weight,
):
    return run(
        tokens, norm_gain, inner_weight.transpose(2, 1, 0), state_weight, step_weight.T,
        step_bias, decay_rate, skip_scale, conv_inner, conv_state, out_gain, out_weight.T,
    ).T


def solution(mesh):
    return jax.shard_map(
        body,
        mesh=mesh,
        in_specs=(
            P("seq", None), P(), P(None, None, ("grp", "seq")), P(), P(None, "grp"), P("grp"),
            P("grp"), P("grp"), P(None, "grp"), P(), P("grp"), P(None, "grp"),
        ),
        out_specs=P("seq", "grp"),
        check_vma=False,
    )
```
